256 devices in a mesh: gx: 8 (over z), gy: 4 (over y), gz: 8 (over x, core).
Axes of the slice: x: 4, y: 4, z: 8, core: 2. Of those that a mesh axis runs over, the one named last changes fastest.
Arguments:
- point_data: float32 [1, 6, 131072], P(None, None, ('gx', 'gy', 'gz')), may hold values from -1 to 1
- neighbours: int32 [1, 64, 64, 64, 32], P(None, 'gx', 'gy', 'gz'), may hold values from 0 to 131071, as said below
- counts: int32 [1, 64, 64, 64], P(None, 'gx', 'gy', 'gz'), may hold values from 1 to 32, as said below
- kernel_in: bfloat16 [6, 80], replicated, may hold values from -2.5 to 2.5
- kernel_mid: bfloat16 [80, 80], replicated, may hold values from -0.625 to 0.625
- kernel_out: bfloat16 [80, 64], replicated, may hold values from -0.625 to 0.625
- spectral: bfloat16 [2, 16, 16, 16, 64, 64], P(None, 'gz', 'gx', 'gy'), may hold values from -48 to 48
- skip_weight: bfloat16 [64, 64], replicated, may hold values from -0.75 to 0.75
Outputs:
- latent_out: float32 [1, 64, 64, 64, 64], P(None, 'gx', 'gy', 'gz')
The draws below stay inside these ranges and needn't reach their ends.
Inputs may be any that keep to these rules, and one draw needn't show every extreme that they name: `neighbours`: points are owned by location: point j of a geometry belongs to the device at position j // 512 in the order gx, gy, gz. Every neighbour of a node is owned by the node's own device or by a device whose gx, gy and gz indices each differ from it by at most one. Slots s >= counts of the node are padding that names some point all the same. `counts`: on every device some node of every geometry has all 32 slots valid.
All inputs are finite; a program needn't handle non-finite values.
Results may differ from the reference program's by a relative error of at most 0.02.
Values may be sent and summed in bfloat16 or wider, within the bound.
A program may use at most 64 MiB of HBM per device.

```python
import math
import jax
import jax.numpy as jnp
from jax import lax

GRID = 64
CH = 64
MODES = 16
KH = 80
NB = 32
PT_DEV = 512
GEOMS = 1
LX = 8
LY = 16
LZ = 8
POINTS = 131072


def draw_neighbours(key, part):
    code_key, slot_key = jax.random.split(jax.random.fold_in(key, 11))
    shape = (GEOMS, GRID, GRID, GRID, NB)
    codes = jax.random.randint(code_key, shape, 0, 54)
    codes = jnp.where(codes >= 27, 13, codes)
    count_x = GRID // LX
    count_y = GRID // LY
    count_z = GRID // LZ
    home_x = (jnp.arange(GRID, dtype=jnp.int32) // LX).reshape(1, GRID, 1, 1, 1)
    home_y = (jnp.arange(GRID, dtype=jnp.int32) // LY).reshape(1, 1, GRID, 1, 1)
    home_z = (jnp.arange(GRID, dtype=jnp.int32) // LZ).reshape(1, 1, 1, GRID, 1)
    owner_x = jnp.clip(home_x + codes // 9 - 1, 0, count_x - 1)
    owner_y = jnp.clip(home_y + codes // 3 % 3 - 1, 0, count_y - 1)
    owner_z = jnp.clip(home_z + codes % 3 - 1, 0, count_z - 1)
    slots = jax.random.randint(slot_key, shape, 0, PT_DEV)
    return (((owner_x * count_y + owner_y) * count_z + owner_z) * PT_DEV + slots).astype(jnp.int32)


def draw_counts(key, part):
    values = jax.random.randint(jax.random.fold_in(key, 12), (GEOMS, GRID, GRID, GRID), 1, NB + 1)
    return values.at[:, ::LX, ::LY, ::LZ].set(NB).astype(jnp.int32)


def block_scale(own_key, extent, cuts, low, high):
    def one(dim, parts):
        draws = jax.random.uniform(jax.random.fold_in(jax.random.fold_in(own_key, 6), dim), (parts,), jnp.float32, low / len(cuts), high / len(cuts))
        return jnp.repeat(jnp.exp(draws), extent[dim] // parts).reshape((-1,) + (1,) * (len(extent) - dim - 1))

    level = one(*cuts[0])
    for cut in cuts[1:]:
        level = level * one(*cut)
    return level


def normal_values(key, shape, deviation, most, pieces=(), kind=jnp.bfloat16):
    drawn = deviation * jax.random.normal(key, shape, jnp.float32)
    if pieces:
        drawn = drawn * block_scale(key, shape, pieces, -0.22, 0.18)
    return jnp.clip(drawn, -most, most).astype(kind)


def setup_inputs(seed: int = 0) -> dict:
    key_list = jax.random.split(jax.random.key(seed), 9)
    return {
        "point_data": jnp.clip(jax.random.uniform(key_list[0], (GEOMS, 6, POINTS), jnp.float32, -1.0, 1.0) * block_scale(key_list[0], (GEOMS, 6, POINTS), ((2, 256),), -0.4, 0.0), -1.0, 1.0),
        "neighbours": draw_neighbours(jax.random.fold_in(key_list[8], 71), 0),
        "counts": draw_counts(jax.random.fold_in(key_list[8], 71), 0),
        "kernel_in": normal_values(key_list[3], (6, KH), 6 ** -0.5, 2.5),
        "kernel_mid": normal_values(key_list[4], (KH, KH), KH ** -0.5, 0.625),
        "kernel_out": normal_values(key_list[5], (KH, CH), KH ** -0.5, 0.625),
        "spectral": normal_values(key_list[6], (2, MODES, MODES, MODES, CH, CH), 8.0, 48.0, ((1, 8), (2, 8), (3, 4))),
        "skip_weight": normal_values(key_list[7], (CH, CH), CH ** -0.5, 0.75),
    }


HIGHEST = lax.Precision.HIGHEST
NORM_FLOOR = 1.0

def tables(length, keep_count, centred):
    position = jnp.arange(length, dtype=jnp.int32)
    frequency = jnp.arange(keep_count, dtype=jnp.int32)
    if centred:
        frequency = jnp.where(frequency < keep_count // 2, frequency, frequency + length - keep_count)
    phases = frequency[:, None] * position[None, :] % length
    angles = phases.astype(jnp.float32) * (2.0 * math.pi / length)
    return (jnp.cos(angles), jnp.sin(angles))

def third_weights(cos_table, sin_table, length):
    factor = jnp.where(jnp.arange(cos_table.shape[0]) == 0, 1.0, 2.0).astype(jnp.float32)[:, None] / length ** 3
    return (cos_table * factor, sin_table * factor)

def contract(pattern, operand, table):
    return jnp.einsum(pattern, operand, table, precision=HIGHEST)

def forward_real(values, cos_table, sin_table, pattern):
    return (contract(pattern, values, cos_table), -contract(pattern, values, sin_table))

def forward_complex(real_part, imag_part, cos_table, sin_table, pattern):
    new_real = contract(pattern, real_part, cos_table) + contract(pattern, imag_part, sin_table)
    new_imag = contract(pattern, imag_part, cos_table) - contract(pattern, real_part, sin_table)
    return (new_real, new_imag)

def inverse_complex(real_part, imag_part, cos_table, sin_table, pattern):
    new_real = contract(pattern, real_part, cos_table) - contract(pattern, imag_part, sin_table)
    new_imag = contract(pattern, real_part, sin_table) + contract(pattern, imag_part, cos_table)
    return (new_real, new_imag)

def inverse_real(real_part, imag_part, cos_table, sin_table, pattern):
    return contract(pattern, real_part, cos_table) - contract(pattern, imag_part, sin_table)

def kernel_mean(pair, valid, kernel_in, kernel_mid, kernel_out):
    hidden_one = jax.nn.gelu(jnp.dot(kernel_in.T, pair, preferred_element_type=jnp.float32), approximate=True).astype(jnp.bfloat16)
    hidden_two = jax.nn.gelu(jnp.dot(kernel_mid.T, hidden_one, preferred_element_type=jnp.float32), approximate=True).astype(jnp.bfloat16)
    values = jnp.dot(kernel_out.T, hidden_two, preferred_element_type=jnp.float32)
    values = values.reshape(values.shape[0], -1, NB)
    slots = jnp.arange(NB, dtype=jnp.int32)
    used = (slots[None, :] < valid[:, None]).astype(jnp.float32)
    total = lax.optimization_barrier(jnp.sum(values * used[None], axis=2))
    return (total / valid.astype(jnp.float32)[None]).T.astype(jnp.bfloat16)

def reference(point_data, neighbours, counts, kernel_in, kernel_mid, kernel_out, spectral, skip_weight):
    centres = (jnp.arange(GRID, dtype=jnp.int32).astype(jnp.float32) + 0.5) / GRID
    row_y = jnp.broadcast_to(centres[:, None, None], (GRID, GRID, NB)).reshape(1, -1)
    row_z = jnp.broadcast_to(centres[None, :, None], (GRID, GRID, NB)).reshape(1, -1)

    def one_slab(step):
        geometry = step // GRID
        slab = step % GRID
        points = lax.dynamic_index_in_dim(point_data, geometry, 0, keepdims=False)
        near = lax.dynamic_index_in_dim(lax.dynamic_index_in_dim(neighbours, geometry, 0, keepdims=False), slab, 0, keepdims=False).reshape(-1)
        valid = lax.dynamic_index_in_dim(lax.dynamic_index_in_dim(counts, geometry, 0, keepdims=False), slab, 0, keepdims=False).reshape(-1)
        picked = jnp.take(points, near, axis=1)
        row_x = (slab.astype(jnp.float32) + 0.5) / GRID
        pair = jnp.concatenate([picked[0:1] - row_x, picked[1:2] - row_y, picked[2:3] - row_z, picked[3:6]], axis=0).astype(jnp.bfloat16)
        return kernel_mean(pair, valid, kernel_in, kernel_mid, kernel_out)
    latent = lax.map(one_slab, jnp.arange(GEOMS * GRID, dtype=jnp.int32)).reshape(GEOMS, GRID, GRID, GRID, CH)
    cos_centred, sin_centred = tables(GRID, MODES, True)
    cos_third, sin_third = tables(GRID, MODES, False)
    back_cos, back_sin = third_weights(cos_third, sin_third, GRID)
    latent_wide = latent.astype(jnp.float32)
    real_part, imag_part = forward_real(latent_wide, cos_third, sin_third, 'gxyzc,kz->gxykc')
    real_part, imag_part = forward_complex(real_part, imag_part, cos_centred, sin_centred, 'gxykc,jy->gxjkc')
    real_part, imag_part = forward_complex(real_part, imag_part, cos_centred, sin_centred, 'gxjkc,ix->gijkc')
    spec_real = lax.optimization_barrier(real_part.astype(jnp.bfloat16)).astype(jnp.float32)
    spec_imag = lax.optimization_barrier(imag_part.astype(jnp.bfloat16)).astype(jnp.float32)
    mix_real = spectral[0].astype(jnp.float32)
    mix_imag = spectral[1].astype(jnp.float32)
    mixed_real = jnp.einsum('gijkc,ijkco->gijko', spec_real, mix_real) - jnp.einsum('gijkc,ijkco->gijko', spec_imag, mix_imag)
    mixed_imag = jnp.einsum('gijkc,ijkco->gijko', spec_real, mix_imag) + jnp.einsum('gijkc,ijkco->gijko', spec_imag, mix_real)
    mixed_real = lax.optimization_barrier(mixed_real.astype(jnp.bfloat16)).astype(jnp.float32)
    mixed_imag = lax.optimization_barrier(mixed_imag.astype(jnp.bfloat16)).astype(jnp.float32)
    real_part, imag_part = inverse_complex(mixed_real, mixed_imag, cos_centred, sin_centred, 'gijkc,ix->gxjkc')
    real_part, imag_part = inverse_complex(real_part, imag_part, cos_centred, sin_centred, 'gxjkc,jy->gxykc')
    branch = inverse_real(real_part, imag_part, back_cos, back_sin, 'gxykc,kz->gxyzc')
    cells_total = float(GRID ** 3)
    mean = lax.optimization_barrier(jnp.sum(branch, axis=(1, 2, 3))) / cells_total
    centred_branch = branch - mean[:, None, None, None, :]
    variance = lax.optimization_barrier(jnp.sum(centred_branch * centred_branch, axis=(1, 2, 3))) / cells_total
    skip = jnp.dot(latent.reshape(-1, CH), skip_weight, preferred_element_type=jnp.float32).reshape(GEOMS, GRID, GRID, GRID, CH)
    normed = centred_branch / jnp.sqrt(variance + NORM_FLOOR)[:, None, None, None, :]
    return jax.nn.gelu(normed + skip, approximate=True)
```

```python
import functools
import math

import jax
import jax.numpy as jnp
import numpy as np
from jax import lax
from jax.experimental import pallas as pl
from jax.experimental.pallas import tpu as pltpu
from jax.sharding import PartitionSpec as P

GRID = 64
MODES = 16
NB = 32
KH = 80
CH = 64
PTS = 512
NX, NY, NZ = 8, 4, 8
F32 = jnp.float32
BF16 = jnp.bfloat16
MESH_ID = pl.DeviceIdType.MESH


def dot(a, b):
    return jnp.dot(a, b, preferred_element_type=F32)


def gelu(v):
    inner = v * (0.7978845608028654 + 0.035677408136300125 * (v * v))
    half = 0.5 * v
    return half + half * jnp.tanh(inner)


def split_two(values):
    upper = values.astype(BF16)
    return upper, (values - upper.astype(F32)).astype(BF16)


def halo_kernel(pts_ref, out_ref, own, around, rows, send_sem, recv_sem):
    at = (lax.axis_index("gx"), lax.axis_index("gy"), lax.axis_index("gz"))
    sizes = (NX, NY, NZ)
    steps = [
        (dx, dy, dz)
        for dx in (-1, 0, 1)
        for dy in (-1, 0, 1)
        for dz in (-1, 0, 1)
        if (dx, dy, dz) != (0, 0, 0)
    ]

    def peer(step):
        return tuple(lax.rem(a + d + n, n) for a, d, n in zip(at, step, sizes))

    barrier = pltpu.get_barrier_semaphore()
    for step in steps:
        pl.semaphore_signal(barrier, inc=1, device_id=peer(step), device_id_type=MESH_ID)
    pl.semaphore_wait(barrier, len(steps))
    for step in steps:
        slot = ((1 - step[0]) * 3 + (1 - step[1])) * 3 + (1 - step[2])
        pltpu.make_async_remote_copy(
            src_ref=pts_ref,
            dst_ref=around.at[slot],
            send_sem=send_sem,
            recv_sem=recv_sem,
            device_id=peer(step),
            device_id_type=MESH_ID,
        ).start()
    around[13] = pts_ref[...]
    rows[pl.ds(240, 16), :] = jnp.zeros((16, PTS), F32)
    many = around.at[pl.ds(0, 26)]
    pltpu.make_async_copy(many, many, recv_sem).wait()
    for b in range(27):
        block = around[b]
        place = block[0:3]
        upper = place.astype(BF16).astype(F32)
        rows[pl.ds(9 * b, 9), :] = jnp.concatenate([upper, place - upper, block[3:6]], axis=0)
    out_ref[...] = rows[...].astype(BF16)
    pltpu.make_async_copy(many, many, send_sem).wait()


def halo_table(points):
    return pl.pallas_call(
        halo_kernel,
        out_shape=jax.ShapeDtypeStruct((256, PTS), BF16),
        in_specs=[pl.BlockSpec(memory_space=pltpu.VMEM)],
        out_specs=pl.BlockSpec(memory_space=pltpu.VMEM),
        scratch_shapes=[
            pltpu.VMEM((8, 128), F32),
            pltpu.VMEM((27, 6, PTS), F32),
            pltpu.VMEM((256, PTS), F32),
            pltpu.SemaphoreType.DMA,
            pltpu.SemaphoreType.DMA,
        ],
        compiler_params=pltpu.CompilerParams(collective_id=0, has_side_effects=True),
        name="halo",
    )(points)


def encode_kernel(
    tab_ref, blk_ref, slot_ref, cnt_ref, pre_ref, ids_ref, rowblk_ref, win_ref, wmid_ref, wout_ref,
    wskip_ref, lat_ref, skip_ref, acc, held,
):
    one = jnp.ones((PTS, 128), BF16)
    none = jnp.zeros((PTS, 128), BF16)
    lanes = 2

    def slab(x, carry):
        acc[...] = jnp.zeros((KH, 128), F32)
        base = pre_ref[x]
        valid = cnt_ref[x]

        def chunk(c, inner):
            first = pl.multiple_of(c * 8, 8)
            slots = slot_ref[x, pl.ds(first, 8), :]
            blocks = blk_ref[x, pl.ds(first, 8), :]
            total = jnp.zeros((KH, 128), F32)
            for part in range(8 // lanes):
                hot = []
                for s in range(part * lanes, (part + 1) * lanes):
                    row = jnp.broadcast_to(slots[s : s + 1], (PTS, 128)).astype(BF16)
                    hot.append(jnp.where(ids_ref[...] == row, one, none))
                found = dot(tab_ref[...], jnp.concatenate(hot, axis=1)).astype(BF16)
                kept = []
                for n, s in enumerate(range(part * lanes, (part + 1) * lanes)):
                    row = jnp.broadcast_to(blocks[s : s + 1], (256, 128)).astype(BF16)
                    kept.append(
                        jnp.where(
                            rowblk_ref[...] == row, found[:, n * 128 : (n + 1) * 128], none[0:256]
                        )
                    )
                pre = dot(win_ref[...], jnp.concatenate(kept, axis=1))
                pre = pre + jnp.concatenate([base] * lanes, axis=1)
                hidden = gelu(pre).astype(BF16)
                hidden = gelu(dot(wmid_ref[...], hidden)).astype(BF16).astype(F32)
                for n, s in enumerate(range(part * lanes, (part + 1) * lanes)):
                    used = valid > (c * 8 + s).astype(F32)
                    total = total + jnp.where(used, hidden[:, n * 128 : (n + 1) * 128], 0.0)
            acc[...] += total
            return inner

        lax.fori_loop(0, NB // 8, chunk, 0)
        upper, lower = split_two(acc[...])
        values = dot(wout_ref[...], upper) + dot(wout_ref[...], lower)
        latent = (values / valid).astype(BF16)
        skip_ref[x] = dot(wskip_ref[...], latent)
        held[x] = latent.astype(F32)
        return carry

    lax.fori_loop(0, 8, slab, 0)
    for x in range(8):
        lat_ref[:, x, :] = held[x]


def encode(tab, blk, slot, cnt, pre, ids, rowblk, win, wmid, wout, wskip):
    vmem = pl.BlockSpec(memory_space=pltpu.VMEM)
    return pl.pallas_call(
        encode_kernel,
        out_shape=(
            jax.ShapeDtypeStruct((CH, 8, 128), F32),
            jax.ShapeDtypeStruct((8, CH, 128), F32),
        ),
        in_specs=[vmem] * 11,
        out_specs=(vmem, vmem),
        scratch_shapes=[pltpu.VMEM((KH, 128), F32), pltpu.VMEM((8, CH, 128), F32)],
        name="encode",
    )(tab, blk, slot, cnt, pre, ids, rowblk, win, wmid, wout, wskip)


@functools.cache
def transform_tables():
    m = np.arange(GRID)
    centred = np.where(np.arange(MODES) < MODES // 2, np.arange(MODES), np.arange(MODES) - MODES)
    third = np.arange(MODES)

    def angles(f):
        return 2.0 * np.pi * ((f[:, None] * m[None, :]) % GRID) / GRID

    cos_c, sin_c = np.cos(angles(centred)), np.sin(angles(centred))
    cos_t, sin_t = np.cos(angles(third)), np.sin(angles(third))
    eye_y, eye_k = np.eye(16), np.eye(4)
    both = np.stack([cos_t, -sin_t], axis=-1)
    fz = np.einsum(
        "kqzr,yw->qyzkwr", both.reshape(MODES, NZ, 8, 2), eye_y
    ).reshape(NZ, 16, 8, 4, 4, 16, 2)
    fz = fz.transpose(0, 1, 2, 3, 5, 4, 6).reshape(1024, 512)
    turn = np.stack([np.stack([cos_c, -sin_c], -1), np.stack([sin_c, cos_c], -1)], -2)
    fy = np.einsum("jpyro,kl->pykrojl", turn.reshape(MODES, NY, 16, 2, 2), eye_k).reshape(512, 128)
    fx = np.concatenate([cos_c, sin_c], axis=0)
    ix = np.concatenate([cos_c.T, sin_c.T], axis=0)
    back = np.stack([np.stack([cos_c, sin_c], -1), np.stack([-sin_c, cos_c], -1)], -2)
    iy = np.einsum("jqyro,kl->rjkqylo", back.reshape(MODES, NY, 16, 2, 2), eye_k).reshape(128, 512)
    weight = np.where(third == 0, 1.0, 2.0)[:, None, None] / GRID**3
    iz = np.einsum(
        "kqzr,yw->kyrqwz", (both * weight).reshape(MODES, NZ, 8, 2), eye_y
    ).reshape(4, 4, 16, 2, NZ, 16, 8)
    iz = iz.transpose(0, 2, 1, 3, 4, 5, 6).reshape(512, 1024)
    mirror = np.zeros((MODES, MODES))
    for i in range(MODES):
        if i != MODES // 2:
            mirror[i, (MODES - i) % MODES] = 1.0
    flip = np.einsum(
        "rs,ij,kl->riksjl", np.diag([1.0, -1.0]), mirror.T, np.diag([1.0, 0, 0, 0])
    ).reshape(128, 128)
    return fz, fy, fx, ix, iy, iz, mirror, flip


def two_tables(table):
    import ml_dtypes

    upper = table.astype(np.float32).astype(ml_dtypes.bfloat16)
    lower = (table - upper.astype(np.float64)).astype(np.float32).astype(ml_dtypes.bfloat16)
    return jnp.asarray(upper), jnp.asarray(lower)


def layer_kernel(
    lat_ref, skip_ref, w0_ref, w1_ref, fzh_ref, fzl_ref, fyh_ref, fyl_ref, fxh_ref, fxl_ref,
    ixh_ref, ixl_ref, iyh_ref, iyl_ref, izh_ref, mir_ref, flip_ref, out_ref,
    s1, r1, s2, r2, s3, r3, s4, r4, s5, r5, s6, r6, s7, r7, sv, rv, s8, r8, spec, grid, wide,
    send_sem, recv_sem,
):
    gx, gy, gz = lax.axis_index("gx"), lax.axis_index("gy"), lax.axis_index("gz")
    barrier = pltpu.get_barrier_semaphore()

    def along_x(d):
        return (lax.rem(gx + d, NX), gy, gz)

    def along_y(d):
        return (gx, lax.rem(gy + d, NY), gz)

    def along_z(d):
        return (gx, gy, lax.rem(gz + d, NZ))

    plane = [
        (lax.rem(gx + dx, NX), gy, lax.rem(gz + dz, NZ))
        for dx in range(NX)
        for dz in range(NZ)
        if (dx, dz) != (0, 0)
    ]
    peers = plane + [along_y(d) for d in range(1, NY)]
    for peer in peers:
        pl.semaphore_signal(barrier, inc=1, device_id=peer, device_id_type=MESH_ID)
    s1[...] = lat_ref[...].reshape(NZ, 64, 128).astype(BF16)
    pl.semaphore_wait(barrier, len(peers))

    def send(n, source, target, peer):
        pltpu.make_async_remote_copy(
            src_ref=source,
            dst_ref=target,
            send_sem=send_sem.at[n],
            recv_sem=recv_sem.at[n],
            device_id=peer,
            device_id_type=MESH_ID,
        ).start()

    def arrived(n, buffer, count):
        part = buffer.at[pl.ds(0, count)]
        pltpu.make_async_copy(part, part, recv_sem.at[n]).wait()

    def left(n, buffer, count):
        part = buffer.at[pl.ds(0, count)]
        pltpu.make_async_copy(part, part, send_sem.at[n]).wait()

    for d in range(1, NZ):
        peer = along_z(d)
        send(0, s1.at[peer[2]], r1.at[gz], peer)
    r1[gz] = s1[gz]
    arrived(0, r1, NZ - 1)
    row = jnp.concatenate([r1[q] for q in range(NZ)], axis=1)
    deep = dot(row, fzh_ref[...]) + dot(row, fzl_ref[...])
    for q in range(NY):
        s2[q] = deep[:, q * 128 : (q + 1) * 128]
    for d in range(1, NY):
        peer = along_y(d)
        send(1, s2.at[peer[1]], r2.at[gy], peer)
    r2[gy] = s2[gy]
    arrived(1, r2, NY - 1)
    upper, lower = split_two(jnp.concatenate([r2[q] for q in range(NY)], axis=1))
    flat = dot(upper, fyh_ref[...]) + dot(upper, fyl_ref[...]) + dot(lower, fyh_ref[...])
    s3[...] = flat.reshape(NX, 8, 128)
    for d in range(1, NX):
        peer = along_x(d)
        send(2, s3.at[peer[0]], r3.at[gx], peer)
    r3[gx] = s3[gx]
    arrived(2, r3, NX - 1)
    upper, lower = split_two(r3[...].reshape(GRID, 128))
    both = dot(fxh_ref[...], upper) + dot(fxl_ref[...], upper) + dot(fxh_ref[...], lower)
    lane = lax.broadcasted_iota(jnp.int32, (MODES, 128), 1)
    turned = pltpu.roll(both[MODES:], 64, axis=1)
    modes = both[:MODES] + jnp.where(lane < 64, turned, -turned)
    for q in range(NZ):
        s4[q] = modes[2 * q : 2 * q + 2]
    for peer in plane:
        send(3, s4.at[peer[2]], r4.at[gz * NX + gx], peer)
    r4[gz * NX + gx] = s4[gz]
    arrived(3, r4, 63)
    for c in range(CH):
        for i in range(2):
            spec[i, pl.ds(c, 1), :] = r4[c, pl.ds(i, 1), :]
    srow = lax.broadcasted_iota(jnp.int32, (MODES, 128), 0)
    pick = jnp.where(lane == (srow // 8) * 64 + gx * 8 + srow % 8, 1.0, 0.0).astype(BF16)
    found = []
    for i in range(2):
        values = spec[i].astype(BF16)
        found.append(
            lax.dot_general(
                pick,
                jnp.concatenate([values, values], axis=0),
                (((1,), (1,)), ((), ())),
                preferred_element_type=F32,
            )
        )
    rows = jnp.concatenate(
        [found[0][0:8], found[1][0:8], found[0][8:16], found[1][8:16]], axis=0
    )
    spread = jnp.concatenate([rows] * 8, axis=1)
    big_row = lax.broadcasted_iota(jnp.int32, (32, 1024), 0)
    big_lane = lax.broadcasted_iota(jnp.int32, (32, 1024), 1)
    spread = jnp.where(big_lane // CH == big_row % MODES, spread, 0.0).astype(BF16)
    by_real, by_imag = dot(spread, w0_ref[...]), dot(spread, w1_ref[...])
    mixed_real = by_real[0:16] - by_imag[16:32]
    mixed_imag = by_imag[0:16] + by_real[16:32]
    for i in range(2):
        mine = jnp.concatenate(
            [mixed_real[8 * i : 8 * i + 8], mixed_imag[8 * i : 8 * i + 8]], axis=0
        ).astype(BF16)
        placed = lax.dot_general(
            mine, pick, (((0,), (0,)), ((), ())), preferred_element_type=F32
        )
        spec[i] = placed
    for c in range(CH):
        for i in range(2):
            s5[c, pl.ds(i, 1), :] = spec[i, pl.ds(c, 1), :]
    for peer in plane:
        send(4, s5.at[peer[2] * NX + peer[0]], r5.at[gz * NX + gx], peer)
    r5[gz * NX + gx] = s5[gz * NX + gx]
    arrived(4, r5, 63)
    for q in range(NZ):
        pair = r5[q * NX]
        for n in range(1, NX):
            pair = pair + r5[q * NX + n]
        grid[pl.ds(2 * q, 2), :] = pair
    is_mean = (srow == 0) & ((lane == 0) | (lane == 64)) & (gy == 0)
    values = jnp.where(is_mean, 0.0, grid[...])
    exact = values.astype(BF16)
    weight = jnp.where((lane % 4 == 0) & (gy == 0), 0.5, 2.0)
    pairs = dot(dot(mir_ref[...], exact).astype(BF16), flip_ref[...])
    pairs = jnp.where(gy == 0, 0.5 * pairs, 0.0)
    power = values * (weight * values + pairs)
    power = jnp.sum(jnp.sum(power, axis=1, keepdims=True), axis=0, keepdims=True)
    both = dot(ixh_ref[...], exact) + dot(ixl_ref[...], exact)
    lane = lax.broadcasted_iota(jnp.int32, (GRID, 128), 1)
    turned = pltpu.roll(both[GRID:], 64, axis=1)
    cells = both[:GRID] + jnp.where(lane < 64, -turned, turned)
    s6[:, 0:8, :] = cells.reshape(NX, 8, 128)
    s6[:, 8:16, :] = jnp.broadcast_to(power[None], (NX, 8, 128))
    for d in range(1, NX):
        peer = along_x(d)
        send(5, s6.at[peer[0]], r6.at[gx], peer)
    r6[gx] = s6[gx]
    arrived(5, r6, NX - 1)
    plain = r6[:, 0:8, :].reshape(64, 128).astype(BF16)
    flat = dot(plain, iyh_ref[...]) + dot(plain, iyl_ref[...])
    own_power = r6[:, 8:16, :].reshape(64, 128)
    for q in range(NY):
        s7[q] = flat[:, q * 128 : (q + 1) * 128].astype(BF16)
    sv[...] = own_power
    rv[gy] = own_power
    r7[gy] = s7[gy]
    for d in range(1, NY):
        peer = along_y(d)
        send(6, s7.at[peer[1]], r7.at[gy], peer)
        send(7, sv, rv.at[gy], peer)
    arrived(6, r7, NY - 1)
    row = jnp.concatenate([r7[q] for q in range(NY)], axis=1)
    depth = dot(row, izh_ref[...])
    arrived(7, rv, NY - 1)
    power = (rv[0] + rv[1]) + (rv[2] + rv[3])
    scale = 1.0 / jnp.sqrt(power * (1.0 / float(GRID) ** 6) + 1.0)
    for q in range(NZ):
        s8[q] = (depth[:, q * 128 : (q + 1) * 128] * scale).astype(BF16)
    for d in range(1, NZ):
        peer = along_z(d)
        send(8, s8.at[peer[2]], r8.at[gz], peer)
    r8[gz] = s8[gz]
    arrived(8, r8, NZ - 1)
    wide[...] = r8[...].astype(F32).reshape(CH, 8, 128)
    for x in range(8):
        out_ref[x] = gelu(wide[:, x, :] + skip_ref[x]).T
    left(0, r1, NZ - 1)
    left(1, r2, NY - 1)
    left(2, r3, NX - 1)
    left(3, r4, 63)
    left(4, r5, 63)
    left(5, r6, NX - 1)
    left(6, r7, NY - 1)
    left(7, rv, NY - 1)
    left(8, r8, NZ - 1)


def layer(lat, skip, w0, w1):
    fz, fy, fx, ix, iy, iz, mirror, flip = transform_tables()
    tables = [*two_tables(fz), *two_tables(fy), *two_tables(fx), *two_tables(ix), *two_tables(iy)]
    tables += [two_tables(iz)[0], two_tables(mirror)[0], two_tables(flip)[0]]
    vmem = pl.BlockSpec(memory_space=pltpu.VMEM)
    v = pltpu.VMEM
    return pl.pallas_call(
        layer_kernel,
        out_shape=jax.ShapeDtypeStruct((8, 128, CH), F32),
        in_specs=[vmem] * (4 + len(tables)),
        out_specs=vmem,
        scratch_shapes=[
            v((NZ, 64, 128), BF16), v((NZ, 64, 128), BF16),
            v((NY, 64, 128), F32), v((NY, 64, 128), F32),
            v((NX, 8, 128), F32), v((NX, 8, 128), F32),
            v((NZ, 2, 128), F32), v((CH, 2, 128), F32),
            v((CH, 2, 128), F32), v((CH, 2, 128), F32),
            v((NX, 16, 128), F32), v((NX, 16, 128), F32),
            v((NY, 64, 128), BF16), v((NY, 64, 128), BF16),
            v((64, 128), F32), v((NY, 64, 128), F32),
            v((NZ, 64, 128), BF16), v((NZ, 64, 128), BF16),
            v((2, CH, 128), F32), v((MODES, 128), F32), v((CH, 8, 128), F32),
            pltpu.SemaphoreType.DMA((9,)), pltpu.SemaphoreType.DMA((9,)),
        ],
        compiler_params=pltpu.CompilerParams(collective_id=1, has_side_effects=True),
        name="layer",
    )(lat, skip, w0, w1, *tables)


def body(point_data, neighbours, counts, kernel_in, kernel_mid, kernel_out, spectral, skip_weight):
    place = [lax.axis_index(a) for a in ("gx", "gy", "gz")]
    tab = halo_table(point_data[0])
    near = jnp.swapaxes(neighbours.reshape(8, 128, NB), 1, 2)
    owner = near // PTS
    offset_z = owner % NZ - place[2] + 1
    offset_y = owner // NZ % NY - place[1] + 1
    offset_x = owner // (NZ * NY) - place[0] + 1
    blk = ((offset_x * 3 + offset_y) * 3 + offset_z).astype(F32)
    slot = (near % PTS - 256).astype(F32)
    cnt = counts.reshape(8, 1, 128).astype(F32)
    wide_in = kernel_in.astype(F32)

    def centre(start, count):
        cells = start * count + jnp.arange(count, dtype=jnp.int32)
        return (cells.astype(F32) + 0.5) / GRID

    cx, cy, cz = centre(place[0], 8), centre(place[1], 16), centre(place[2], 8)
    inner = (
        wide_in[1][:, None, None] * cy[None, :, None] + wide_in[2][:, None, None] * cz[None, None, :]
    ).reshape(KH, 128)
    pre = -(inner[None] + (wide_in[0][None, :] * cx[:, None])[:, :, None])
    nine = jnp.concatenate([kernel_in[0:3], kernel_in[0:3], kernel_in[3:6]], axis=0)
    win = jnp.pad(jnp.concatenate([nine] * 27, axis=0), ((0, 13), (0, 0))).T
    ids = jnp.broadcast_to((jnp.arange(PTS) - 256).astype(BF16)[:, None], (PTS, 128))
    rowblk = jnp.broadcast_to((jnp.arange(256) // 9).astype(BF16)[:, None], (256, 128))
    lat, skip = encode(
        tab, blk, slot, cnt, pre, ids, rowblk, win, kernel_mid.T, kernel_out.T, skip_weight.T
    )
    out = layer(lat, skip, spectral[0].reshape(1024, CH), spectral[1].reshape(1024, CH))
    return out.reshape(1, 8, 16, 8, CH)


def solution(mesh):
    cells = P(None, "gx", "gy", "gz", None)
    return jax.shard_map(
        body,
        mesh=mesh,
        in_specs=(
            P(None, None, ("gx", "gy", "gz")),
            cells,
            P(None, "gx", "gy", "gz"),
            P(),
            P(),
            P(),
            P(None, "gz", "gx", "gy", None, None),
            P(),
        ),
        out_specs=cells,
        check_vma=False,
    )
```

```python
import functools
import math

import jax
import jax.numpy as jnp
import numpy as np
from jax import lax
from jax.experimental import pallas as pl
from jax.experimental.pallas import tpu as pltpu
from jax.sharding import PartitionSpec as P

GRID = 64
MODES = 16
NB = 32
KH = 80
CH = 64
PTS = 512
NX, NY, NZ = 8, 4, 8
F32 = jnp.float32
BF16 = jnp.bfloat16
MESH_ID = pl.DeviceIdType.MESH


def dot(a, b):
    return jnp.dot(a, b, preferred_element_type=F32)


def gelu(v):
    inner = v * (0.7978845608028654 + 0.035677408136300125 * (v * v))
    half = 0.5 * v
    return half + half * jnp.tanh(inner)


def split_two(values):
    upper = values.astype(BF16)
    return upper, (values - upper.astype(F32)).astype(BF16)


def halo_kernel(pts_ref, out_ref, own, around, rows, send_sem, recv_sem):
    at = (lax.axis_index("gx"), lax.axis_index("gy"), lax.axis_index("gz"))
    sizes = (NX, NY, NZ)
    steps = [
        (dx, dy, dz)
        for dx in (-1, 0, 1)
        for dy in (-1, 0, 1)
        for dz in (-1, 0, 1)
        if (dx, dy, dz) != (0, 0, 0)
    ]

    def peer(step):
        return tuple(lax.rem(a + d + n, n) for a, d, n in zip(at, step, sizes))

    barrier = pltpu.get_barrier_semaphore()
    for step in steps:
        pl.semaphore_signal(barrier, inc=1, device_id=peer(step), device_id_type=MESH_ID)
    pl.semaphore_wait(barrier, len(steps))
    for step in steps:
        slot = ((1 - step[0]) * 3 + (1 - step[1])) * 3 + (1 - step[2])
        pltpu.make_async_remote_copy(
            src_ref=pts_ref,
            dst_ref=around.at[slot],
            send_sem=send_sem,
            recv_sem=recv_sem,
            device_id=peer(step),
            device_id_type=MESH_ID,
        ).start()
    around[13] = pts_ref[...]
    rows[pl.ds(240, 16), :] = jnp.zeros((16, PTS), F32)
    many = around.at[pl.ds(0, 26)]
    pltpu.make_async_copy(many, many, recv_sem).wait()
    for b in range(27):
        block = around[b]
        place = block[0:3]
        upper = place.astype(BF16).astype(F32)
        rows[pl.ds(9 * b, 9), :] = jnp.concatenate([upper, place - upper, block[3:6]], axis=0)
    out_ref[...] = rows[...].astype(BF16)
    pltpu.make_async_copy(many, many, send_sem).wait()


def halo_table(points):
    return pl.pallas_call(
        halo_kernel,
        out_shape=jax.ShapeDtypeStruct((256, PTS), BF16),
        in_specs=[pl.BlockSpec(memory_space=pltpu.VMEM)],
        out_specs=pl.BlockSpec(memory_space=pltpu.VMEM),
        scratch_shapes=[
            pltpu.VMEM((8, 128), F32),
            pltpu.VMEM((27, 6, PTS), F32),
            pltpu.VMEM((256, PTS), F32),
            pltpu.SemaphoreType.DMA,
            pltpu.SemaphoreType.DMA,
        ],
        compiler_params=pltpu.CompilerParams(collective_id=0, has_side_effects=True),
        name="halo",
    )(points)


def dot_first(a, b):
    return lax.dot_general(a, b, (((0,), (0,)), ((), ())), preferred_element_type=F32)


def twice_gelu(v):
    inner = v * (0.7978845608028654 + 0.035677408136300125 * (v * v))
    return v + v * jnp.tanh(inner)


CHUNKS = 32
PART = 256


def encode_kernel(
    tab_ref, blk_ref, slot_ref, cnt_ref, kin_ref, kmid_ref, kout_ref, wskip_ref,
    lat_ref, skip_ref, acc, pre, ids, rowblk, win, wmid, masked_a, masked_b, hid_a, hid_b,
):
    def iota(shape, dim):
        return lax.broadcasted_iota(jnp.int32, shape, dim)

    ids[...] = (iota((PTS, 128), 0) - 256).astype(F32).astype(BF16)
    rowblk[...] = (iota((256, 128), 0) // 9).astype(F32).astype(BF16)
    col = iota((6, 256), 1)
    nine = col % 9
    source = jnp.where(nine < 3, nine, nine - 3)
    chosen = jnp.where((source == iota((6, 256), 0)) & (col < 243), 1.0, 0.0).astype(BF16)
    win[...] = dot_first(kin_ref[...], chosen).astype(BF16)
    eye = jnp.where(iota((KH, KH), 0) == iota((KH, KH), 1), 0.5, 0.0).astype(BF16)
    wmid[...] = dot_first(kmid_ref[...], eye).astype(BF16)
    row, lane = iota((6, 128), 0), iota((6, 128), 1)
    index_y = lax.axis_index("gy") * 16 + lane // 8
    index_z = lax.axis_index("gz") * 8 + lane % 8
    for x in range(8):
        index = jnp.where(row == 0, lax.axis_index("gx") * 8 + x, jnp.where(row == 1, index_y, index_z))
        centre = jnp.where(row < 3, -(index.astype(F32) + 0.5) / GRID, 0.0).astype(BF16)
        pre[x] = dot_first(kin_ref[...], centre)
    acc[...] = jnp.zeros((8, KH, 128), F32)
    one = jnp.ones((PTS, 128), BF16)
    none = jnp.zeros((PTS, 128), BF16)

    def step(t, masked_out, masked_in, hid_out, hid_in):
        early = jnp.minimum(t, CHUNKS - 1)
        middle = jnp.clip(t - 1, 0, CHUNKS - 1)
        late = jnp.maximum(t - 2, 0)
        slots, blocks = slot_ref[early], blk_ref[early]
        base = jnp.concatenate([pre[middle // 4]] * 2, axis=1)
        valid = jnp.where(t >= 2, cnt_ref[late // 4], 0.0)
        first = (late % 4 * 8).astype(F32)
        total = jnp.zeros((KH, 128), F32)
        for part in range(4):
            span = pl.ds(part * PART, PART)
            hot = []
            for s in (2 * part, 2 * part + 1):
                chosen = jnp.broadcast_to(slots[s : s + 1], (PTS, 128)).astype(BF16)
                hot.append(jnp.where(ids[...] == chosen, one, none))
            found = dot(tab_ref[...], jnp.concatenate(hot, axis=1))
            ahead = dot(win[...], masked_in[:, span])
            last = dot(wmid[...], hid_in[:, span])
            hid_out[:, span] = twice_gelu(ahead + base).astype(BF16)
            last = twice_gelu(last).astype(BF16).astype(F32)
            for n in range(2):
                used = valid > first + (2 * part + n)
                total = total + jnp.where(used, last[:, n * 128 : (n + 1) * 128], 0.0)
            found = found.astype(BF16)
            for n in range(2):
                s = 2 * part + n
                chosen = jnp.broadcast_to(blocks[s : s + 1], (256, 128)).astype(BF16)
                masked_out[:, pl.ds(s * 128, 128)] = jnp.where(
                    rowblk[...] == chosen, found[:, n * 128 : (n + 1) * 128], none[0:256]
                )
        acc[late // 4] += total

    def two_steps(tt, carry):
        step(2 * tt, masked_a, masked_b, hid_a, hid_b)
        step(2 * tt + 1, masked_b, masked_a, hid_b, hid_a)
        return carry

    lax.fori_loop(0, CHUNKS // 2 + 1, two_steps, 0)
    for x in range(8):
        upper, lower = split_two(0.5 * acc[x])
        values = dot_first(kout_ref[...], upper) + dot_first(kout_ref[...], lower)
        latent = (values / cnt_ref[x]).astype(BF16)
        skip_ref[x] = dot_first(wskip_ref[...], latent)
        lat_ref[x] = latent.astype(F32)


def encode(tab, blk, slot, cnt, kin, kmid, kout, wskip):
    vmem = pl.BlockSpec(memory_space=pltpu.VMEM)
    v = pltpu.VMEM
    return pl.pallas_call(
        encode_kernel,
        out_shape=(
            jax.ShapeDtypeStruct((8, CH, 128), F32),
            jax.ShapeDtypeStruct((8, CH, 128), F32),
        ),
        in_specs=[vmem] * 8,
        out_specs=(vmem, vmem),
        scratch_shapes=[
            v((8, KH, 128), F32), v((8, KH, 128), F32),
            v((PTS, 128), BF16), v((256, 128), BF16), v((KH, 256), BF16), v((KH, KH), BF16),
            v((256, 1024), BF16), v((256, 1024), BF16), v((KH, 1024), BF16), v((KH, 1024), BF16),
        ],
        name="encode",
    )(tab, blk, slot, cnt, kin, kmid, kout, wskip)


@functools.cache
def transform_tables():
    m = np.arange(GRID)
    centred = np.where(np.arange(MODES) < MODES // 2, np.arange(MODES), np.arange(MODES) - MODES)
    third = np.arange(MODES)

    def angles(f):
        return 2.0 * np.pi * ((f[:, None] * m[None, :]) % GRID) / GRID

    cos_c, sin_c = np.cos(angles(centred)), np.sin(angles(centred))
    cos_t, sin_t = np.cos(angles(third)), np.sin(angles(third))
    eye_y, eye_k = np.eye(16), np.eye(4)
    both = np.stack([cos_t, -sin_t], axis=-1)
    fz = np.einsum(
        "kqzr,yw->qyzkwr", both.reshape(MODES, NZ, 8, 2), eye_y
    ).reshape(NZ, 16, 8, 4, 4, 16, 2)
    fz = fz.transpose(0, 1, 2, 3, 5, 4, 6).reshape(1024, 512)
    turn = np.stack([np.stack([cos_c, -sin_c], -1), np.stack([sin_c, cos_c], -1)], -2)
    fy = np.einsum("jpyro,kl->pykrojl", turn.reshape(MODES, NY, 16, 2, 2), eye_k).reshape(512, 128)
    fx = np.concatenate([cos_c, sin_c], axis=0)
    ix = np.concatenate([cos_c.T, sin_c.T], axis=0)
    back = np.stack([np.stack([cos_c, sin_c], -1), np.stack([-sin_c, cos_c], -1)], -2)
    iy = np.einsum("jqyro,kl->rjkqylo", back.reshape(MODES, NY, 16, 2, 2), eye_k).reshape(128, 512)
    weight = np.where(third == 0, 1.0, 2.0)[:, None, None] / GRID**3
    iz = np.einsum(
        "kqzr,yw->kyrqwz", (both * weight).reshape(MODES, NZ, 8, 2), eye_y
    ).reshape(4, 4, 16, 2, NZ, 16, 8)
    iz = iz.transpose(0, 2, 1, 3, 4, 5, 6).reshape(512, 1024)
    mirror = np.zeros((MODES, MODES))
    for i in range(MODES):
        if i != MODES // 2:
            mirror[i, (MODES - i) % MODES] = 1.0
    flip = np.einsum(
        "rs,ij,kl->riksjl", np.diag([1.0, -1.0]), mirror.T, np.diag([1.0, 0, 0, 0])
    ).reshape(128, 128)
    return fz, fy, fx, ix, iy, iz, mirror, flip


def two_tables(table):
    import ml_dtypes

    upper = table.astype(np.float32).astype(ml_dtypes.bfloat16)
    lower = (table - upper.astype(np.float64)).astype(np.float32).astype(ml_dtypes.bfloat16)
    return jnp.asarray(upper), jnp.asarray(lower)


def layer_kernel(
    lat_ref, skip_ref, w_ref, fzh_ref, fzl_ref, fyh_ref, fyl_ref, fxh_ref, fxl_ref,
    ixh_ref, ixl_ref, iyh_ref, iyl_ref, izh_ref, mir_ref, flip_ref, out_ref,
    s1, r1, s2, r2, s3, r3, s4, r4, s5, r5, s6, r6, s7, r7, sv, rv, s8, r8, spec, grid, wide,
    send_sem, recv_sem,
):
    gx, gy, gz = lax.axis_index("gx"), lax.axis_index("gy"), lax.axis_index("gz")
    barrier = pltpu.get_barrier_semaphore()

    def along_x(d):
        return (lax.rem(gx + d, NX), gy, gz)

    def along_y(d):
        return (gx, lax.rem(gy + d, NY), gz)

    def along_z(d):
        return (gx, gy, lax.rem(gz + d, NZ))

    plane = [
        (lax.rem(gx + dx, NX), gy, lax.rem(gz + dz, NZ))
        for dx in range(NX)
        for dz in range(NZ)
        if (dx, dz) != (0, 0)
    ]
    peers = plane + [along_y(d) for d in range(1, NY)]
    for peer in peers:
        pl.semaphore_signal(barrier, inc=1, device_id=peer, device_id_type=MESH_ID)
    for q in range(NZ):
        s1[q] = lat_ref[:, pl.ds(8 * q, 8), :].reshape(64, 128).astype(BF16)
    pl.semaphore_wait(barrier, len(peers))

    def send(n, source, target, peer):
        pltpu.make_async_remote_copy(
            src_ref=source,
            dst_ref=target,
            send_sem=send_sem.at[n],
            recv_sem=recv_sem.at[n],
            device_id=peer,
            device_id_type=MESH_ID,
        ).start()

    def arrived(n, buffer, count):
        part = buffer.at[pl.ds(0, count)]
        pltpu.make_async_copy(part, part, recv_sem.at[n]).wait()

    def left(n, buffer, count):
        part = buffer.at[pl.ds(0, count)]
        pltpu.make_async_copy(part, part, send_sem.at[n]).wait()

    for d in range(1, NZ):
        peer = along_z(d)
        send(0, s1.at[peer[2]], r1.at[gz], peer)
    r1[gz] = s1[gz]
    arrived(0, r1, NZ - 1)
    row = jnp.concatenate([r1[q] for q in range(NZ)], axis=1)
    deep = dot(row, fzh_ref[...]) + dot(row, fzl_ref[...])
    for q in range(NY):
        s2[q] = deep[:, q * 128 : (q + 1) * 128]
    for d in range(1, NY):
        peer = along_y(d)
        send(1, s2.at[peer[1]], r2.at[gy], peer)
    r2[gy] = s2[gy]
    arrived(1, r2, NY - 1)
    upper, lower = split_two(jnp.concatenate([r2[q] for q in range(NY)], axis=1))
    flat = dot(upper, fyh_ref[...]) + dot(upper, fyl_ref[...]) + dot(lower, fyh_ref[...])
    for x in range(8):
        s3[:, x, :] = flat[8 * x : 8 * x + 8]
    for d in range(1, NX):
        peer = along_x(d)
        send(2, s3.at[peer[0]], r3.at[gx], peer)
    r3[gx] = s3[gx]
    arrived(2, r3, NX - 1)
    upper, lower = split_two(r3[...].reshape(GRID, 128))
    both = dot(fxh_ref[...], upper) + dot(fxl_ref[...], upper) + dot(fxh_ref[...], lower)
    lane = lax.broadcasted_iota(jnp.int32, (MODES, 128), 1)
    turned = pltpu.roll(both[MODES:], 64, axis=1)
    modes = both[:MODES] + jnp.where(lane < 64, turned, -turned)
    for q in range(NZ):
        s4[q] = modes[2 * q : 2 * q + 2]
    for peer in plane:
        send(3, s4.at[peer[2]], r4.at[gz * NX + gx], peer)
    r4[gz * NX + gx] = s4[gz]
    arrived(3, r4, 63)
    for c in range(CH):
        for i in range(2):
            spec[i, pl.ds(c, 1), :] = r4[c, pl.ds(i, 1), :]
    srow = lax.broadcasted_iota(jnp.int32, (MODES, 128), 0)
    pick = jnp.where(lane == (srow // 8) * 64 + gx * 8 + srow % 8, 1.0, 0.0).astype(BF16)
    found = []
    for i in range(2):
        values = spec[i].astype(BF16)
        found.append(
            lax.dot_general(
                pick,
                jnp.concatenate([values, values], axis=0),
                (((1,), (1,)), ((), ())),
                preferred_element_type=F32,
            )
        )
    rows = jnp.concatenate(
        [found[0][0:8], found[1][0:8], found[0][8:16], found[1][8:16]], axis=0
    )
    spread = jnp.concatenate([rows] * 8, axis=1)
    big_row = lax.broadcasted_iota(jnp.int32, (32, 1024), 0)
    big_lane = lax.broadcasted_iota(jnp.int32, (32, 1024), 1)
    spread = jnp.where(big_lane // CH == big_row % MODES, spread, 0.0).astype(BF16)
    by_real, by_imag = dot(spread, w_ref[0:1024]), dot(spread, w_ref[1024:2048])
    mixed_real = by_real[0:16] - by_imag[16:32]
    mixed_imag = by_imag[0:16] + by_real[16:32]
    for i in range(2):
        mine = jnp.concatenate(
            [mixed_real[8 * i : 8 * i + 8], mixed_imag[8 * i : 8 * i + 8]], axis=0
        ).astype(BF16)
        placed = lax.dot_general(
            mine, pick, (((0,), (0,)), ((), ())), preferred_element_type=F32
        )
        spec[i] = placed
    for c in range(CH):
        for i in range(2):
            s5[c, pl.ds(i, 1), :] = spec[i, pl.ds(c, 1), :]
    for peer in plane:
        send(4, s5.at[peer[2] * NX + peer[0]], r5.at[gz * NX + gx], peer)
    r5[gz * NX + gx] = s5[gz * NX + gx]
    arrived(4, r5, 63)
    for q in range(NZ):
        pair = r5[q * NX]
        for n in range(1, NX):
            pair = pair + r5[q * NX + n]
        grid[pl.ds(2 * q, 2), :] = pair
    is_mean = (srow == 0) & ((lane == 0) | (lane == 64)) & (gy == 0)
    values = jnp.where(is_mean, 0.0, grid[...])
    exact = values.astype(BF16)
    weight = jnp.where((lane % 4 == 0) & (gy == 0), 0.5, 2.0)
    pairs = dot(dot(mir_ref[...], exact).astype(BF16), flip_ref[...])
    pairs = jnp.where(gy == 0, 0.5 * pairs, 0.0)
    power = values * (weight * values + pairs)
    power = jnp.sum(jnp.sum(power, axis=1, keepdims=True), axis=0, keepdims=True)
    both = dot(ixh_ref[...], exact) + dot(ixl_ref[...], exact)
    lane = lax.broadcasted_iota(jnp.int32, (GRID, 128), 1)
    turned = pltpu.roll(both[GRID:], 64, axis=1)
    cells = both[:GRID] + jnp.where(lane < 64, -turned, turned)
    s6[:, 0:8, :] = cells.reshape(NX, 8, 128)
    s6[:, 8:16, :] = jnp.broadcast_to(power[None], (NX, 8, 128))
    for d in range(1, NX):
        peer = along_x(d)
        send(5, s6.at[peer[0]], r6.at[gx], peer)
    r6[gx] = s6[gx]
    arrived(5, r6, NX - 1)
    plain = jnp.concatenate([r6[:, x, :] for x in range(8)], axis=0).astype(BF16)
    flat = dot(plain, iyh_ref[...]) + dot(plain, iyl_ref[...])
    own_power = jnp.concatenate([r6[:, 8, :]] * 8, axis=0)
    for q in range(NY):
        s7[q] = flat[:, q * 128 : (q + 1) * 128].astype(BF16)
    sv[...] = own_power
    rv[gy] = own_power
    r7[gy] = s7[gy]
    for d in range(1, NY):
        peer = along_y(d)
        send(6, s7.at[peer[1]], r7.at[gy], peer)
        send(7, sv, rv.at[gy], peer)
    arrived(6, r7, NY - 1)
    row = jnp.concatenate([r7[q] for q in range(NY)], axis=1)
    depth = dot(row, izh_ref[...])
    arrived(7, rv, NY - 1)
    power = (rv[0] + rv[1]) + (rv[2] + rv[3])
    scale = 1.0 / jnp.sqrt(power * (1.0 / float(GRID) ** 6) + 1.0)
    for q in range(NZ):
        s8[q] = (depth[:, q * 128 : (q + 1) * 128] * scale).astype(BF16)
    for d in range(1, NZ):
        peer = along_z(d)
        send(8, s8.at[peer[2]], r8.at[gz], peer)
    r8[gz] = s8[gz]
    arrived(8, r8, NZ - 1)
    wide[...] = r8[...].astype(F32)
    for x in range(8):
        out_ref[x] = gelu(wide[:, pl.ds(8 * x, 8), :].reshape(CH, 128) + skip_ref[x]).T
    left(0, r1, NZ - 1)
    left(1, r2, NY - 1)
    left(2, r3, NX - 1)
    left(3, r4, 63)
    left(4, r5, 63)
    left(5, r6, NX - 1)
    left(6, r7, NY - 1)
    left(7, rv, NY - 1)
    left(8, r8, NZ - 1)


def layer(lat, skip, weights):
    fz, fy, fx, ix, iy, iz, mirror, flip = transform_tables()
    tables = [*two_tables(fz), *two_tables(fy), *two_tables(fx), *two_tables(ix), *two_tables(iy)]
    tables += [two_tables(iz)[0], two_tables(mirror)[0], two_tables(flip)[0]]
    vmem = pl.BlockSpec(memory_space=pltpu.VMEM)
    v = pltpu.VMEM
    return pl.pallas_call(
        layer_kernel,
        out_shape=jax.ShapeDtypeStruct((8, 128, CH), F32),
        in_specs=[vmem] * (3 + len(tables)),
        out_specs=vmem,
        scratch_shapes=[
            v((NZ, 64, 128), BF16), v((NZ, 64, 128), BF16),
            v((NY, 64, 128), F32), v((NY, 64, 128), F32),
            v((NX, 8, 128), F32), v((NX, 8, 128), F32),
            v((NZ, 2, 128), F32), v((CH, 2, 128), F32),
            v((CH, 2, 128), F32), v((CH, 2, 128), F32),
            v((NX, 16, 128), F32), v((NX, 16, 128), F32),
            v((NY, 64, 128), BF16), v((NY, 64, 128), BF16),
            v((64, 128), F32), v((NY, 64, 128), F32),
            v((NZ, 64, 128), BF16), v((NZ, 64, 128), BF16),
            v((2, CH, 128), F32), v((MODES, 128), F32), v((NZ, 64, 128), F32),
            pltpu.SemaphoreType.DMA((9,)), pltpu.SemaphoreType.DMA((9,)),
        ],
        compiler_params=pltpu.CompilerParams(collective_id=1, has_side_effects=True),
        name="layer",
    )(lat, skip, weights, *tables)


def body(point_data, neighbours, counts, kernel_in, kernel_mid, kernel_out, spectral, skip_weight):
    place = [lax.axis_index(a) for a in ("gx", "gy", "gz")]
    tab = halo_table(point_data[0])
    near = jnp.swapaxes(neighbours.reshape(8, 128, NB), 1, 2)
    owner = near // PTS
    offset_z = owner % NZ - place[2] + 1
    offset_y = owner // NZ % NY - place[1] + 1
    offset_x = owner // (NZ * NY) - place[0] + 1
    blk = ((offset_x * 3 + offset_y) * 3 + offset_z).astype(F32).reshape(CHUNKS, 8, 128)
    slot = (near % PTS - 256).astype(F32).reshape(CHUNKS, 8, 128)
    cnt = counts.reshape(8, 1, 128).astype(F32)
    lat, skip = encode(
        tab, blk, slot, cnt, kernel_in, kernel_mid, kernel_out, skip_weight
    )
    out = layer(lat, skip, spectral.reshape(2048, CH))
    return out.reshape(1, 8, 16, 8, CH)


def solution(mesh):
    cells = P(None, "gx", "gy", "gz", None)
    return jax.shard_map(
        body,
        mesh=mesh,
        in_specs=(
            P(None, None, ("gx", "gy", "gz")),
            cells,
            P(None, "gx", "gy", "gz"),
            P(),
            P(),
            P(),
            P(None, "gz", "gx", "gy", None, None),
            P(),
        ),
        out_specs=cells,
        check_vma=False,
    )
```

```python
import functools
import math

import jax
import jax.numpy as jnp
import numpy as np
from jax import lax
from jax.experimental import pallas as pl
from jax.experimental.pallas import tpu as pltpu
from jax.sharding import PartitionSpec as P

GRID = 64
MODES = 16
NB = 32
KH = 80
CH = 64
PTS = 512
NX, NY, NZ = 8, 4, 8
F32 = jnp.float32
BF16 = jnp.bfloat16
MESH_ID = pl.DeviceIdType.MESH


def dot(a, b):
    return jnp.dot(a, b, preferred_element_type=F32)


def gelu(v):
    inner = v * (0.7978845608028654 + 0.035677408136300125 * (v * v))
    half = 0.5 * v
    return half + half * jnp.tanh(inner)


def split_two(values):
    upper = values.astype(BF16)
    return upper, (values - upper.astype(F32)).astype(BF16)


def halo_kernel(pts_ref, out_ref, own, around, rows, send_sem, recv_sem):
    at = (lax.axis_index("gx"), lax.axis_index("gy"), lax.axis_index("gz"))
    sizes = (NX, NY, NZ)
    steps = [
        (dx, dy, dz)
        for dx in (-1, 0, 1)
        for dy in (-1, 0, 1)
        for dz in (-1, 0, 1)
        if (dx, dy, dz) != (0, 0, 0)
    ]

    def peer(step):
        return tuple(lax.rem(a + d + n, n) for a, d, n in zip(at, step, sizes))

    barrier = pltpu.get_barrier_semaphore()
    for step in steps:
        pl.semaphore_signal(barrier, inc=1, device_id=peer(step), device_id_type=MESH_ID)
    pl.semaphore_wait(barrier, len(steps))
    for step in steps:
        slot = ((1 - step[0]) * 3 + (1 - step[1])) * 3 + (1 - step[2])
        pltpu.make_async_remote_copy(
            src_ref=pts_ref,
            dst_ref=around.at[slot],
            send_sem=send_sem,
            recv_sem=recv_sem,
            device_id=peer(step),
            device_id_type=MESH_ID,
        ).start()
    around[13] = pts_ref[...]
    rows[pl.ds(240, 16), :] = jnp.zeros((16, PTS), F32)
    many = around.at[pl.ds(0, 26)]
    pltpu.make_async_copy(many, many, recv_sem).wait()
    for b in range(27):
        block = around[b]
        place = block[0:3]
        upper = place.astype(BF16).astype(F32)
        rows[pl.ds(9 * b, 9), :] = jnp.concatenate([upper, place - upper, block[3:6]], axis=0)
    out_ref[...] = rows[...].astype(BF16)
    pltpu.make_async_copy(many, many, send_sem).wait()


def halo_table(points):
    return pl.pallas_call(
        halo_kernel,
        out_shape=jax.ShapeDtypeStruct((256, PTS), BF16),
        in_specs=[pl.BlockSpec(memory_space=pltpu.VMEM)],
        out_specs=pl.BlockSpec(memory_space=pltpu.VMEM),
        scratch_shapes=[
            pltpu.VMEM((8, 128), F32),
            pltpu.VMEM((27, 6, PTS), F32),
            pltpu.VMEM((256, PTS), F32),
            pltpu.SemaphoreType.DMA,
            pltpu.SemaphoreType.DMA,
        ],
        compiler_params=pltpu.CompilerParams(collective_id=0, has_side_effects=True),
        name="halo",
    )(points)


def dot_first(a, b):
    return lax.dot_general(a, b, (((0,), (0,)), ((), ())), preferred_element_type=F32)


def twice_gelu(v):
    inner = v * (0.7978845608028654 + 0.035677408136300125 * (v * v))
    return v + v * jnp.tanh(inner)


CHUNKS = 32
PART = 256


def encode_kernel(
    tab_ref, blk_ref, slot_ref, cnt_ref, kin_ref, kmid_ref, kout_ref, wskip_ref,
    lat_ref, skip_ref, acc, pre, ids, rowblk, win, wmid, masked_a, masked_b, hid_a, hid_b,
):
    def iota(shape, dim):
        return lax.broadcasted_iota(jnp.int32, shape, dim)

    ids[...] = (iota((PTS, 128), 0) - 256).astype(F32).astype(BF16)
    rowblk[...] = (iota((256, 128), 0) // 9).astype(F32).astype(BF16)
    col = iota((6, 256), 1)
    nine = col % 9
    source = jnp.where(nine < 3, nine, nine - 3)
    chosen = jnp.where((source == iota((6, 256), 0)) & (col < 243), 1.0, 0.0).astype(BF16)
    win[...] = dot_first(kin_ref[...], chosen).astype(BF16)
    eye = jnp.where(iota((KH, KH), 0) == iota((KH, KH), 1), 0.5, 0.0).astype(BF16)
    wmid[...] = dot_first(kmid_ref[...], eye).astype(BF16)
    row, lane = iota((6, 128), 0), iota((6, 128), 1)
    index_y = lax.axis_index("gy") * 16 + lane // 8
    index_z = lax.axis_index("gz") * 8 + lane % 8
    for x in range(8):
        index = jnp.where(row == 0, lax.axis_index("gx") * 8 + x, jnp.where(row == 1, index_y, index_z))
        centre = jnp.where(row < 3, -(index.astype(F32) + 0.5) / GRID, 0.0).astype(BF16)
        pre[x] = dot_first(kin_ref[...], centre)
    acc[...] = jnp.zeros((8, KH, 128), F32)
    one = jnp.ones((PTS, 128), BF16)
    none = jnp.zeros((PTS, 128), BF16)

    def step(t, masked_out, masked_in, hid_out, hid_in):
        early = jnp.minimum(t, CHUNKS - 1)
        middle = jnp.clip(t - 1, 0, CHUNKS - 1)
        late = jnp.maximum(t - 2, 0)
        slots, blocks = slot_ref[early], blk_ref[early]
        base = jnp.concatenate([pre[middle // 4]] * 2, axis=1)
        valid = jnp.where(t >= 2, cnt_ref[late // 4], 0.0)
        first = (late % 4 * 8).astype(F32)
        total = jnp.zeros((KH, 128), F32)
        for part in range(4):
            span = pl.ds(part * PART, PART)
            hot = []
            for s in (2 * part, 2 * part + 1):
                chosen = jnp.broadcast_to(slots[s : s + 1], (PTS, 128)).astype(BF16)
                hot.append(jnp.where(ids[...] == chosen, one, none))
            found = dot(tab_ref[...], jnp.concatenate(hot, axis=1))
            ahead = dot(win[...], masked_in[:, span])
            last = dot(wmid[...], hid_in[:, span])
            hid_out[:, span] = twice_gelu(ahead + base).astype(BF16)
            last = twice_gelu(last).astype(BF16).astype(F32)
            for n in range(2):
                used = valid > first + (2 * part + n)
                total = total + jnp.where(used, last[:, n * 128 : (n + 1) * 128], 0.0)
            found = found.astype(BF16)
            for n in range(2):
                s = 2 * part + n
                chosen = jnp.broadcast_to(blocks[s : s + 1], (256, 128)).astype(BF16)
                masked_out[:, pl.ds(s * 128, 128)] = jnp.where(
                    rowblk[...] == chosen, found[:, n * 128 : (n + 1) * 128], none[0:256]
                )
        acc[late // 4] += total

    def two_steps(tt, carry):
        step(2 * tt, masked_a, masked_b, hid_a, hid_b)
        step(2 * tt + 1, masked_b, masked_a, hid_b, hid_a)
        return carry

    lax.fori_loop(0, CHUNKS // 2 + 1, two_steps, 0)
    for x in range(8):
        upper, lower = split_two(0.5 * acc[x])
        values = dot_first(kout_ref[...], upper) + dot_first(kout_ref[...], lower)
        latent = (values / cnt_ref[x]).astype(BF16)
        skip_ref[x] = dot_first(wskip_ref[...], latent)
        lat_ref[x] = latent.astype(F32)


def encode(tab, blk, slot, cnt, kin, kmid, kout, wskip):
    vmem = pl.BlockSpec(memory_space=pltpu.VMEM)
    v = pltpu.VMEM
    return pl.pallas_call(
        encode_kernel,
        out_shape=(
            jax.ShapeDtypeStruct((8, CH, 128), F32),
            jax.ShapeDtypeStruct((8, CH, 128), F32),
        ),
        in_specs=[vmem] * 8,
        out_specs=(vmem, vmem),
        scratch_shapes=[
            v((8, KH, 128), F32), v((8, KH, 128), F32),
            v((PTS, 128), BF16), v((256, 128), BF16), v((KH, 256), BF16), v((KH, KH), BF16),
            v((256, 1024), BF16), v((256, 1024), BF16), v((KH, 1024), BF16), v((KH, 1024), BF16),
        ],
        name="encode",
    )(tab, blk, slot, cnt, kin, kmid, kout, wskip)


@functools.cache
def transform_tables():
    m = np.arange(GRID)
    centred = np.where(np.arange(MODES) < MODES // 2, np.arange(MODES), np.arange(MODES) - MODES)
    third = np.arange(MODES)

    def angles(f):
        return 2.0 * np.pi * ((f[:, None] * m[None, :]) % GRID) / GRID

    cos_c, sin_c = np.cos(angles(centred)), np.sin(angles(centred))
    cos_t, sin_t = np.cos(angles(third)), np.sin(angles(third))
    eye_k = np.eye(4)
    both = np.stack([cos_t, -sin_t], axis=-1)
    fz = np.broadcast_to(
        both.reshape(4, 4, GRID, 2).transpose(2, 0, 1, 3)[:, :, None], (GRID, 4, 16, 4, 2)
    ).reshape(GRID, 512)
    turn = np.stack([np.stack([cos_c, -sin_c], -1), np.stack([sin_c, cos_c], -1)], -2)
    fy = np.einsum("jcpyro,kl->pykrjocl", turn.reshape(8, 2, NY, 16, 2, 2), eye_k).reshape(512, 128)
    first = np.stack([cos_c, sin_c]).reshape(2, 8, 2, NX, 8)
    fx = np.broadcast_to(
        first.transpose(3, 2, 1, 0, 4)[..., None], (NX, 2, 8, 2, 8, 8)
    ).reshape(NX, 16, 128)
    ix = np.broadcast_to(
        first.transpose(3, 4, 0, 2, 1)[..., None], (NX, 8, 2, 2, 8, 8)
    ).reshape(NX, 8, 256)
    back = np.stack([np.stack([cos_c, sin_c], -1), np.stack([-sin_c, cos_c], -1)], -2)
    iy = np.einsum("jcqyro,kl->jrckqylo", back.reshape(8, 2, NY, 16, 2, 2), eye_k).reshape(128, 512)
    weight = np.where(third == 0, 1.0, 2.0)[:, None, None] / GRID**3
    iz = np.broadcast_to(
        (both * weight).transpose(0, 2, 1).reshape(32, NZ, 1, 8), (32, NZ, 16, 8)
    ).reshape(32, 1024)
    return fz, fy, fx, ix, iy, iz


def two_tables(table):
    import ml_dtypes

    upper = table.astype(np.float32).astype(ml_dtypes.bfloat16)
    lower = (table - upper.astype(np.float64)).astype(np.float32).astype(ml_dtypes.bfloat16)
    return jnp.asarray(upper), jnp.asarray(lower)


def wide_table(table):
    return jnp.asarray(np.ascontiguousarray(table, dtype=np.float32))


def iota(shape, dim):
    return lax.broadcasted_iota(jnp.int32, shape, dim)


def block_swap(x):
    row, lane = iota(x.shape, 0), iota(x.shape, 1) // 16
    for bit in (1, 2, 4):
        high, right = (row & bit) != 0, (lane & bit) != 0
        down = pltpu.roll(pltpu.roll(x, bit, axis=0), 128 - 16 * bit, axis=1)
        up = pltpu.roll(pltpu.roll(x, x.shape[0] - bit, axis=0), 16 * bit, axis=1)
        x = jnp.where(high == right, x, jnp.where(high, down, up))
    return x


def layer_kernel(
    lat_ref, skip_ref, w_ref, fzc_ref, fyh_ref, fyl_ref, fxc_ref, ixc_ref, iyh_ref, iyl_ref,
    izc_ref, out_ref,
    s1, r1, s2, r2, s4, r4, s5, r5, s7, r7, sv, rv, s8, r8, fzh, fzl, iz, grid, wide,
    send_sem, recv_sem,
):
    gx, gy, gz = lax.axis_index("gx"), lax.axis_index("gy"), lax.axis_index("gz")
    me = gz * NX + gx
    barrier = pltpu.get_barrier_semaphore()

    def along_y(d):
        return (gx, lax.rem(gy + d, NY), gz)

    def along_z(d):
        return (gx, gy, lax.rem(gz + d, NZ))

    plane = [
        (lax.rem(gx + dx, NX), gy, lax.rem(gz + dz, NZ))
        for dx in range(NX)
        for dz in range(NZ)
        if (dx, dz) != (0, 0)
    ]
    peers = plane + [along_y(d) for d in range(1, NY)]
    for peer in peers:
        pl.semaphore_signal(barrier, inc=1, device_id=peer, device_id_type=MESH_ID)
    for q in range(NZ):
        s1[q] = lat_ref[:, pl.ds(8 * q, 8), :].reshape(64, 128).astype(BF16)
    own_y = iota((128, 512), 0) // 8 == iota((128, 512), 1) % 128 // 8
    for q in range(NZ):
        part = jnp.concatenate([fzc_ref[pl.ds(8 * q, 8), :]] * 16, axis=0)
        upper, lower = split_two(jnp.where(own_y, part, 0.0))
        fzh[pl.ds(128 * q, 128), :] = upper
        fzl[pl.ds(128 * q, 128), :] = lower
    own_y = iota((128, 1024), 0) // 8 == iota((128, 1024), 1) % 128 // 8
    for q in range(NY):
        part = jnp.concatenate([izc_ref[pl.ds(8 * q, 8), :]] * 16, axis=0)
        iz[pl.ds(128 * q, 128), :] = jnp.where(own_y, part, 0.0).astype(BF16)
    part = jnp.concatenate(
        [jnp.broadcast_to(fxc_ref[gx, pl.ds(n, 1), :], (8, 128)) for n in range(16)], axis=0
    )
    row, lane = iota((128, 128), 0), iota((128, 128), 1)
    fxh, fxl = split_two(jnp.where(row % 8 == lane % 8, part, 0.0))
    part = jnp.concatenate(
        [jnp.broadcast_to(ixc_ref[gx, pl.ds(n, 1), :], (8, 256)) for n in range(8)], axis=0
    )
    ixh, ixl = split_two(jnp.where(iota((64, 256), 0) % 8 == iota((64, 256), 1) % 8, part, 0.0))
    row_i, lane_i = row // 8 % 8 * 2 + row // 64, lane // 8 % 8 * 2 + lane // 64
    mirror = (row % 8 == lane % 8) & (row_i != 8) & (lane_i == (16 - row_i) % 16)
    mirror = jnp.where(mirror, 1.0, 0.0).astype(BF16)
    row_j, lane_j = row // 16 * 2 + row // 4 % 2, lane // 16 * 2 + lane // 4 % 2
    flip = (row % 4 == 0) & (lane % 4 == 0) & (row // 8 % 2 == lane // 8 % 2)
    flip = flip & (lane_j != 8) & (row_j == (16 - lane_j) % 16)
    flip = jnp.where(flip, jnp.where(lane // 8 % 2 == 0, 1.0, -1.0), 0.0).astype(BF16)
    pick = jnp.where(iota((16, 128), 1) % 16 == iota((16, 128), 0), 1.0, 0.0).astype(BF16)
    gather = jnp.where(iota((8, 64), 1) // 8 == iota((8, 64), 0), 1.0, 0.0).astype(BF16)
    own_channel = iota((64, 128), 0) % 8 == iota((64, 128), 1) // 16
    own_mode = iota((32, 1024), 1) // CH == iota((32, 1024), 0) % MODES
    pl.semaphore_wait(barrier, len(peers))

    def send(n, source, target, peer):
        pltpu.make_async_remote_copy(
            src_ref=source,
            dst_ref=target,
            send_sem=send_sem.at[n],
            recv_sem=recv_sem.at[n],
            device_id=peer,
            device_id_type=MESH_ID,
        ).start()

    def arrived(n, buffer, count):
        part = buffer.at[pl.ds(0, count)]
        pltpu.make_async_copy(part, part, recv_sem.at[n]).wait()

    def left(n, buffer, count):
        part = buffer.at[pl.ds(0, count)]
        pltpu.make_async_copy(part, part, send_sem.at[n]).wait()

    for d in range(1, NZ):
        peer = along_z(d)
        send(0, s1.at[peer[2]], r1.at[gz], peer)
    r1[gz] = s1[gz]
    arrived(0, r1, NZ - 1)
    line = jnp.concatenate([r1[q] for q in range(NZ)], axis=1)
    deep = dot(line, fzh[...]) + dot(line, fzl[...])
    for q in range(NY):
        s2[q] = deep[:, q * 128 : (q + 1) * 128]
    for d in range(1, NY):
        peer = along_y(d)
        send(1, s2.at[peer[1]], r2.at[gy], peer)
    r2[gy] = s2[gy]
    arrived(1, r2, NY - 1)
    upper, lower = split_two(jnp.concatenate([r2[q] for q in range(NY)], axis=1))
    flat = dot(upper, fyh_ref[...]) + dot(upper, fyl_ref[...]) + dot(lower, fyh_ref[...])
    real = iota((64, 128), 1) // 8 % 2 == 0
    turned = jnp.where(real, pltpu.roll(flat, 120, axis=1), -pltpu.roll(flat, 8, axis=1))
    upper, lower = split_two(jnp.concatenate([flat, turned], axis=0))
    share = block_swap(dot(fxh, upper) + dot(fxl, upper) + dot(fxh, lower))
    for i in range(2):
        s4[:, i, :] = share[64 * i : 64 * i + 64]
    for peer in plane:
        send(2, s4.at[peer[2] * NX + peer[0]], r4.at[me], peer)
    r4[me] = s4[me]
    arrived(2, r4, 63)
    for q in range(NZ):
        pair = r4[q * NX]
        for n in range(1, NX):
            pair = pair + r4[q * NX + n]
        grid[pl.ds(2 * q, 2), :] = pair
    found = []
    for i in range(2):
        values = jnp.concatenate(
            [jnp.broadcast_to(grid[pl.ds(2 * q + i, 1), :], (8, 128)) for q in range(NZ)], axis=0
        )
        values = jnp.where(own_channel, values, 0.0).astype(BF16)
        found.append(
            lax.dot_general(
                pick,
                jnp.concatenate([values, values], axis=0),
                (((1,), (1,)), ((), ())),
                preferred_element_type=F32,
            )
        )
    rows = jnp.concatenate(
        [found[0][0:8], found[1][0:8], found[0][8:16], found[1][8:16]], axis=0
    )
    spread = jnp.where(own_mode, jnp.concatenate([rows] * 8, axis=1), 0.0).astype(BF16)
    by_real, by_imag = dot(spread, w_ref[0:1024]), dot(spread, w_ref[1024:2048])
    mixed_real = by_real[0:16] - by_imag[16:32]
    mixed_imag = by_imag[0:16] + by_real[16:32]
    for i in range(2):
        mine = jnp.concatenate(
            [mixed_real[8 * i : 8 * i + 8], mixed_imag[8 * i : 8 * i + 8]], axis=0
        ).astype(BF16)
        placed = jnp.where(own_channel, dot_first(mine, pick), 0.0).astype(BF16)
        s5[:, i, :] = dot(gather, placed)
    for peer in plane:
        send(3, s5.at[peer[2]], r5.at[me], peer)
    r5[me] = s5[gz]
    arrived(3, r5, 63)
    values = block_swap(jnp.concatenate([r5[:, i, :] for i in range(2)], axis=0))
    is_mean = (row < 8) & ((lane == 0) | (lane == 8)) & (gy == 0)
    values = jnp.where(is_mean, 0.0, values)
    exact = values.astype(BF16)
    real = lane // 8 % 2 == 0
    turned = jnp.where(real, -pltpu.roll(values, 120, axis=1), pltpu.roll(values, 8, axis=1))
    stacked = jnp.concatenate([exact, turned.astype(BF16)], axis=0)
    plain = (dot(ixh, stacked) + dot(ixl, stacked)).astype(BF16)
    flat = dot(plain, iyh_ref[...]) + dot(plain, iyl_ref[...])
    for q in range(NY):
        s7[q] = flat[:, q * 128 : (q + 1) * 128].astype(BF16)
    for d in range(1, NY):
        peer = along_y(d)
        send(4, s7.at[peer[1]], r7.at[gy], peer)
    r7[gy] = s7[gy]
    weight = jnp.where((lane % 4 == 0) & (gy == 0), 0.5, 2.0)
    pairs = dot(dot(mirror, exact).astype(BF16), flip)
    pairs = jnp.where(gy == 0, 0.5 * pairs, 0.0)
    power = jnp.sum(values * (weight * values + pairs), axis=1, keepdims=True)
    power = jnp.sum(power.reshape(16, 8, 1), axis=0)
    sv[...] = jnp.broadcast_to(power, (8, 128))
    for d in range(1, NY):
        send(5, sv, rv.at[gy], along_y(d))
    rv[gy] = sv[...]
    arrived(4, r7, NY - 1)
    line = jnp.concatenate([r7[q] for q in range(NY)], axis=1)
    depth = dot(line, iz[...])
    arrived(5, rv, NY - 1)
    power = (rv[0] + rv[1]) + (rv[2] + rv[3])
    scale = 1.0 / jnp.sqrt(power * (1.0 / float(GRID) ** 6) + 1.0)
    scale = jnp.concatenate([scale] * 8, axis=0)
    for q in range(NZ):
        s8[q] = (depth[:, q * 128 : (q + 1) * 128] * scale).astype(BF16)
    for d in range(1, NZ):
        peer = along_z(d)
        send(6, s8.at[peer[2]], r8.at[gz], peer)
    r8[gz] = s8[gz]
    arrived(6, r8, NZ - 1)
    wide[...] = r8[...].astype(F32)
    for x in range(8):
        out_ref[x] = gelu(wide[:, pl.ds(8 * x, 8), :].reshape(CH, 128) + skip_ref[x]).T
    left(0, r1, NZ - 1)
    left(1, r2, NY - 1)
    left(2, r4, 63)
    left(3, r5, 63)
    left(4, r7, NY - 1)
    left(5, rv, NY - 1)
    left(6, r8, NZ - 1)


def layer(lat, skip, weights):
    fz, fy, fx, ix, iy, iz = transform_tables()
    tables = [wide_table(fz), *two_tables(fy), wide_table(fx), wide_table(ix)]
    tables += [*two_tables(iy), wide_table(iz)]
    vmem = pl.BlockSpec(memory_space=pltpu.VMEM)
    v = pltpu.VMEM
    return pl.pallas_call(
        layer_kernel,
        out_shape=jax.ShapeDtypeStruct((8, 128, CH), F32),
        in_specs=[vmem] * (3 + len(tables)),
        out_specs=vmem,
        scratch_shapes=[
            v((NZ, 64, 128), BF16), v((NZ, 64, 128), BF16),
            v((NY, 64, 128), F32), v((NY, 64, 128), F32),
            v((CH, 2, 128), F32), v((CH, 2, 128), F32),
            v((NZ, 2, 128), F32), v((CH, 2, 128), F32),
            v((NY, 64, 128), BF16), v((NY, 64, 128), BF16),
            v((8, 128), F32), v((NY, 8, 128), F32),
            v((NZ, 64, 128), BF16), v((NZ, 64, 128), BF16),
            v((1024, 512), BF16), v((1024, 512), BF16), v((512, 1024), BF16),
            v((MODES, 128), F32), v((NZ, 64, 128), F32),
            pltpu.SemaphoreType.DMA((7,)), pltpu.SemaphoreType.DMA((7,)),
        ],
        compiler_params=pltpu.CompilerParams(collective_id=1, has_side_effects=True),
        name="layer",
    )(lat, skip, weights, *tables)


def body(point_data, neighbours, counts, kernel_in, kernel_mid, kernel_out, spectral, skip_weight):
    place = [lax.axis_index(a) for a in ("gx", "gy", "gz")]
    tab = halo_table(point_data[0])
    near = jnp.swapaxes(neighbours.reshape(8, 128, NB), 1, 2)
    owner = near // PTS
    offset_z = owner % NZ - place[2] + 1
    offset_y = owner // NZ % NY - place[1] + 1
    offset_x = owner // (NZ * NY) - place[0] + 1
    blk = ((offset_x * 3 + offset_y) * 3 + offset_z).astype(F32).reshape(CHUNKS, 8, 128)
    slot = (near % PTS - 256).astype(F32).reshape(CHUNKS, 8, 128)
    cnt = counts.reshape(8, 1, 128).astype(F32)
    lat, skip = encode(
        tab, blk, slot, cnt, kernel_in, kernel_mid, kernel_out, skip_weight
    )
    out = layer(lat, skip, spectral.reshape(2048, CH))
    return out.reshape(1, 8, 16, 8, CH)


def solution(mesh):
    cells = P(None, "gx", "gy", "gz", None)
    return jax.shard_map(
        body,
        mesh=mesh,
        in_specs=(
            P(None, None, ("gx", "gy", "gz")),
            cells,
            P(None, "gx", "gy", "gz"),
            P(),
            P(),
            P(),
            P(None, "gz", "gx", "gy", None, None),
            P(),
        ),
        out_specs=cells,
        check_vma=False,
    )
```

```python
import functools
import math

import jax
import jax.numpy as jnp
import numpy as np
from jax import lax
from jax.experimental import pallas as pl
from jax.experimental.pallas import tpu as pltpu
from jax.sharding import PartitionSpec as P

GRID = 64
MODES = 16
NB = 32
KH = 80
CH = 64
PTS = 512
NX, NY, NZ = 8, 4, 8
F32 = jnp.float32
BF16 = jnp.bfloat16
MESH_ID = pl.DeviceIdType.MESH


def dot(a, b):
    return jnp.dot(a, b, preferred_element_type=F32)


def gelu(v):
    inner = v * (0.7978845608028654 + 0.035677408136300125 * (v * v))
    half = 0.5 * v
    return half + half * jnp.tanh(inner)


def split_two(values):
    upper = values.astype(BF16)
    return upper, (values - upper.astype(F32)).astype(BF16)


def dot_first(a, b):
    return lax.dot_general(a, b, (((0,), (0,)), ((), ())), preferred_element_type=F32)


def twice_gelu(v):
    inner = v * (0.7978845608028654 + 0.035677408136300125 * (v * v))
    return v + v * jnp.tanh(inner)


CHUNKS = 32
PART = 256


@functools.cache
def transform_tables():
    m = np.arange(GRID)
    centred = np.where(np.arange(MODES) < MODES // 2, np.arange(MODES), np.arange(MODES) - MODES)
    third = np.arange(MODES)

    def angles(f):
        return 2.0 * np.pi * ((f[:, None] * m[None, :]) % GRID) / GRID

    cos_c, sin_c = np.cos(angles(centred)), np.sin(angles(centred))
    cos_t, sin_t = np.cos(angles(third)), np.sin(angles(third))
    eye_k = np.eye(4)
    both = np.stack([cos_t, -sin_t], axis=-1)
    fz = np.broadcast_to(
        both.reshape(4, 4, GRID, 2).transpose(2, 0, 1, 3)[:, :, None], (GRID, 4, 16, 4, 2)
    ).reshape(GRID, 512)
    turn = np.stack([np.stack([cos_c, -sin_c], -1), np.stack([sin_c, cos_c], -1)], -2)
    fy = np.einsum("jcpyro,kl->pykrjocl", turn.reshape(8, 2, NY, 16, 2, 2), eye_k).reshape(512, 128)
    first = np.stack([cos_c, sin_c]).reshape(2, 8, 2, NX, 8)
    fx = np.broadcast_to(
        first.transpose(3, 2, 1, 0, 4)[..., None], (NX, 2, 8, 2, 8, 8)
    ).reshape(NX, 16, 128)
    ix = np.broadcast_to(
        first.transpose(3, 4, 0, 2, 1)[..., None], (NX, 8, 2, 2, 8, 8)
    ).reshape(NX, 8, 256)
    back = np.stack([np.stack([cos_c, sin_c], -1), np.stack([-sin_c, cos_c], -1)], -2)
    iy = np.einsum("jcqyro,kl->jrckqylo", back.reshape(8, 2, NY, 16, 2, 2), eye_k).reshape(128, 512)
    weight = np.where(third == 0, 1.0, 2.0)[:, None, None] / GRID**3
    iz = np.broadcast_to(
        (both * weight).transpose(0, 2, 1).reshape(32, NZ, 1, 8), (32, NZ, 16, 8)
    ).reshape(32, 1024)
    return fz, fy, fx, ix, iy, iz


def two_tables(table):
    import ml_dtypes

    upper = table.astype(np.float32).astype(ml_dtypes.bfloat16)
    lower = (table - upper.astype(np.float64)).astype(np.float32).astype(ml_dtypes.bfloat16)
    return jnp.asarray(upper), jnp.asarray(lower)


def wide_table(table):
    return jnp.asarray(np.ascontiguousarray(table, dtype=np.float32))


def iota(shape, dim):
    return lax.broadcasted_iota(jnp.int32, shape, dim)


def block_swap(x):
    row, lane = iota(x.shape, 0), iota(x.shape, 1) // 16
    for bit in (1, 2, 4):
        high, right = (row & bit) != 0, (lane & bit) != 0
        down = pltpu.roll(pltpu.roll(x, bit, axis=0), 128 - 16 * bit, axis=1)
        up = pltpu.roll(pltpu.roll(x, x.shape[0] - bit, axis=0), 16 * bit, axis=1)
        x = jnp.where(high == right, x, jnp.where(high, down, up))
    return x


def whole_kernel(
    pts_ref, cnt_ref, kin_ref, kmid_ref, kout_ref, wskip_ref,
    near_hbm, w_hbm, fzc_hbm, fyh_hbm, fyl_hbm, fxc_hbm, ixc_hbm, iyh_hbm, iyl_hbm, izc_hbm,
    out_ref,
    near, w_ref, fzc_ref, fyh_ref, fyl_ref, fxc_ref, ixc_ref, iyh_ref, iyl_ref, izc_ref,
    around, table_rows, tab, slot_ids, block_ids, valid_slots, pre, ids, rowblk, win, wmid,
    masked_a, masked_b, hid_a, hid_b, acc, lat_ref, skip_ref, fxh, fxl, ixh, ixl,
    s1, r1, s2, r2, s4, r4, s5, r5, s7, r7, sv, rv, s8, r8, fzh, fzl, iz, grid, wide,
    send_sem, recv_sem, in_sem,
):
    gx, gy, gz = lax.axis_index("gx"), lax.axis_index("gy"), lax.axis_index("gz")
    me = gz * NX + gx
    barrier = pltpu.get_barrier_semaphore()
    fetched = [
        (near_hbm, near), (fzc_hbm, fzc_ref), (fxc_hbm.at[gx], fxc_ref), (ixc_hbm.at[gx], ixc_ref),
        (izc_hbm, izc_ref), (fyh_hbm, fyh_ref), (fyl_hbm, fyl_ref), (iyh_hbm, iyh_ref),
        (iyl_hbm, iyl_ref), (w_hbm, w_ref),
    ]

    def fetch(n):
        return pltpu.make_async_copy(fetched[n][0], fetched[n][1], in_sem.at[n])

    for n in range(len(fetched)):
        fetch(n).start()

    def along_y(d):
        return (gx, lax.rem(gy + d, NY), gz)

    def along_z(d):
        return (gx, gy, lax.rem(gz + d, NZ))

    def beside(step):
        return tuple(lax.rem(p + d + n, n) for p, d, n in zip((gx, gy, gz), step, (NX, NY, NZ)))

    plane = [
        (lax.rem(gx + dx, NX), gy, lax.rem(gz + dz, NZ))
        for dx in range(NX)
        for dz in range(NZ)
        if (dx, dz) != (0, 0)
    ]
    steps = [
        (dx, dy, dz)
        for dx in (-1, 0, 1)
        for dy in (-1, 0, 1)
        for dz in (-1, 0, 1)
        if (dx, dy, dz) != (0, 0, 0)
    ]
    apart = [beside(s) for s in steps if s[1] != 0 and (s[0], s[2]) != (0, 0)]
    peers = plane + [along_y(d) for d in range(1, NY)] + apart
    for peer in peers:
        pl.semaphore_signal(barrier, inc=1, device_id=peer, device_id_type=MESH_ID)

    ids[...] = (iota((PTS, 128), 0) - 256).astype(F32).astype(BF16)
    rowblk[...] = (iota((256, 128), 0) // 9).astype(F32).astype(BF16)
    col = iota((6, 256), 1)
    nine = col % 9
    source = jnp.where(nine < 3, nine, nine - 3)
    chosen = jnp.where((source == iota((6, 256), 0)) & (col < 243), 1.0, 0.0).astype(BF16)
    win[...] = dot_first(kin_ref[...], chosen).astype(BF16)
    eye = jnp.where(iota((KH, KH), 0) == iota((KH, KH), 1), 0.5, 0.0).astype(BF16)
    wmid[...] = dot_first(kmid_ref[...], eye).astype(BF16)
    row, lane = iota((6, 128), 0), iota((6, 128), 1)
    index_y, index_z = gy * 16 + lane // 8, gz * 8 + lane % 8
    for x in range(8):
        index = jnp.where(row == 0, gx * 8 + x, jnp.where(row == 1, index_y, index_z))
        centre = jnp.where(row < 3, -(index.astype(F32) + 0.5) / GRID, 0.0).astype(BF16)
        pre[x] = dot_first(kin_ref[...], centre)
    by_row = jnp.where(iota((16, 128), 1) // 8 == iota((16, 128), 0), 1.0, 0.0).astype(BF16)
    spread = dot(cnt_ref[...].astype(F32).astype(BF16), by_row)
    spread = jnp.where(iota((64, 128), 0) % 8 == iota((64, 128), 1) % 8, spread, 0.0)
    gather = jnp.where(iota((8, 64), 1) // 8 == iota((8, 64), 0), 1.0, 0.0).astype(BF16)
    spread = dot(gather, spread.astype(BF16))
    for x in range(8):
        valid_slots[x] = jnp.broadcast_to(spread[x : x + 1], (8, 128))
    acc[...] = jnp.zeros((8, KH, 128), F32)
    table_rows[pl.ds(240, 16), :] = jnp.zeros((16, PTS), F32)
    fetch(0).wait()
    for x in range(8):
        point = near[x].T
        owner = point >> 9
        offset_z = (owner & 7) - gz + 1
        offset_y = ((owner >> 3) & 3) - gy + 1
        offset_x = (owner >> 5) - gx + 1
        block = ((offset_x * 3 + offset_y) * 3 + offset_z).astype(F32)
        block_ids[pl.ds(4 * x, 4)] = block.reshape(4, 8, 128)
        slot_ids[pl.ds(4 * x, 4)] = ((point & 511) - 256).astype(F32).reshape(4, 8, 128)
    pl.semaphore_wait(barrier, len(peers))

    def send(n, source, target, peer):
        pltpu.make_async_remote_copy(
            src_ref=source,
            dst_ref=target,
            send_sem=send_sem.at[n],
            recv_sem=recv_sem.at[n],
            device_id=peer,
            device_id_type=MESH_ID,
        ).start()

    def arrived(n, buffer, count):
        part = buffer.at[pl.ds(0, count)]
        pltpu.make_async_copy(part, part, recv_sem.at[n]).wait()

    def left(n, buffer, count):
        part = buffer.at[pl.ds(0, count)]
        pltpu.make_async_copy(part, part, send_sem.at[n]).wait()

    for step in steps:
        block = ((1 - step[0]) * 3 + (1 - step[1])) * 3 + (1 - step[2])
        send(7, pts_ref, around.at[block], beside(step))
    around[13] = pts_ref[...]
    for n in range(1, 5):
        fetch(n).wait()
    own_y = iota((128, 512), 0) // 8 == iota((128, 512), 1) % 128 // 8
    for q in range(NZ):
        part = jnp.concatenate([fzc_ref[pl.ds(8 * q, 8), :]] * 16, axis=0)
        upper, lower = split_two(jnp.where(own_y, part, 0.0))
        fzh[pl.ds(128 * q, 128), :] = upper
        fzl[pl.ds(128 * q, 128), :] = lower
    own_y = iota((128, 1024), 0) // 8 == iota((128, 1024), 1) % 128 // 8
    for q in range(NY):
        part = jnp.concatenate([izc_ref[pl.ds(8 * q, 8), :]] * 16, axis=0)
        iz[pl.ds(128 * q, 128), :] = jnp.where(own_y, part, 0.0).astype(BF16)
    part = jnp.concatenate(
        [jnp.broadcast_to(fxc_ref[pl.ds(n, 1), :], (8, 128)) for n in range(16)], axis=0
    )
    row, lane = iota((128, 128), 0), iota((128, 128), 1)
    fxh[...], fxl[...] = split_two(jnp.where(row % 8 == lane % 8, part, 0.0))
    part = jnp.concatenate(
        [jnp.broadcast_to(ixc_ref[pl.ds(n, 1), :], (8, 256)) for n in range(8)], axis=0
    )
    ixh[...], ixl[...] = split_two(jnp.where(iota((64, 256), 0) % 8 == iota((64, 256), 1) % 8, part, 0.0))
    arrived(7, around, 26)
    for b in range(27):
        for t in range(4):
            block = around[b, pl.ds(t, 6, stride=4), :]
            place = block[0:3]
            upper = place.astype(BF16).astype(F32)
            table_rows[pl.ds(9 * b, 9), pl.ds(128 * t, 128)] = jnp.concatenate(
                [upper, place - upper, block[3:6]], axis=0
            )
    tab[...] = table_rows[...].astype(BF16)
    one = jnp.ones((PTS, 128), BF16)
    none = jnp.zeros((PTS, 128), BF16)

    def step(t, masked_out, masked_in, hid_out, hid_in):
        early = jnp.minimum(t, CHUNKS - 1)
        middle = jnp.clip(t - 1, 0, CHUNKS - 1)
        late = jnp.maximum(t - 2, 0)
        slots, blocks = slot_ids[early], block_ids[early]
        base = jnp.concatenate([pre[middle // 4]] * 2, axis=1)
        valid = jnp.where(t >= 2, valid_slots[late // 4], 0.0)[0:1]
        first = (late % 4 * 8).astype(F32)
        total = jnp.zeros((KH, 128), F32)
        for part in range(4):
            span = pl.ds(part * PART, PART)
            hot = []
            for s in (2 * part, 2 * part + 1):
                chosen = jnp.broadcast_to(slots[s : s + 1], (PTS, 128)).astype(BF16)
                hot.append(jnp.where(ids[...] == chosen, one, none))
            found = dot(tab[...], jnp.concatenate(hot, axis=1))
            ahead = dot(win[...], masked_in[:, span])
            last = dot(wmid[...], hid_in[:, span])
            hid_out[:, span] = twice_gelu(ahead + base).astype(BF16)
            last = twice_gelu(last).astype(BF16).astype(F32)
            for n in range(2):
                used = valid > first + (2 * part + n)
                total = total + jnp.where(used, last[:, n * 128 : (n + 1) * 128], 0.0)
            found = found.astype(BF16)
            for n in range(2):
                s = 2 * part + n
                chosen = jnp.broadcast_to(blocks[s : s + 1], (256, 128)).astype(BF16)
                masked_out[:, pl.ds(s * 128, 128)] = jnp.where(
                    rowblk[...] == chosen, found[:, n * 128 : (n + 1) * 128], none[0:256]
                )
        acc[late // 4] += total

    for unset in (masked_a, masked_b):
        unset[...] = jnp.zeros((256, 1024), BF16)
    for unset in (hid_a, hid_b):
        unset[...] = jnp.zeros((KH, 1024), BF16)

    def two_steps(tt, carry):
        step(2 * tt, masked_a, masked_b, hid_a, hid_b)
        step(2 * tt + 1, masked_b, masked_a, hid_b, hid_a)
        return carry

    lax.fori_loop(0, CHUNKS // 2 + 1, two_steps, 0)
    for x in range(8):
        upper, lower = split_two(0.5 * acc[x])
        values = dot(kout_ref[...], upper) + dot(kout_ref[...], lower)
        latent = (values / valid_slots[x, 0:1]).astype(BF16)
        skip_ref[x] = dot_first(wskip_ref[...], latent)
        lat_ref[x] = latent.astype(F32)
    for q in range(NZ):
        s1[q] = lat_ref[:, pl.ds(8 * q, 8), :].reshape(64, 128).astype(BF16)
    for d in range(1, NZ):
        peer = along_z(d)
        send(0, s1.at[peer[2]], r1.at[gz], peer)
    r1[gz] = s1[gz]
    row, lane = iota((128, 128), 0), iota((128, 128), 1)
    row_i, lane_i = row // 8 % 8 * 2 + row // 64, lane // 8 % 8 * 2 + lane // 64
    mirror = (row % 8 == lane % 8) & (row_i != 8) & (lane_i == (16 - row_i) % 16)
    mirror = jnp.where(mirror, 1.0, 0.0).astype(BF16)
    row_j, lane_j = row // 16 * 2 + row // 4 % 2, lane // 16 * 2 + lane // 4 % 2
    flip = (row % 4 == 0) & (lane % 4 == 0) & (row // 8 % 2 == lane // 8 % 2)
    flip = flip & (lane_j != 8) & (row_j == (16 - lane_j) % 16)
    flip = jnp.where(flip, jnp.where(lane // 8 % 2 == 0, 1.0, -1.0), 0.0).astype(BF16)
    pick = jnp.where(iota((16, 128), 1) % 16 == iota((16, 128), 0), 1.0, 0.0).astype(BF16)
    own_channel = iota((64, 128), 0) % 8 == iota((64, 128), 1) // 16
    own_mode = iota((32, 1024), 1) // CH == iota((32, 1024), 0) % MODES
    for n in range(5, 10):
        fetch(n).wait()
    arrived(0, r1, NZ - 1)
    line = jnp.concatenate([r1[q] for q in range(NZ)], axis=1)
    deep = dot(line, fzh[...]) + dot(line, fzl[...])
    for q in range(NY):
        s2[q] = deep[:, q * 128 : (q + 1) * 128]
    for d in range(1, NY):
        peer = along_y(d)
        send(1, s2.at[peer[1]], r2.at[gy], peer)
    r2[gy] = s2[gy]
    arrived(1, r2, NY - 1)
    upper, lower = split_two(jnp.concatenate([r2[q] for q in range(NY)], axis=1))
    flat = dot(upper, fyh_ref[...]) + dot(upper, fyl_ref[...]) + dot(lower, fyh_ref[...])
    real = iota((64, 128), 1) // 8 % 2 == 0
    turned = jnp.where(real, pltpu.roll(flat, 120, axis=1), -pltpu.roll(flat, 8, axis=1))
    upper, lower = split_two(jnp.concatenate([flat, turned], axis=0))
    share = block_swap(dot(fxh[...], upper) + dot(fxl[...], upper) + dot(fxh[...], lower))
    for i in range(2):
        s4[:, i, :] = share[64 * i : 64 * i + 64]
    for peer in plane:
        send(2, s4.at[peer[2] * NX + peer[0]], r4.at[me], peer)
    r4[me] = s4[me]
    arrived(2, r4, 63)
    for q in range(NZ):
        pair = r4[q * NX]
        for n in range(1, NX):
            pair = pair + r4[q * NX + n]
        grid[pl.ds(2 * q, 2), :] = pair
    found = []
    for i in range(2):
        values = jnp.concatenate(
            [jnp.broadcast_to(grid[pl.ds(2 * q + i, 1), :], (8, 128)) for q in range(NZ)], axis=0
        )
        values = jnp.where(own_channel, values, 0.0).astype(BF16)
        found.append(
            lax.dot_general(
                pick,
                jnp.concatenate([values, values], axis=0),
                (((1,), (1,)), ((), ())),
                preferred_element_type=F32,
            )
        )
    rows = jnp.concatenate(
        [found[0][0:8], found[1][0:8], found[0][8:16], found[1][8:16]], axis=0
    )
    spread = jnp.where(own_mode, jnp.concatenate([rows] * 8, axis=1), 0.0).astype(BF16)
    by_real, by_imag = dot(spread, w_ref[0:1024]), dot(spread, w_ref[1024:2048])
    mixed_real = by_real[0:16] - by_imag[16:32]
    mixed_imag = by_imag[0:16] + by_real[16:32]
    for i in range(2):
        mine = jnp.concatenate(
            [mixed_real[8 * i : 8 * i + 8], mixed_imag[8 * i : 8 * i + 8]], axis=0
        ).astype(BF16)
        placed = jnp.where(own_channel, dot_first(mine, pick), 0.0).astype(BF16)
        s5[:, i, :] = dot(gather, placed)
    for peer in plane:
        send(3, s5.at[peer[2]], r5.at[me], peer)
    r5[me] = s5[gz]
    arrived(3, r5, 63)
    values = block_swap(jnp.concatenate([r5[:, i, :] for i in range(2)], axis=0))
    is_mean = (row < 8) & ((lane == 0) | (lane == 8)) & (gy == 0)
    values = jnp.where(is_mean, 0.0, values)
    exact = values.astype(BF16)
    real = lane // 8 % 2 == 0
    turned = jnp.where(real, -pltpu.roll(values, 120, axis=1), pltpu.roll(values, 8, axis=1))
    stacked = jnp.concatenate([exact, turned.astype(BF16)], axis=0)
    plain = (dot(ixh[...], stacked) + dot(ixl[...], stacked)).astype(BF16)
    flat = dot(plain, iyh_ref[...]) + dot(plain, iyl_ref[...])
    for q in range(NY):
        s7[q] = flat[:, q * 128 : (q + 1) * 128].astype(BF16)
    for d in range(1, NY):
        peer = along_y(d)
        send(4, s7.at[peer[1]], r7.at[gy], peer)
    r7[gy] = s7[gy]
    weight = jnp.where((lane % 4 == 0) & (gy == 0), 0.5, 2.0)
    pairs = dot(dot(mirror, exact).astype(BF16), flip)
    pairs = jnp.where(gy == 0, 0.5 * pairs, 0.0)
    power = jnp.sum(values * (weight * values + pairs), axis=1, keepdims=True)
    power = jnp.sum(power.reshape(16, 8, 1), axis=0)
    sv[...] = jnp.broadcast_to(power, (8, 128))
    for d in range(1, NY):
        send(5, sv, rv.at[gy], along_y(d))
    rv[gy] = sv[...]
    arrived(4, r7, NY - 1)
    line = jnp.concatenate([r7[q] for q in range(NY)], axis=1)
    depth = dot(line, iz[...])
    arrived(5, rv, NY - 1)
    power = (rv[0] + rv[1]) + (rv[2] + rv[3])
    scale = 1.0 / jnp.sqrt(power * (1.0 / float(GRID) ** 6) + 1.0)
    scale = jnp.concatenate([scale] * 8, axis=0)
    for q in range(NZ):
        s8[q] = (depth[:, q * 128 : (q + 1) * 128] * scale).astype(BF16)
    for d in range(1, NZ):
        peer = along_z(d)
        send(6, s8.at[peer[2]], r8.at[gz], peer)
    r8[gz] = s8[gz]
    arrived(6, r8, NZ - 1)
    wide[...] = r8[...].astype(F32)
    for x in range(8):
        out_ref[x] = gelu(wide[:, pl.ds(8 * x, 8), :].reshape(CH, 128) + skip_ref[x]).T
    left(0, r1, NZ - 1)
    left(1, r2, NY - 1)
    left(2, r4, 63)
    left(3, r5, 63)
    left(4, r7, NY - 1)
    left(5, rv, NY - 1)
    left(6, r8, NZ - 1)
    left(7, around, 26)


def whole(points, counts, kin, kmid, kout, wskip, near, weights):
    fz, fy, fx, ix, iy, iz = transform_tables()
    tables = [wide_table(fz), *two_tables(fy), wide_table(fx), wide_table(ix)]
    tables += [*two_tables(iy), wide_table(iz)]
    vmem, anywhere = (pl.BlockSpec(memory_space=m) for m in (pltpu.VMEM, pl.ANY))
    v = pltpu.VMEM
    return pl.pallas_call(
        whole_kernel,
        out_shape=jax.ShapeDtypeStruct((8, 128, CH), F32),
        in_specs=[vmem] * 6 + [anywhere] * (2 + len(tables)),
        out_specs=vmem,
        scratch_shapes=[
            v((8, 128, NB), jnp.int32), v((2048, CH), BF16),
            v((GRID, 512), F32), v((512, 128), BF16), v((512, 128), BF16),
            v((16, 128), F32), v((8, 256), F32), v((128, 512), BF16), v((128, 512), BF16),
            v((32, 1024), F32),
            v((27, 24, 128), F32), v((256, PTS), F32), v((256, PTS), BF16),
            v((CHUNKS, 8, 128), F32), v((CHUNKS, 8, 128), F32), v((8, 8, 128), F32),
            v((8, KH, 128), F32), v((PTS, 128), BF16), v((256, 128), BF16),
            v((KH, 256), BF16), v((KH, KH), BF16),
            v((256, 1024), BF16), v((256, 1024), BF16), v((KH, 1024), BF16), v((KH, 1024), BF16),
            v((8, KH, 128), F32), v((8, CH, 128), F32), v((8, CH, 128), F32),
            v((128, 128), BF16), v((128, 128), BF16), v((64, 256), BF16), v((64, 256), BF16),
            v((NZ, 64, 128), BF16), v((NZ, 64, 128), BF16),
            v((NY, 64, 128), F32), v((NY, 64, 128), F32),
            v((CH, 2, 128), F32), v((CH, 2, 128), F32),
            v((NZ, 2, 128), F32), v((CH, 2, 128), F32),
            v((NY, 64, 128), BF16), v((NY, 64, 128), BF16),
            v((8, 128), F32), v((NY, 8, 128), F32),
            v((NZ, 64, 128), BF16), v((NZ, 64, 128), BF16),
            v((1024, 512), BF16), v((1024, 512), BF16), v((512, 1024), BF16),
            v((MODES, 128), F32), v((NZ, 64, 128), F32),
            pltpu.SemaphoreType.DMA((8,)), pltpu.SemaphoreType.DMA((8,)),
            pltpu.SemaphoreType.DMA((10,)),
        ],
        compiler_params=pltpu.CompilerParams(collective_id=0, has_side_effects=True),
        name="whole",
    )(points, counts, kin, kmid, kout, wskip, near, weights, *tables)


def body(point_data, neighbours, counts, kernel_in, kernel_mid, kernel_out, spectral, skip_weight):
    out = whole(
        point_data.reshape(24, 128),
        jnp.swapaxes(counts[0], 1, 2).reshape(64, 16),
        kernel_in,
        kernel_mid,
        kernel_out.T,
        skip_weight,
        neighbours.reshape(8, 128, NB),
        spectral.reshape(2048, CH),
    )
    return out.reshape(1, 8, 16, 8, CH)


def solution(mesh):
    cells = P(None, "gx", "gy", "gz", None)
    return jax.shard_map(
        body,
        mesh=mesh,
        in_specs=(
            P(None, None, ("gx", "gy", "gz")),
            cells,
            P(None, "gx", "gy", "gz"),
            P(),
            P(),
            P(),
            P(None, "gz", "gx", "gy", None, None),
            P(),
        ),
        out_specs=cells,
        check_vma=False,
    )
```

```python
import functools
import math

import jax
import jax.numpy as jnp
import numpy as np
from jax import lax
from jax.experimental import pallas as pl
from jax.experimental.pallas import tpu as pltpu
from jax.sharding import PartitionSpec as P

GRID = 64
MODES = 16
NB = 32
KH = 80
CH = 64
PTS = 512
NX, NY, NZ = 8, 4, 8
F32 = jnp.float32
BF16 = jnp.bfloat16
MESH_ID = pl.DeviceIdType.MESH


def dot(a, b):
    return jnp.dot(a, b, preferred_element_type=F32)


def gelu(v):
    inner = v * (0.7978845608028654 + 0.035677408136300125 * (v * v))
    half = 0.5 * v
    return half + half * jnp.tanh(inner)


def split_two(values):
    upper = values.astype(BF16)
    return upper, (values - upper.astype(F32)).astype(BF16)


def dot_first(a, b):
    return lax.dot_general(a, b, (((0,), (0,)), ((), ())), preferred_element_type=F32)


def twice_gelu(v):
    v = v.astype(BF16)
    inner = v * (BF16(0.7978845608028654) + BF16(0.035677408136300125) * (v * v))
    return v + v * jnp.tanh(inner)


def looked_up(lookup, chosen, block):
    low = chosen & 127
    odd, upper = (chosen & 128) != 0, (chosen & 256) != 0
    bits = [(block & (1 << n)) != 0 for n in range(5)]

    def tile(n):
        return jnp.take_along_axis(lookup[n], low, axis=1, mode="promise_in_bounds")

    def tree(first, level):
        if level < 0:
            near, far = (
                jnp.where(odd, tile(4 * first + n + 1), tile(4 * first + n)) for n in (0, 2)
            )
            return jnp.where(upper, far, near)
        left = tree(first, level - 1)
        if first + (1 << level) >= 27:
            return left
        return jnp.where(bits[level], tree(first + (1 << level), level - 1), left)

    return tree(0, 4)


CHUNKS = 32
BY_LANES = (6, 7)
PART = 256


@functools.cache
def transform_tables():
    m = np.arange(GRID)
    centred = np.where(np.arange(MODES) < MODES // 2, np.arange(MODES), np.arange(MODES) - MODES)
    third = np.arange(MODES)

    def angles(f):
        return 2.0 * np.pi * ((f[:, None] * m[None, :]) % GRID) / GRID

    cos_c, sin_c = np.cos(angles(centred)), np.sin(angles(centred))
    cos_t, sin_t = np.cos(angles(third)), np.sin(angles(third))
    eye_k = np.eye(4)
    both = np.stack([cos_t, -sin_t], axis=-1)
    fz = np.broadcast_to(
        both.reshape(4, 4, GRID, 2).transpose(2, 0, 1, 3)[:, :, None], (GRID, 4, 16, 4, 2)
    ).reshape(GRID, 512)
    turn = np.stack([np.stack([cos_c, -sin_c], -1), np.stack([sin_c, cos_c], -1)], -2)
    fy = np.einsum("jcpyro,kl->pykrjocl", turn.reshape(8, 2, NY, 16, 2, 2), eye_k).reshape(512, 128)
    first = np.stack([cos_c, sin_c]).reshape(2, 8, 2, NX, 8)
    fx = np.broadcast_to(
        first.transpose(3, 2, 1, 0, 4)[..., None], (NX, 2, 8, 2, 8, 8)
    ).reshape(NX, 16, 128)
    ix = np.broadcast_to(
        first.transpose(3, 4, 0, 2, 1)[..., None], (NX, 8, 2, 2, 8, 8)
    ).reshape(NX, 8, 256)
    back = np.stack([np.stack([cos_c, sin_c], -1), np.stack([-sin_c, cos_c], -1)], -2)
    iy = np.einsum("jcqyro,kl->jrckqylo", back.reshape(8, 2, NY, 16, 2, 2), eye_k).reshape(128, 512)
    weight = np.where(third == 0, 1.0, 2.0)[:, None, None] / GRID**3
    iz = np.broadcast_to(
        (both * weight).transpose(0, 2, 1).reshape(32, NZ, 1, 8), (32, NZ, 16, 8)
    ).reshape(32, 1024)
    return fz, fy, fx, ix, iy, iz


def two_tables(table):
    import ml_dtypes

    upper = table.astype(np.float32).astype(ml_dtypes.bfloat16)
    lower = (table - upper.astype(np.float64)).astype(np.float32).astype(ml_dtypes.bfloat16)
    return jnp.asarray(upper), jnp.asarray(lower)


def wide_table(table):
    return jnp.asarray(np.ascontiguousarray(table, dtype=np.float32))


def iota(shape, dim):
    return lax.broadcasted_iota(jnp.int32, shape, dim)


def block_swap(x):
    row, lane = iota(x.shape, 0), iota(x.shape, 1) // 16
    for bit in (1, 2, 4):
        high, right = (row & bit) != 0, (lane & bit) != 0
        down = pltpu.roll(pltpu.roll(x, bit, axis=0), 128 - 16 * bit, axis=1)
        up = pltpu.roll(pltpu.roll(x, x.shape[0] - bit, axis=0), 16 * bit, axis=1)
        x = jnp.where(high == right, x, jnp.where(high, down, up))
    return x


def whole_kernel(
    pts_ref, cnt_ref, kin_ref, kmid_ref, kout_ref, wskip_ref,
    near_hbm, w_hbm, fzc_hbm, fyh_hbm, fyl_hbm, fxc_hbm, ixc_hbm, iyh_hbm, iyl_hbm, izc_hbm,
    out_ref,
    near, w_ref, fzc_ref, fyh_ref, fyl_ref, fxc_ref, ixc_ref, iyh_ref, iyl_ref, izc_ref,
    around, table_rows, tab, slot_ids, block_ids, valid_slots,
    lookup, centres, win_few, pair_a, pair_b, pre, rowblk, win, wmid,
    masked_a, masked_b, hid_a, hid_b, acc, lat_ref, skip_ref, fxh, fxl, ixh, ixl,
    s1, r1, s2, r2, s4, r4, s5, r5, s7, r7, sv, rv, s8, r8, fzh, fzl, iz, grid, wide,
    send_sem, recv_sem, in_sem,
):
    gx, gy, gz = lax.axis_index("gx"), lax.axis_index("gy"), lax.axis_index("gz")
    me = gz * NX + gx
    barrier = pltpu.get_barrier_semaphore()
    fetched = [
        (near_hbm, near), (fzc_hbm, fzc_ref), (fxc_hbm.at[gx], fxc_ref), (ixc_hbm.at[gx], ixc_ref),
        (izc_hbm, izc_ref), (fyh_hbm, fyh_ref), (fyl_hbm, fyl_ref), (iyh_hbm, iyh_ref),
        (iyl_hbm, iyl_ref), (w_hbm, w_ref),
    ]

    def fetch(n):
        return pltpu.make_async_copy(fetched[n][0], fetched[n][1], in_sem.at[n])

    for n in range(len(fetched)):
        fetch(n).start()

    def along_y(d):
        return (gx, lax.rem(gy + d, NY), gz)

    def along_z(d):
        return (gx, gy, lax.rem(gz + d, NZ))

    def beside(step):
        return tuple(lax.rem(p + d + n, n) for p, d, n in zip((gx, gy, gz), step, (NX, NY, NZ)))

    plane = [
        (lax.rem(gx + dx, NX), gy, lax.rem(gz + dz, NZ))
        for dx in range(NX)
        for dz in range(NZ)
        if (dx, dz) != (0, 0)
    ]
    steps = [
        (dx, dy, dz)
        for dx in (-1, 0, 1)
        for dy in (-1, 0, 1)
        for dz in (-1, 0, 1)
        if (dx, dy, dz) != (0, 0, 0)
    ]
    apart = [beside(s) for s in steps if s[1] != 0 and (s[0], s[2]) != (0, 0)]
    peers = plane + [along_y(d) for d in range(1, NY)] + apart
    for peer in peers:
        pl.semaphore_signal(barrier, inc=1, device_id=peer, device_id_type=MESH_ID)

    rowblk[...] = (iota((256, 128), 0) // 9).astype(F32).astype(BF16)
    col = iota((6, 256), 1)
    nine = col % 9
    source = jnp.where(nine < 3, nine, nine - 3)
    chosen = jnp.where((source == iota((6, 256), 0)) & (col < 243), 1.0, 0.0).astype(BF16)
    win[...] = dot_first(kin_ref[...], chosen).astype(BF16)
    eye = jnp.where(iota((KH, KH), 0) == iota((KH, KH), 1), 0.5, 0.0).astype(BF16)
    wmid[...] = dot_first(kmid_ref[...], eye).astype(BF16)
    few = jnp.where(iota((6, 8), 0) == iota((6, 8), 1), 1.0, 0.0).astype(BF16)
    win_few[...] = dot_first(kin_ref[...], few).astype(BF16)
    row, lane = iota((8, 128), 0), iota((8, 128), 1)
    index_y, index_z = gy * 16 + lane // 8, gz * 8 + lane % 8
    for x in range(8):
        index = jnp.where(row == 0, gx * 8 + x, jnp.where(row == 1, index_y, index_z))
        centre = jnp.where(row < 3, -(index.astype(F32) + 0.5) / GRID, 0.0)
        centres[x] = centre
        pre[x] = dot_first(kin_ref[...], centre[0:6].astype(BF16))
    by_row = jnp.where(iota((16, 128), 1) // 8 == iota((16, 128), 0), 1.0, 0.0).astype(BF16)
    spread = dot(cnt_ref[...].astype(F32).astype(BF16), by_row)
    spread = jnp.where(iota((64, 128), 0) % 8 == iota((64, 128), 1) % 8, spread, 0.0)
    gather = jnp.where(iota((8, 64), 1) // 8 == iota((8, 64), 0), 1.0, 0.0).astype(BF16)
    spread = dot(gather, spread.astype(BF16))
    for x in range(8):
        valid_slots[x] = jnp.broadcast_to(spread[x : x + 1], (8, 128))
    acc[...] = jnp.zeros((8, KH, 128), F32)
    table_rows[pl.ds(240, 16), :] = jnp.zeros((16, PTS), F32)
    lookup[:, 6:8, :] = jnp.zeros((108, 2, 128), F32)
    fetch(0).wait()
    for x in range(8):
        point = near[x].T
        owner = point >> 9
        offset_z = (owner & 7) - gz + 1
        offset_y = ((owner >> 3) & 3) - gy + 1
        offset_x = (owner >> 5) - gx + 1
        block = (offset_x * 3 + offset_y) * 3 + offset_z
        block_ids[pl.ds(4 * x, 4)] = block.reshape(4, 8, 128)
        slot_ids[pl.ds(4 * x, 4)] = (point & 511).reshape(4, 8, 128)
    pl.semaphore_wait(barrier, len(peers))

    def send(n, source, target, peer):
        pltpu.make_async_remote_copy(
            src_ref=source,
            dst_ref=target,
            send_sem=send_sem.at[n],
            recv_sem=recv_sem.at[n],
            device_id=peer,
            device_id_type=MESH_ID,
        ).start()

    def arrived(n, buffer, count):
        part = buffer.at[pl.ds(0, count)]
        pltpu.make_async_copy(part, part, recv_sem.at[n]).wait()

    def left(n, buffer, count):
        part = buffer.at[pl.ds(0, count)]
        pltpu.make_async_copy(part, part, send_sem.at[n]).wait()

    for step in steps:
        block = ((1 - step[0]) * 3 + (1 - step[1])) * 3 + (1 - step[2])
        send(7, pts_ref, around.at[block], beside(step))
    around[13] = pts_ref[...]
    for n in range(1, 5):
        fetch(n).wait()
    own_y = iota((128, 512), 0) // 8 == iota((128, 512), 1) % 128 // 8
    for q in range(NZ):
        part = jnp.concatenate([fzc_ref[pl.ds(8 * q, 8), :]] * 16, axis=0)
        upper, lower = split_two(jnp.where(own_y, part, 0.0))
        fzh[pl.ds(128 * q, 128), :] = upper
        fzl[pl.ds(128 * q, 128), :] = lower
    own_y = iota((128, 1024), 0) // 8 == iota((128, 1024), 1) % 128 // 8
    for q in range(NY):
        part = jnp.concatenate([izc_ref[pl.ds(8 * q, 8), :]] * 16, axis=0)
        iz[pl.ds(128 * q, 128), :] = jnp.where(own_y, part, 0.0).astype(BF16)
    part = jnp.concatenate(
        [jnp.broadcast_to(fxc_ref[pl.ds(n, 1), :], (8, 128)) for n in range(16)], axis=0
    )
    row, lane = iota((128, 128), 0), iota((128, 128), 1)
    fxh[...], fxl[...] = split_two(jnp.where(row % 8 == lane % 8, part, 0.0))
    part = jnp.concatenate(
        [jnp.broadcast_to(ixc_ref[pl.ds(n, 1), :], (8, 256)) for n in range(8)], axis=0
    )
    ixh[...], ixl[...] = split_two(jnp.where(iota((64, 256), 0) % 8 == iota((64, 256), 1) % 8, part, 0.0))
    arrived(7, around, 26)
    for b in range(27):
        for t in range(4):
            block = around[b, pl.ds(t, 6, stride=4), :]
            lookup[4 * b + t, 0:6, :] = block
            place = block[0:3]
            upper = place.astype(BF16).astype(F32)
            table_rows[pl.ds(9 * b, 9), pl.ds(128 * t, 128)] = jnp.concatenate(
                [upper, place - upper, block[3:6]], axis=0
            )
    tab[...] = table_rows[...].astype(BF16)
    none = jnp.zeros((256, 128), BF16)
    low_ids = iota((64, 128), 0)

    def step(t, masked_out, masked_in, pair_out, pair_in, hid_out, hid_in):
        early = jnp.minimum(t, CHUNKS - 1)
        middle = jnp.clip(t - 1, 0, CHUNKS - 1)
        late = jnp.maximum(t - 2, 0)
        slots, owners = slot_ids[early], block_ids[early]
        blocks = owners.astype(F32)
        centre = centres[early // 4]
        base = jnp.concatenate([pre[middle // 4]] * 2, axis=1)
        valid = jnp.where(t >= 2, valid_slots[late // 4], 0.0)[0:1]
        first = (late % 4 * 8).astype(F32)
        total = jnp.zeros((KH, 128), F32)
        for part in range(4):
            span = pl.ds(part * PART, PART)
            by_lanes = 2 * part in BY_LANES
            if by_lanes:
                ahead = dot(win_few[...], pair_in[...])
            else:
                hot = []
                for s in (2 * part, 2 * part + 1):
                    chosen = jnp.broadcast_to(slots[s : s + 1], (8, 128))
                    low = jnp.broadcast_to((chosen & 63)[0:1], (64, 128))
                    low = jnp.where(low == low_ids, 1.0, 0.0).astype(BF16)
                    high = chosen >> 6
                    for n in range(8):
                        here = jnp.where(high == n, 1.0, 0.0)
                        here = jnp.concatenate([here] * 8, axis=0).astype(BF16)
                        hot.append(low * here)
                hot = [jnp.concatenate(hot[:8], axis=0), jnp.concatenate(hot[8:], axis=0)]
                found = dot(tab[...], jnp.concatenate(hot, axis=1))
                ahead = dot(win[...], masked_in[:, span]) + base
            last = dot(wmid[...], hid_in[:, span])
            hid_out[:, span] = twice_gelu(ahead)
            last = twice_gelu(last).astype(F32)
            for n in range(2):
                used = valid > first + (2 * part + n)
                total = total + jnp.where(used, last[:, n * 128 : (n + 1) * 128], 0.0)
            if by_lanes:
                for n in range(2):
                    s = 2 * part + n
                    chosen = jnp.broadcast_to(slots[s : s + 1], (8, 128))
                    block = jnp.broadcast_to(owners[s : s + 1], (8, 128))
                    pair = looked_up(lookup, chosen, block) + centre
                    pair_out[:, pl.ds(n * 128, 128)] = pair.astype(BF16)
            else:
                found = found.astype(BF16)
                for n in range(2):
                    s = 2 * part + n
                    chosen = jnp.broadcast_to(blocks[s : s + 1], (256, 128)).astype(BF16)
                    masked_out[:, pl.ds(s * 128, 128)] = jnp.where(
                        rowblk[...] == chosen, found[:, n * 128 : (n + 1) * 128], none
                    )
        acc[late // 4] += total

    for unset in (masked_a, masked_b):
        unset[...] = jnp.zeros((256, 1024), BF16)
    for unset in (pair_a, pair_b):
        unset[...] = jnp.zeros((8, 256), BF16)
    for unset in (hid_a, hid_b):
        unset[...] = jnp.zeros((KH, 1024), BF16)

    def two_steps(tt, carry):
        step(2 * tt, masked_a, masked_b, pair_a, pair_b, hid_a, hid_b)
        step(2 * tt + 1, masked_b, masked_a, pair_b, pair_a, hid_b, hid_a)
        return carry

    lax.fori_loop(0, CHUNKS // 2 + 1, two_steps, 0)
    for x in range(8):
        upper, lower = split_two(0.5 * acc[x])
        values = dot(kout_ref[...], upper) + dot(kout_ref[...], lower)
        latent = (values / valid_slots[x, 0:1]).astype(BF16)
        skip_ref[x] = dot_first(wskip_ref[...], latent)
        lat_ref[x] = latent.astype(F32)
    for q in range(NZ):
        s1[q] = lat_ref[:, pl.ds(8 * q, 8), :].reshape(64, 128).astype(BF16)
    for d in range(1, NZ):
        peer = along_z(d)
        send(0, s1.at[peer[2]], r1.at[gz], peer)
    r1[gz] = s1[gz]
    row, lane = iota((128, 128), 0), iota((128, 128), 1)
    row_i, lane_i = row // 8 % 8 * 2 + row // 64, lane // 8 % 8 * 2 + lane // 64
    mirror = (row % 8 == lane % 8) & (row_i != 8) & (lane_i == (16 - row_i) % 16)
    mirror = jnp.where(mirror, 1.0, 0.0).astype(BF16)
    row_j, lane_j = row // 16 * 2 + row // 4 % 2, lane // 16 * 2 + lane // 4 % 2
    flip = (row % 4 == 0) & (lane % 4 == 0) & (row // 8 % 2 == lane // 8 % 2)
    flip = flip & (lane_j != 8) & (row_j == (16 - lane_j) % 16)
    flip = jnp.where(flip, jnp.where(lane // 8 % 2 == 0, 1.0, -1.0), 0.0).astype(BF16)
    pick = jnp.where(iota((16, 128), 1) % 16 == iota((16, 128), 0), 1.0, 0.0).astype(BF16)
    own_channel = iota((64, 128), 0) % 8 == iota((64, 128), 1) // 16
    own_mode = iota((32, 1024), 1) // CH == iota((32, 1024), 0) % MODES
    for n in range(5, 10):
        fetch(n).wait()
    arrived(0, r1, NZ - 1)
    line = jnp.concatenate([r1[q] for q in range(NZ)], axis=1)
    deep = dot(line, fzh[...]) + dot(line, fzl[...])
    for q in range(NY):
        s2[q] = deep[:, q * 128 : (q + 1) * 128]
    for d in range(1, NY):
        peer = along_y(d)
        send(1, s2.at[peer[1]], r2.at[gy], peer)
    r2[gy] = s2[gy]
    arrived(1, r2, NY - 1)
    upper, lower = split_two(jnp.concatenate([r2[q] for q in range(NY)], axis=1))
    flat = dot(upper, fyh_ref[...]) + dot(upper, fyl_ref[...]) + dot(lower, fyh_ref[...])
    real = iota((64, 128), 1) // 8 % 2 == 0
    turned = jnp.where(real, pltpu.roll(flat, 120, axis=1), -pltpu.roll(flat, 8, axis=1))
    upper, lower = split_two(jnp.concatenate([flat, turned], axis=0))
    share = block_swap(dot(fxh[...], upper) + dot(fxl[...], upper) + dot(fxh[...], lower))
    for i in range(2):
        s4[:, i, :] = share[64 * i : 64 * i + 64]
    for peer in plane:
        send(2, s4.at[peer[2] * NX + peer[0]], r4.at[me], peer)
    r4[me] = s4[me]
    arrived(2, r4, 63)
    for q in range(NZ):
        pair = r4[q * NX]
        for n in range(1, NX):
            pair = pair + r4[q * NX + n]
        grid[pl.ds(2 * q, 2), :] = pair
    found = []
    for i in range(2):
        values = jnp.concatenate(
            [jnp.broadcast_to(grid[pl.ds(2 * q + i, 1), :], (8, 128)) for q in range(NZ)], axis=0
        )
        values = jnp.where(own_channel, values, 0.0).astype(BF16)
        found.append(
            lax.dot_general(
                pick,
                jnp.concatenate([values, values], axis=0),
                (((1,), (1,)), ((), ())),
                preferred_element_type=F32,
            )
        )
    rows = jnp.concatenate(
        [found[0][0:8], found[1][0:8], found[0][8:16], found[1][8:16]], axis=0
    )
    spread = jnp.where(own_mode, jnp.concatenate([rows] * 8, axis=1), 0.0).astype(BF16)
    by_real, by_imag = dot(spread, w_ref[0:1024]), dot(spread, w_ref[1024:2048])
    mixed_real = by_real[0:16] - by_imag[16:32]
    mixed_imag = by_imag[0:16] + by_real[16:32]
    for i in range(2):
        mine = jnp.concatenate(
            [mixed_real[8 * i : 8 * i + 8], mixed_imag[8 * i : 8 * i + 8]], axis=0
        ).astype(BF16)
        placed = jnp.where(own_channel, dot_first(mine, pick), 0.0).astype(BF16)
        s5[:, i, :] = dot(gather, placed)
    for peer in plane:
        send(3, s5.at[peer[2]], r5.at[me], peer)
    r5[me] = s5[gz]
    arrived(3, r5, 63)
    values = block_swap(jnp.concatenate([r5[:, i, :] for i in range(2)], axis=0))
    is_mean = (row < 8) & ((lane == 0) | (lane == 8)) & (gy == 0)
    values = jnp.where(is_mean, 0.0, values)
    exact = values.astype(BF16)
    real = lane // 8 % 2 == 0
    turned = jnp.where(real, -pltpu.roll(values, 120, axis=1), pltpu.roll(values, 8, axis=1))
    stacked = jnp.concatenate([exact, turned.astype(BF16)], axis=0)
    plain = (dot(ixh[...], stacked) + dot(ixl[...], stacked)).astype(BF16)
    flat = dot(plain, iyh_ref[...]) + dot(plain, iyl_ref[...])
    for q in range(NY):
        s7[q] = flat[:, q * 128 : (q + 1) * 128].astype(BF16)
    for d in range(1, NY):
        peer = along_y(d)
        send(4, s7.at[peer[1]], r7.at[gy], peer)
    r7[gy] = s7[gy]
    weight = jnp.where((lane % 4 == 0) & (gy == 0), 0.5, 2.0)
    pairs = dot(dot(mirror, exact).astype(BF16), flip)
    pairs = jnp.where(gy == 0, 0.5 * pairs, 0.0)
    power = jnp.sum(values * (weight * values + pairs), axis=1, keepdims=True)
    power = jnp.sum(power.reshape(16, 8, 1), axis=0)
    sv[...] = jnp.broadcast_to(power, (8, 128))
    for d in range(1, NY):
        send(5, sv, rv.at[gy], along_y(d))
    rv[gy] = sv[...]
    arrived(4, r7, NY - 1)
    line = jnp.concatenate([r7[q] for q in range(NY)], axis=1)
    depth = dot(line, iz[...])
    arrived(5, rv, NY - 1)
    power = (rv[0] + rv[1]) + (rv[2] + rv[3])
    scale = 1.0 / jnp.sqrt(power * (1.0 / float(GRID) ** 6) + 1.0)
    scale = jnp.concatenate([scale] * 8, axis=0)
    for q in range(NZ):
        s8[q] = (depth[:, q * 128 : (q + 1) * 128] * scale).astype(BF16)
    for d in range(1, NZ):
        peer = along_z(d)
        send(6, s8.at[peer[2]], r8.at[gz], peer)
    r8[gz] = s8[gz]
    arrived(6, r8, NZ - 1)
    wide[...] = r8[...].astype(F32)
    for x in range(8):
        out_ref[x] = gelu(wide[:, pl.ds(8 * x, 8), :].reshape(CH, 128) + skip_ref[x]).T
    left(0, r1, NZ - 1)
    left(1, r2, NY - 1)
    left(2, r4, 63)
    left(3, r5, 63)
    left(4, r7, NY - 1)
    left(5, rv, NY - 1)
    left(6, r8, NZ - 1)
    left(7, around, 26)


def whole(points, counts, kin, kmid, kout, wskip, near, weights):
    fz, fy, fx, ix, iy, iz = transform_tables()
    tables = [wide_table(fz), *two_tables(fy), wide_table(fx), wide_table(ix)]
    tables += [*two_tables(iy), wide_table(iz)]
    vmem, anywhere = (pl.BlockSpec(memory_space=m) for m in (pltpu.VMEM, pl.ANY))
    v = pltpu.VMEM
    return pl.pallas_call(
        whole_kernel,
        out_shape=jax.ShapeDtypeStruct((8, 128, CH), F32),
        in_specs=[vmem] * 6 + [anywhere] * (2 + len(tables)),
        out_specs=vmem,
        scratch_shapes=[
            v((8, 128, NB), jnp.int32), v((2048, CH), BF16),
            v((GRID, 512), F32), v((512, 128), BF16), v((512, 128), BF16),
            v((16, 128), F32), v((8, 256), F32), v((128, 512), BF16), v((128, 512), BF16),
            v((32, 1024), F32),
            v((27, 24, 128), F32), v((256, PTS), F32), v((256, PTS), BF16),
            v((CHUNKS, 8, 128), jnp.int32), v((CHUNKS, 8, 128), jnp.int32), v((8, 8, 128), F32),
            v((108, 8, 128), F32), v((8, 8, 128), F32), v((KH, 8), BF16),
            v((8, 256), BF16), v((8, 256), BF16),
            v((8, KH, 128), F32), v((256, 128), BF16),
            v((KH, 256), BF16), v((KH, KH), BF16),
            v((256, 1024), BF16), v((256, 1024), BF16), v((KH, 1024), BF16), v((KH, 1024), BF16),
            v((8, KH, 128), F32), v((8, CH, 128), F32), v((8, CH, 128), F32),
            v((128, 128), BF16), v((128, 128), BF16), v((64, 256), BF16), v((64, 256), BF16),
            v((NZ, 64, 128), BF16), v((NZ, 64, 128), BF16),
            v((NY, 64, 128), F32), v((NY, 64, 128), F32),
            v((CH, 2, 128), F32), v((CH, 2, 128), F32),
            v((NZ, 2, 128), F32), v((CH, 2, 128), F32),
            v((NY, 64, 128), BF16), v((NY, 64, 128), BF16),
            v((8, 128), F32), v((NY, 8, 128), F32),
            v((NZ, 64, 128), BF16), v((NZ, 64, 128), BF16),
            v((1024, 512), BF16), v((1024, 512), BF16), v((512, 1024), BF16),
            v((MODES, 128), F32), v((NZ, 64, 128), F32),
            pltpu.SemaphoreType.DMA((8,)), pltpu.SemaphoreType.DMA((8,)),
            pltpu.SemaphoreType.DMA((10,)),
        ],
        compiler_params=pltpu.CompilerParams(collective_id=0, has_side_effects=True),
        name="whole",
    )(points, counts, kin, kmid, kout, wskip, near, weights, *tables)


def body(point_data, neighbours, counts, kernel_in, kernel_mid, kernel_out, spectral, skip_weight):
    out = whole(
        point_data.reshape(24, 128),
        jnp.swapaxes(counts[0], 1, 2).reshape(64, 16),
        kernel_in,
        kernel_mid,
        kernel_out.T,
        skip_weight,
        neighbours.reshape(8, 128, NB),
        spectral.reshape(2048, CH),
    )
    return out.reshape(1, 8, 16, 8, CH)


def solution(mesh):
    cells = P(None, "gx", "gy", "gz", None)
    return jax.shard_map(
        body,
        mesh=mesh,
        in_specs=(
            P(None, None, ("gx", "gy", "gz")),
            cells,
            P(None, "gx", "gy", "gz"),
            P(),
            P(),
            P(),
            P(None, "gz", "gx", "gy", None, None),
            P(),
        ),
        out_specs=cells,
        check_vma=False,
    )
```

```python
import functools
import math

import jax
import jax.numpy as jnp
import numpy as np
from jax import lax
from jax.experimental import pallas as pl
from jax.experimental.pallas import tpu as pltpu
from jax.sharding import PartitionSpec as P

GRID = 64
MODES = 16
NB = 32
KH = 80
CH = 64
PTS = 512
NX, NY, NZ = 8, 4, 8
F32 = jnp.float32
BF16 = jnp.bfloat16
MESH_ID = pl.DeviceIdType.MESH


def dot(a, b):
    return jnp.dot(a, b, preferred_element_type=F32)


def gelu(v):
    inner = v * (0.7978845608028654 + 0.035677408136300125 * (v * v))
    half = 0.5 * v
    return half + half * jnp.tanh(inner)


def split_two(values):
    upper = values.astype(BF16)
    return upper, (values - upper.astype(F32)).astype(BF16)


def dot_first(a, b):
    return lax.dot_general(a, b, (((0,), (0,)), ((), ())), preferred_element_type=F32)


def twice_gelu(v):
    v = v.astype(BF16)
    inner = v * (BF16(0.7978845608028654) + BF16(0.035677408136300125) * (v * v))
    return v + v * jnp.tanh(inner)


def looked_up(lookup, chosen, block):
    low = chosen & 127
    odd, upper = (chosen & 128) != 0, (chosen & 256) != 0
    bits = [(block & (1 << n)) != 0 for n in range(5)]

    def tile(n):
        return jnp.take_along_axis(lookup[n], low, axis=1, mode="promise_in_bounds")

    def tree(first, level):
        if level < 0:
            near, far = (
                jnp.where(odd, tile(4 * first + n + 1), tile(4 * first + n)) for n in (0, 2)
            )
            return jnp.where(upper, far, near)
        left = tree(first, level - 1)
        if first + (1 << level) >= 27:
            return left
        return jnp.where(bits[level], tree(first + (1 << level), level - 1), left)

    return tree(0, 4)


CHUNKS = 32
BY_LANES = (6, 7)
PART = 256


@functools.cache
def transform_tables():
    m = np.arange(GRID)
    centred = np.where(np.arange(MODES) < MODES // 2, np.arange(MODES), np.arange(MODES) - MODES)
    third = np.arange(MODES)

    def angles(f):
        return 2.0 * np.pi * ((f[:, None] * m[None, :]) % GRID) / GRID

    cos_c, sin_c = np.cos(angles(centred)), np.sin(angles(centred))
    cos_t, sin_t = np.cos(angles(third)), np.sin(angles(third))
    eye_k = np.eye(4)
    both = np.stack([cos_t, -sin_t], axis=-1)
    fz = np.broadcast_to(
        both.reshape(4, 4, GRID, 2).transpose(2, 0, 1, 3)[:, :, None], (GRID, 4, 16, 4, 2)
    ).reshape(GRID, 512)
    turn = np.stack([np.stack([cos_c, -sin_c], -1), np.stack([sin_c, cos_c], -1)], -2)
    fy = np.einsum("jcpyro,kl->pykrjocl", turn.reshape(8, 2, NY, 16, 2, 2), eye_k).reshape(512, 128)
    first = np.stack([cos_c, sin_c]).reshape(2, 8, 2, NX, 8)
    fx = np.broadcast_to(
        first.transpose(3, 2, 1, 0, 4)[..., None], (NX, 2, 8, 2, 8, 8)
    ).reshape(NX, 16, 128)
    ix = np.broadcast_to(
        first.transpose(3, 4, 0, 2, 1)[..., None], (NX, 8, 2, 2, 8, 8)
    ).reshape(NX, 8, 256)
    back = np.stack([np.stack([cos_c, sin_c], -1), np.stack([-sin_c, cos_c], -1)], -2)
    iy = np.einsum("jcqyro,kl->jrckqylo", back.reshape(8, 2, NY, 16, 2, 2), eye_k).reshape(128, 512)
    weight = np.where(third == 0, 1.0, 2.0)[:, None, None] / GRID**3
    iz = np.broadcast_to(
        (both * weight).transpose(0, 2, 1).reshape(32, NZ, 1, 8), (32, NZ, 16, 8)
    ).reshape(32, 1024)
    return fz, fy, fx, ix, iy, iz


def two_tables(table):
    import ml_dtypes

    upper = table.astype(np.float32).astype(ml_dtypes.bfloat16)
    lower = (table - upper.astype(np.float64)).astype(np.float32).astype(ml_dtypes.bfloat16)
    return jnp.asarray(upper), jnp.asarray(lower)


def wide_table(table):
    return jnp.asarray(np.ascontiguousarray(table, dtype=np.float32))


def iota(shape, dim):
    return lax.broadcasted_iota(jnp.int32, shape, dim)


def block_swap(x):
    row, lane = iota(x.shape, 0), iota(x.shape, 1) // 16
    for bit in (1, 2, 4):
        high, right = (row & bit) != 0, (lane & bit) != 0
        down = pltpu.roll(pltpu.roll(x, bit, axis=0), 128 - 16 * bit, axis=1)
        up = pltpu.roll(pltpu.roll(x, x.shape[0] - bit, axis=0), 16 * bit, axis=1)
        x = jnp.where(high == right, x, jnp.where(high, down, up))
    return x


def whole_kernel(
    pts_hbm, cnt_hbm, kin_hbm, kmid_hbm, kout_hbm, wskip_hbm, near_hbm, w_hbm, fzc_hbm, fyh_hbm, fyl_hbm, fxc_hbm, ixc_hbm, iyh_hbm, iyl_hbm, izc_hbm,
    out_ref,
    pts_ref, cnt_ref, kin_ref, kmid_ref, kout_ref, wskip_ref, near, w_ref, fzc_ref, fyh_ref, fyl_ref, fxc_ref, ixc_ref, iyh_ref, iyl_ref, izc_ref,
    around, table_rows, tab, slot_ids, block_ids, valid_slots,
    lookup, centres, win_few, pair_a, pair_b, pre, rowblk, win, wmid,
    masked_a, masked_b, hid_a, hid_b, acc, lat_ref, skip_ref, fxh, fxl, ixh, ixl,
    s1, r1, s2, r2, s4, r4, s5, r5, s7, r7, sv, rv, s8, r8, fzh, fzl, iz, grid, wide,
    send_sem, recv_sem, in_sem,
):
    gx, gy, gz = lax.axis_index("gx"), lax.axis_index("gy"), lax.axis_index("gz")
    me = gz * NX + gx
    barrier = pltpu.get_barrier_semaphore()
    fetched = [
        (near_hbm, near), (fzc_hbm, fzc_ref), (fxc_hbm.at[gx], fxc_ref), (ixc_hbm.at[gx], ixc_ref),
        (izc_hbm, izc_ref), (fyh_hbm, fyh_ref), (fyl_hbm, fyl_ref), (iyh_hbm, iyh_ref),
        (iyl_hbm, iyl_ref), (w_hbm, w_ref), (kin_hbm, kin_ref), (kmid_hbm, kmid_ref),
        (cnt_hbm, cnt_ref), (pts_hbm, pts_ref), (kout_hbm, kout_ref), (wskip_hbm, wskip_ref),
    ]

    def fetch(n):
        return pltpu.make_async_copy(fetched[n][0], fetched[n][1], in_sem.at[n])

    for n in (13, 10, 11, 12, 0, 14, 15, *range(1, 10)):
        fetch(n).start()

    def along_y(d):
        return (gx, lax.rem(gy + d, NY), gz)

    def along_z(d):
        return (gx, gy, lax.rem(gz + d, NZ))

    far_z = (4, 3, 5, 2, 6, 1, 7)

    def beside(step):
        return tuple(lax.rem(p + d + n, n) for p, d, n in zip((gx, gy, gz), step, (NX, NY, NZ)))

    plane = [
        (lax.rem(gx + dx, NX), gy, lax.rem(gz + dz, NZ))
        for dx, dz in sorted(
            ((dx, dz) for dx in range(NX) for dz in range(NZ) if (dx, dz) != (0, 0)),
            key=lambda d: -2 * min(d[0], NX - d[0]) - min(d[1], NZ - d[1]),
        )
    ]
    steps = [
        (dx, dy, dz)
        for dx in (-1, 0, 1)
        for dy in (-1, 0, 1)
        for dz in (-1, 0, 1)
        if (dx, dy, dz) != (0, 0, 0)
    ]
    apart = [beside(s) for s in steps if s[1] != 0 and (s[0], s[2]) != (0, 0)]
    peers = plane + [along_y(d) for d in range(1, NY)] + apart
    for peer in peers:
        pl.semaphore_signal(barrier, inc=1, device_id=peer, device_id_type=MESH_ID)

    for n in range(10, 16):
        fetch(n).wait()
    rowblk[...] = iota((256, 128), 0) // 9
    col = iota((6, 256), 1)
    nine = col % 9
    source = jnp.where(nine < 3, nine, nine - 3)
    chosen = jnp.where((source == iota((6, 256), 0)) & (col < 243), 1.0, 0.0).astype(BF16)
    win[...] = dot_first(kin_ref[...], chosen).astype(BF16)
    eye = jnp.where(iota((KH, KH), 0) == iota((KH, KH), 1), 0.5, 0.0).astype(BF16)
    wmid[...] = dot_first(kmid_ref[...], eye).astype(BF16)
    few = jnp.where(iota((6, 8), 0) == iota((6, 8), 1), 1.0, 0.0).astype(BF16)
    win_few[...] = dot_first(kin_ref[...], few).astype(BF16)
    row, lane = iota((8, 128), 0), iota((8, 128), 1)
    index_y, index_z = gy * 16 + lane // 8, gz * 8 + lane % 8
    for x in range(8):
        index = jnp.where(row == 0, gx * 8 + x, jnp.where(row == 1, index_y, index_z))
        centre = jnp.where(row < 3, -(index.astype(F32) + 0.5) / GRID, 0.0)
        centres[x] = centre
        pre[x] = dot_first(kin_ref[...], centre[0:6].astype(BF16))
    by_row = jnp.where(iota((16, 128), 1) // 8 == iota((16, 128), 0), 1.0, 0.0).astype(BF16)
    spread = dot(cnt_ref[...].astype(F32).astype(BF16), by_row)
    spread = jnp.where(iota((64, 128), 0) % 8 == iota((64, 128), 1) % 8, spread, 0.0)
    gather = jnp.where(iota((8, 64), 1) // 8 == iota((8, 64), 0), 1.0, 0.0).astype(BF16)
    spread = dot(gather, spread.astype(BF16))
    for x in range(8):
        valid_slots[x] = jnp.broadcast_to(spread[x : x + 1], (8, 128))
    acc[...] = jnp.zeros((8, KH, 128), F32)
    table_rows[pl.ds(240, 16), :] = jnp.zeros((16, PTS), F32)
    lookup[:, 6:8, :] = jnp.zeros((108, 2, 128), F32)
    fetch(0).wait()
    for x in range(8):
        point = near[x].T
        owner = point >> 9
        offset_z = (owner & 7) - gz + 1
        offset_y = ((owner >> 3) & 3) - gy + 1
        offset_x = (owner >> 5) - gx + 1
        block = (offset_x * 3 + offset_y) * 3 + offset_z
        block_ids[pl.ds(4 * x, 4)] = block.reshape(4, 8, 128)
        slot_ids[pl.ds(4 * x, 4)] = (point & 511).reshape(4, 8, 128)
    pl.semaphore_wait(barrier, len(peers))

    def send(n, source, target, peer):
        pltpu.make_async_remote_copy(
            src_ref=source,
            dst_ref=target,
            send_sem=send_sem.at[n],
            recv_sem=recv_sem.at[n],
            device_id=peer,
            device_id_type=MESH_ID,
        ).start()

    def arrived(n, buffer, count):
        part = buffer.at[pl.ds(0, count)]
        pltpu.make_async_copy(part, part, recv_sem.at[n]).wait()

    def left(n, buffer, count):
        part = buffer.at[pl.ds(0, count)]
        pltpu.make_async_copy(part, part, send_sem.at[n]).wait()

    for step in steps:
        block = ((1 - step[0]) * 3 + (1 - step[1])) * 3 + (1 - step[2])
        send(7, pts_ref, around.at[block], beside(step))
    around[13] = pts_ref[...]
    for n in range(1, 5):
        fetch(n).wait()
    own_y = iota((128, 512), 0) // 8 == iota((128, 512), 1) % 128 // 8
    for q in range(NZ):
        part = jnp.concatenate([fzc_ref[pl.ds(8 * q, 8), :]] * 16, axis=0)
        upper, lower = split_two(jnp.where(own_y, part, 0.0))
        fzh[pl.ds(128 * q, 128), :] = upper
        fzl[pl.ds(128 * q, 128), :] = lower
    own_y = iota((128, 1024), 0) // 8 == iota((128, 1024), 1) % 128 // 8
    for q in range(NY):
        part = jnp.concatenate([izc_ref[pl.ds(8 * q, 8), :]] * 16, axis=0)
        iz[pl.ds(128 * q, 128), :] = jnp.where(own_y, part, 0.0).astype(BF16)
    part = jnp.concatenate(
        [jnp.broadcast_to(fxc_ref[pl.ds(n, 1), :], (8, 128)) for n in range(16)], axis=0
    )
    row, lane = iota((128, 128), 0), iota((128, 128), 1)
    fxh[...], fxl[...] = split_two(jnp.where(row % 8 == lane % 8, part, 0.0))
    part = jnp.concatenate(
        [jnp.broadcast_to(ixc_ref[pl.ds(n, 1), :], (8, 256)) for n in range(8)], axis=0
    )
    ixh[...], ixl[...] = split_two(jnp.where(iota((64, 256), 0) % 8 == iota((64, 256), 1) % 8, part, 0.0))
    arrived(7, around, 26)
    for b in range(27):
        for t in range(4):
            block = around[b, pl.ds(t, 6, stride=4), :]
            lookup[4 * b + t, 0:6, :] = block
            place = block[0:3]
            upper = place.astype(BF16).astype(F32)
            table_rows[pl.ds(9 * b, 9), pl.ds(128 * t, 128)] = jnp.concatenate(
                [upper, place - upper, block[3:6]], axis=0
            )
    tab[...] = table_rows[...].astype(BF16)
    low_ids = iota((64, 128), 0)

    def step(t, masked_out, masked_in, pair_out, pair_in, hid_out, hid_in):
        early = jnp.minimum(t, CHUNKS - 1)
        middle = jnp.clip(t - 1, 0, CHUNKS - 1)
        late = jnp.maximum(t - 2, 0)
        slots, owners = slot_ids[early], block_ids[early]
        centre = centres[early // 4]
        base = jnp.concatenate([pre[middle // 4]] * 2, axis=1)
        valid = jnp.where(t >= 2, valid_slots[late // 4], 0.0)[0:1]
        first = (late % 4 * 8).astype(F32)
        total = jnp.zeros((KH, 128), F32)
        for part in range(4):
            span = pl.ds(part * PART, PART)
            by_lanes = 2 * part in BY_LANES
            if by_lanes:
                ahead = dot(win_few[...], pair_in[...])
            else:
                hot = []
                for s in (2 * part, 2 * part + 1):
                    chosen = jnp.broadcast_to(slots[s : s + 1], (8, 128))
                    low = jnp.broadcast_to((chosen & 63)[0:1], (64, 128))
                    low = jnp.where(low == low_ids, 1.0, 0.0).astype(BF16)
                    high = chosen >> 6
                    for n in range(8):
                        here = jnp.where(high == n, 1.0, 0.0)
                        here = jnp.concatenate([here] * 8, axis=0).astype(BF16)
                        hot.append(low * here)
                hot = [jnp.concatenate(hot[:8], axis=0), jnp.concatenate(hot[8:], axis=0)]
                found = dot(tab[...], jnp.concatenate(hot, axis=1))
                ahead = dot(win[...], masked_in[:, span]) + base
            last = dot(wmid[...], hid_in[:, span])
            hid_out[:, span] = twice_gelu(ahead)
            last = twice_gelu(last).astype(F32)
            for n in range(2):
                used = valid > first + (2 * part + n)
                total = total + jnp.where(used, last[:, n * 128 : (n + 1) * 128], 0.0)
            if by_lanes:
                for n in range(2):
                    s = 2 * part + n
                    chosen = jnp.broadcast_to(slots[s : s + 1], (8, 128))
                    block = jnp.broadcast_to(owners[s : s + 1], (8, 128))
                    pair = looked_up(lookup, chosen, block) + centre
                    pair_out[:, pl.ds(n * 128, 128)] = pair.astype(BF16)
            else:
                for n in range(2):
                    s = 2 * part + n
                    chosen = jnp.broadcast_to(owners[s : s + 1], (256, 128))
                    kept = jnp.where(rowblk[...] == chosen, found[:, n * 128 : (n + 1) * 128], 0.0)
                    masked_out[:, pl.ds(s * 128, 128)] = kept.astype(BF16)
        acc[late // 4] += total

    for unset in (masked_a, masked_b):
        unset[...] = jnp.zeros((256, 1024), BF16)
    for unset in (pair_a, pair_b):
        unset[...] = jnp.zeros((8, 256), BF16)
    for unset in (hid_a, hid_b):
        unset[...] = jnp.zeros((KH, 1024), BF16)

    def two_steps(tt, carry):
        step(2 * tt, masked_a, masked_b, pair_a, pair_b, hid_a, hid_b)
        step(2 * tt + 1, masked_b, masked_a, pair_b, pair_a, hid_b, hid_a)
        return carry

    def finish(slabs):
        for x in slabs:
            upper, lower = split_two(0.5 * acc[x])
            values = dot(kout_ref[...], upper) + dot(kout_ref[...], lower)
            latent = (values / valid_slots[x, 0:1]).astype(BF16)
            skip_ref[x] = dot_first(wskip_ref[...], latent)
            lat_ref[x] = latent.astype(F32)
        span = pl.ds(8 * slabs[0], 8 * len(slabs))
        for q in range(NZ):
            ready = lat_ref[slabs[0] : slabs[-1] + 1, pl.ds(8 * q, 8), :]
            s1[q, span, :] = ready.reshape(8 * len(slabs), 128).astype(BF16)
        r1[gz, span, :] = s1[gz, span, :]
        return span

    lax.fori_loop(0, 13, two_steps, 0)
    span = finish(range(6))
    for d in far_z:
        peer = along_z(d)
        send(0, s1.at[peer[2], span], r1.at[gz, span], peer)
    lax.fori_loop(13, CHUNKS // 2 + 1, two_steps, 0)
    span = finish(range(6, 8))
    for d in far_z:
        peer = along_z(d)
        send(8, s1.at[peer[2], span], r1.at[gz, span], peer)
    row, lane = iota((128, 128), 0), iota((128, 128), 1)
    row_i, lane_i = row // 8 % 8 * 2 + row // 64, lane // 8 % 8 * 2 + lane // 64
    mirror = (row % 8 == lane % 8) & (row_i != 8) & (lane_i == (16 - row_i) % 16)
    mirror = jnp.where(mirror, 1.0, 0.0).astype(BF16)
    row_j, lane_j = row // 16 * 2 + row // 4 % 2, lane // 16 * 2 + lane // 4 % 2
    flip = (row % 4 == 0) & (lane % 4 == 0) & (row // 8 % 2 == lane // 8 % 2)
    flip = flip & (lane_j != 8) & (row_j == (16 - lane_j) % 16)
    flip = jnp.where(flip, jnp.where(lane // 8 % 2 == 0, 1.0, -1.0), 0.0).astype(BF16)
    pick = jnp.where(iota((16, 128), 1) % 16 == iota((16, 128), 0), 1.0, 0.0).astype(BF16)
    own_channel = iota((64, 128), 0) % 8 == iota((64, 128), 1) // 16
    own_mode = iota((32, 1024), 1) // CH == iota((32, 1024), 0) % MODES
    for n in range(5, 10):
        fetch(n).wait()
    for n, span in ((0, pl.ds(0, 48)), (8, pl.ds(48, 16))):
        part = r1.at[pl.ds(0, NZ - 1), span]
        pltpu.make_async_copy(part, part, recv_sem.at[n]).wait()
    line = jnp.concatenate([r1[q] for q in range(NZ)], axis=1)
    deep = dot(line, fzh[...]) + dot(line, fzl[...])
    for q in range(NY):
        s2[q] = deep[:, q * 128 : (q + 1) * 128]
    for d in range(1, NY):
        peer = along_y(d)
        send(1, s2.at[peer[1]], r2.at[gy], peer)
    r2[gy] = s2[gy]
    arrived(1, r2, NY - 1)
    upper, lower = split_two(jnp.concatenate([r2[q] for q in range(NY)], axis=1))
    flat = dot(upper, fyh_ref[...]) + dot(upper, fyl_ref[...]) + dot(lower, fyh_ref[...])
    real = iota((64, 128), 1) // 8 % 2 == 0
    turned = jnp.where(real, pltpu.roll(flat, 120, axis=1), -pltpu.roll(flat, 8, axis=1))
    upper, lower = split_two(jnp.concatenate([flat, turned], axis=0))
    share = block_swap(dot(fxh[...], upper) + dot(fxl[...], upper) + dot(fxh[...], lower))
    for i in range(2):
        s4[:, i, :] = share[64 * i : 64 * i + 64]
    for peer in plane:
        send(2, s4.at[peer[2] * NX + peer[0]], r4.at[me], peer)
    r4[me] = s4[me]
    arrived(2, r4, 63)
    for q in range(NZ):
        pair = r4[q * NX]
        for n in range(1, NX):
            pair = pair + r4[q * NX + n]
        grid[pl.ds(2 * q, 2), :] = pair
    found = []
    for i in range(2):
        values = jnp.concatenate(
            [jnp.broadcast_to(grid[pl.ds(2 * q + i, 1), :], (8, 128)) for q in range(NZ)], axis=0
        )
        values = jnp.where(own_channel, values, 0.0).astype(BF16)
        found.append(
            lax.dot_general(
                pick,
                jnp.concatenate([values, values], axis=0),
                (((1,), (1,)), ((), ())),
                preferred_element_type=F32,
            )
        )
    rows = jnp.concatenate(
        [found[0][0:8], found[1][0:8], found[0][8:16], found[1][8:16]], axis=0
    )
    spread = jnp.where(own_mode, jnp.concatenate([rows] * 8, axis=1), 0.0).astype(BF16)
    by_real, by_imag = dot(spread, w_ref[0:1024]), dot(spread, w_ref[1024:2048])
    mixed_real = by_real[0:16] - by_imag[16:32]
    mixed_imag = by_imag[0:16] + by_real[16:32]
    for i in range(2):
        mine = jnp.concatenate(
            [mixed_real[8 * i : 8 * i + 8], mixed_imag[8 * i : 8 * i + 8]], axis=0
        ).astype(BF16)
        placed = jnp.where(own_channel, dot_first(mine, pick), 0.0).astype(BF16)
        s5[:, i, :] = dot(gather, placed)
    for peer in plane:
        send(3, s5.at[peer[2]], r5.at[me], peer)
    r5[me] = s5[gz]
    arrived(3, r5, 63)
    values = block_swap(jnp.concatenate([r5[:, i, :] for i in range(2)], axis=0))
    is_mean = (row < 8) & ((lane == 0) | (lane == 8)) & (gy == 0)
    values = jnp.where(is_mean, 0.0, values)
    exact = values.astype(BF16)
    real = lane // 8 % 2 == 0
    turned = jnp.where(real, -pltpu.roll(values, 120, axis=1), pltpu.roll(values, 8, axis=1))
    stacked = jnp.concatenate([exact, turned.astype(BF16)], axis=0)
    plain = (dot(ixh[...], stacked) + dot(ixl[...], stacked)).astype(BF16)
    flat = dot(plain, iyh_ref[...]) + dot(plain, iyl_ref[...])
    for q in range(NY):
        s7[q] = flat[:, q * 128 : (q + 1) * 128].astype(BF16)
    for d in range(1, NY):
        peer = along_y(d)
        send(4, s7.at[peer[1]], r7.at[gy], peer)
    r7[gy] = s7[gy]
    weight = jnp.where((lane % 4 == 0) & (gy == 0), 0.5, 2.0)
    pairs = dot(dot(mirror, exact).astype(BF16), flip)
    pairs = jnp.where(gy == 0, 0.5 * pairs, 0.0)
    power = jnp.sum(values * (weight * values + pairs), axis=1, keepdims=True)
    power = jnp.sum(power.reshape(16, 8, 1), axis=0)
    sv[...] = jnp.broadcast_to(power, (8, 128))
    for d in range(1, NY):
        send(5, sv, rv.at[gy], along_y(d))
    rv[gy] = sv[...]
    arrived(4, r7, NY - 1)
    line = jnp.concatenate([r7[q] for q in range(NY)], axis=1)
    depth = dot(line, iz[...])
    arrived(5, rv, NY - 1)
    power = (rv[0] + rv[1]) + (rv[2] + rv[3])
    scale = 1.0 / jnp.sqrt(power * (1.0 / float(GRID) ** 6) + 1.0)
    scale = jnp.concatenate([scale] * 8, axis=0)
    for q in range(NZ):
        s8[q] = (depth[:, q * 128 : (q + 1) * 128] * scale).astype(BF16)
    for d in far_z:
        peer = along_z(d)
        send(6, s8.at[peer[2]], r8.at[gz], peer)
    r8[gz] = s8[gz]
    arrived(6, r8, NZ - 1)
    wide[...] = r8[...].astype(F32)
    for x in range(8):
        out_ref[x] = gelu(wide[:, pl.ds(8 * x, 8), :].reshape(CH, 128) + skip_ref[x]).T
    for n, span in ((0, pl.ds(0, 48)), (8, pl.ds(48, 16))):
        part = r1.at[pl.ds(0, NZ - 1), span]
        pltpu.make_async_copy(part, part, send_sem.at[n]).wait()
    left(1, r2, NY - 1)
    left(2, r4, 63)
    left(3, r5, 63)
    left(4, r7, NY - 1)
    left(5, rv, NY - 1)
    left(6, r8, NZ - 1)
    left(7, around, 26)


def whole(points, counts, kin, kmid, kout, wskip, near, weights):
    fz, fy, fx, ix, iy, iz = transform_tables()
    tables = [wide_table(fz), *two_tables(fy), wide_table(fx), wide_table(ix)]
    tables += [*two_tables(iy), wide_table(iz)]
    vmem, anywhere = (pl.BlockSpec(memory_space=m) for m in (pltpu.VMEM, pl.ANY))
    v = pltpu.VMEM
    return pl.pallas_call(
        whole_kernel,
        out_shape=jax.ShapeDtypeStruct((8, 128, CH), F32),
        in_specs=[anywhere] * (8 + len(tables)),
        out_specs=vmem,
        scratch_shapes=[
            v((24, 128), F32), v((64, 16), jnp.int32), v((6, KH), BF16), v((KH, KH), BF16),
            v((CH, KH), BF16), v((CH, CH), BF16),
            v((8, 128, NB), jnp.int32), v((2048, CH), BF16),
            v((GRID, 512), F32), v((512, 128), BF16), v((512, 128), BF16),
            v((16, 128), F32), v((8, 256), F32), v((128, 512), BF16), v((128, 512), BF16),
            v((32, 1024), F32),
            v((27, 24, 128), F32), v((256, PTS), F32), v((256, PTS), BF16),
            v((CHUNKS, 8, 128), jnp.int32), v((CHUNKS, 8, 128), jnp.int32), v((8, 8, 128), F32),
            v((108, 8, 128), F32), v((8, 8, 128), F32), v((KH, 8), BF16),
            v((8, 256), BF16), v((8, 256), BF16),
            v((8, KH, 128), F32), v((256, 128), jnp.int32),
            v((KH, 256), BF16), v((KH, KH), BF16),
            v((256, 1024), BF16), v((256, 1024), BF16), v((KH, 1024), BF16), v((KH, 1024), BF16),
            v((8, KH, 128), F32), v((8, CH, 128), F32), v((8, CH, 128), F32),
            v((128, 128), BF16), v((128, 128), BF16), v((64, 256), BF16), v((64, 256), BF16),
            v((NZ, 64, 128), BF16), v((NZ, 64, 128), BF16),
            v((NY, 64, 128), F32), v((NY, 64, 128), F32),
            v((CH, 2, 128), F32), v((CH, 2, 128), F32),
            v((NZ, 2, 128), F32), v((CH, 2, 128), F32),
            v((NY, 64, 128), BF16), v((NY, 64, 128), BF16),
            v((8, 128), F32), v((NY, 8, 128), F32),
            v((NZ, 64, 128), BF16), v((NZ, 64, 128), BF16),
            v((1024, 512), BF16), v((1024, 512), BF16), v((512, 1024), BF16),
            v((MODES, 128), F32), v((NZ, 64, 128), F32),
            pltpu.SemaphoreType.DMA((9,)), pltpu.SemaphoreType.DMA((9,)),
            pltpu.SemaphoreType.DMA((16,)),
        ],
        compiler_params=pltpu.CompilerParams(collective_id=0, has_side_effects=True),
        name="whole",
    )(points, counts, kin, kmid, kout, wskip, near, weights, *tables)


def body(point_data, neighbours, counts, kernel_in, kernel_mid, kernel_out, spectral, skip_weight):
    out = whole(
        point_data.reshape(24, 128),
        jnp.swapaxes(counts[0], 1, 2).reshape(64, 16),
        kernel_in,
        kernel_mid,
        kernel_out.T,
        skip_weight,
        neighbours.reshape(8, 128, NB),
        spectral.reshape(2048, CH),
    )
    return out.reshape(1, 8, 16, 8, CH)


def solution(mesh):
    cells = P(None, "gx", "gy", "gz", None)
    return jax.shard_map(
        body,
        mesh=mesh,
        in_specs=(
            P(None, None, ("gx", "gy", "gz")),
            cells,
            P(None, "gx", "gy", "gz"),
            P(),
            P(),
            P(),
            P(None, "gz", "gx", "gy", None, None),
            P(),
        ),
        out_specs=cells,
        check_vma=False,
    )
```

```python
import functools
import math

import jax
import jax.numpy as jnp
import numpy as np
from jax import lax
from jax.experimental import pallas as pl
from jax.experimental.pallas import tpu as pltpu
from jax.sharding import PartitionSpec as P

GRID = 64
MODES = 16
NB = 32
KH = 80
CH = 64
PTS = 512
NX, NY, NZ = 8, 4, 8
F32 = jnp.float32
BF16 = jnp.bfloat16
MESH_ID = pl.DeviceIdType.MESH


def dot(a, b):
    return jnp.dot(a, b, preferred_element_type=F32)


def gelu(v):
    inner = v * (0.7978845608028654 + 0.035677408136300125 * (v * v))
    half = 0.5 * v
    return half + half * jnp.tanh(inner)


def split_two(values):
    upper = values.astype(BF16)
    return upper, (values - upper.astype(F32)).astype(BF16)


def dot_first(a, b):
    return lax.dot_general(a, b, (((0,), (0,)), ((), ())), preferred_element_type=F32)


def twice_gelu(v):
    v = v.astype(BF16)
    inner = v * (BF16(0.7978845608028654) + BF16(0.035677408136300125) * (v * v))
    return v + v * jnp.tanh(inner)


def looked_up(lookup, chosen, block):
    low = chosen & 127
    odd, upper = (chosen & 128) != 0, (chosen & 256) != 0
    bits = [(block & (1 << n)) != 0 for n in range(5)]

    def tile(n):
        return jnp.take_along_axis(lookup[n], low, axis=1, mode="promise_in_bounds")

    def tree(first, level):
        if level < 0:
            near, far = (
                jnp.where(odd, tile(4 * first + n + 1), tile(4 * first + n)) for n in (0, 2)
            )
            return jnp.where(upper, far, near)
        left = tree(first, level - 1)
        if first + (1 << level) >= 27:
            return left
        return jnp.where(bits[level], tree(first + (1 << level), level - 1), left)

    return tree(0, 4)


CHUNKS = 32
BY_LANES = (6, 7)
PART = 256


@functools.cache
def transform_tables():
    m = np.arange(GRID)
    centred = np.where(np.arange(MODES) < MODES // 2, np.arange(MODES), np.arange(MODES) - MODES)
    third = np.arange(MODES)

    def angles(f):
        return 2.0 * np.pi * ((f[:, None] * m[None, :]) % GRID) / GRID

    cos_c, sin_c = np.cos(angles(centred)), np.sin(angles(centred))
    cos_t, sin_t = np.cos(angles(third)), np.sin(angles(third))
    eye_k = np.eye(4)
    both = np.stack([cos_t, -sin_t], axis=-1)
    fz = np.broadcast_to(
        both.reshape(4, 4, GRID, 2).transpose(2, 0, 1, 3)[:, :, None], (GRID, 4, 16, 4, 2)
    ).reshape(GRID, 512)
    turn = np.stack([np.stack([cos_c, -sin_c], -1), np.stack([sin_c, cos_c], -1)], -2)
    fy = np.einsum("jcpyro,kl->pykrjocl", turn.reshape(8, 2, NY, 16, 2, 2), eye_k).reshape(512, 128)
    first = np.stack([cos_c, sin_c]).reshape(2, 8, 2, NX, 8)
    fx = np.broadcast_to(
        first.transpose(3, 2, 1, 0, 4)[..., None], (NX, 2, 8, 2, 8, 8)
    ).reshape(NX, 16, 128)
    ix = np.broadcast_to(
        first.transpose(3, 4, 0, 2, 1)[..., None], (NX, 8, 2, 2, 8, 8)
    ).reshape(NX, 8, 256)
    back = np.stack([np.stack([cos_c, sin_c], -1), np.stack([-sin_c, cos_c], -1)], -2)
    iy = np.einsum("jcqyro,kl->jrckqylo", back.reshape(8, 2, NY, 16, 2, 2), eye_k).reshape(128, 512)
    weight = np.where(third == 0, 1.0, 2.0)[:, None, None] / GRID**3
    iz = np.broadcast_to(
        (both * weight).transpose(0, 2, 1).reshape(32, NZ, 1, 8), (32, NZ, 16, 8)
    ).reshape(32, 1024)
    return fz, fy, fx, ix, iy, iz


def two_tables(table):
    import ml_dtypes

    upper = table.astype(np.float32).astype(ml_dtypes.bfloat16)
    lower = (table - upper.astype(np.float64)).astype(np.float32).astype(ml_dtypes.bfloat16)
    return jnp.asarray(upper), jnp.asarray(lower)


def wide_table(table):
    return jnp.asarray(np.ascontiguousarray(table, dtype=np.float32))


def iota(shape, dim):
    return lax.broadcasted_iota(jnp.int32, shape, dim)


def block_swap(x):
    row, lane = iota(x.shape, 0), iota(x.shape, 1) // 16
    for bit in (1, 2, 4):
        high, right = (row & bit) != 0, (lane & bit) != 0
        down = pltpu.roll(pltpu.roll(x, bit, axis=0), 128 - 16 * bit, axis=1)
        up = pltpu.roll(pltpu.roll(x, x.shape[0] - bit, axis=0), 16 * bit, axis=1)
        x = jnp.where(high == right, x, jnp.where(high, down, up))
    return x


def whole_kernel(
    pts_hbm, cnt_hbm, kin_hbm, kmid_hbm, kout_hbm, wskip_hbm, near_hbm, w_hbm, fzc_hbm, fyh_hbm, fyl_hbm, fxc_hbm, ixc_hbm, iyh_hbm, iyl_hbm, izc_hbm,
    out_ref,
    pts_ref, cnt_ref, kin_ref, kmid_ref, kout_ref, wskip_ref, near, w_ref, fzc_ref, fyh_ref, fyl_ref, fxc_ref, ixc_ref, iyh_ref, iyl_ref, izc_ref,
    around, table_rows, tab, slot_ids, block_ids, valid_slots,
    lookup, centres, win_few, pair_a, pair_b, pre, rowblk, win, wmid,
    masked_a, masked_b, hid_a, hid_b, acc, lat_ref, skip_ref, fxh, fxl, ixh, ixl,
    s1, r1, s2, r2, s4, r4, s5, r5, s7, r7, sv, rv, s8, r8, fzh, fzl, iz, grid, wide,
    send_sem, recv_sem, in_sem, heard,
):
    gx, gy, gz = lax.axis_index("gx"), lax.axis_index("gy"), lax.axis_index("gz")
    me = gz * NX + gx
    barrier = pltpu.get_barrier_semaphore()
    fetched = [
        (near_hbm, near), (fzc_hbm, fzc_ref), (fxc_hbm.at[gx], fxc_ref), (ixc_hbm.at[gx], ixc_ref),
        (izc_hbm, izc_ref), (fyh_hbm, fyh_ref), (fyl_hbm, fyl_ref), (iyh_hbm, iyh_ref),
        (iyl_hbm, iyl_ref), (w_hbm, w_ref), (kin_hbm, kin_ref), (kmid_hbm, kmid_ref),
        (cnt_hbm, cnt_ref), (pts_hbm, pts_ref), (kout_hbm, kout_ref), (wskip_hbm, wskip_ref),
    ]

    def fetch(n):
        return pltpu.make_async_copy(fetched[n][0], fetched[n][1], in_sem.at[n])

    for n in (13, 10, 11, 12, 0, 14, 15, *range(1, 10)):
        fetch(n).start()

    def along_y(d):
        return (gx, lax.rem(gy + d, NY), gz)

    def along_z(d):
        return (gx, gy, lax.rem(gz + d, NZ))

    far_z = (4, 3, 5, 2, 6, 1, 7)

    def beside(step):
        return tuple(lax.rem(p + d + n, n) for p, d, n in zip((gx, gy, gz), step, (NX, NY, NZ)))

    plane = [
        (lax.rem(gx + dx, NX), gy, lax.rem(gz + dz, NZ))
        for dx, dz in sorted(
            ((dx, dz) for dx in range(NX) for dz in range(NZ) if (dx, dz) != (0, 0)),
            key=lambda d: -2 * min(d[0], NX - d[0]) - min(d[1], NZ - d[1]),
        )
    ]
    steps = [
        (dx, dy, dz)
        for dx in (-1, 0, 1)
        for dy in (-1, 0, 1)
        for dz in (-1, 0, 1)
        if (dx, dy, dz) != (0, 0, 0)
    ]
    flat_steps = [s for s in steps if s[1] == 0]
    near_steps = flat_steps + [(0, -1, 0), (0, 1, 0)]

    def tell(n, whom):
        for s in whom:
            pl.semaphore_signal(
                heard.at[n], inc=1, device_id=beside(s), device_id_type=MESH_ID
            )

    for s in steps:
        pl.semaphore_signal(barrier, inc=1, device_id=beside(s), device_id_type=MESH_ID)

    for n in range(10, 16):
        fetch(n).wait()
    rowblk[...] = iota((256, 128), 0) // 9
    col = iota((6, 256), 1)
    nine = col % 9
    source = jnp.where(nine < 3, nine, nine - 3)
    chosen = jnp.where((source == iota((6, 256), 0)) & (col < 243), 1.0, 0.0).astype(BF16)
    win[...] = dot_first(kin_ref[...], chosen).astype(BF16)
    eye = jnp.where(iota((KH, KH), 0) == iota((KH, KH), 1), 0.5, 0.0).astype(BF16)
    wmid[...] = dot_first(kmid_ref[...], eye).astype(BF16)
    few = jnp.where(iota((6, 8), 0) == iota((6, 8), 1), 1.0, 0.0).astype(BF16)
    win_few[...] = dot_first(kin_ref[...], few).astype(BF16)
    row, lane = iota((8, 128), 0), iota((8, 128), 1)
    index_y, index_z = gy * 16 + lane // 8, gz * 8 + lane % 8
    for x in range(8):
        index = jnp.where(row == 0, gx * 8 + x, jnp.where(row == 1, index_y, index_z))
        centre = jnp.where(row < 3, -(index.astype(F32) + 0.5) / GRID, 0.0)
        centres[x] = centre
        pre[x] = dot_first(kin_ref[...], centre[0:6].astype(BF16))
    by_row = jnp.where(iota((16, 128), 1) // 8 == iota((16, 128), 0), 1.0, 0.0).astype(BF16)
    spread = dot(cnt_ref[...].astype(F32).astype(BF16), by_row)
    spread = jnp.where(iota((64, 128), 0) % 8 == iota((64, 128), 1) % 8, spread, 0.0)
    gather = jnp.where(iota((8, 64), 1) // 8 == iota((8, 64), 0), 1.0, 0.0).astype(BF16)
    spread = dot(gather, spread.astype(BF16))
    for x in range(8):
        valid_slots[x] = jnp.broadcast_to(spread[x : x + 1], (8, 128))
    acc[...] = jnp.zeros((8, KH, 128), F32)
    table_rows[pl.ds(240, 16), :] = jnp.zeros((16, PTS), F32)
    lookup[:, 6:8, :] = jnp.zeros((108, 2, 128), F32)
    pl.semaphore_wait(barrier, len(steps))
    tell(0, near_steps)

    def send(n, source, target, peer):
        pltpu.make_async_remote_copy(
            src_ref=source,
            dst_ref=target,
            send_sem=send_sem.at[n],
            recv_sem=recv_sem.at[n],
            device_id=peer,
            device_id_type=MESH_ID,
        ).start()

    def arrived(n, buffer, count):
        part = buffer.at[pl.ds(0, count)]
        pltpu.make_async_copy(part, part, recv_sem.at[n]).wait()

    def left(n, buffer, count):
        part = buffer.at[pl.ds(0, count)]
        pltpu.make_async_copy(part, part, send_sem.at[n]).wait()

    for step in steps:
        block = ((1 - step[0]) * 3 + (1 - step[1])) * 3 + (1 - step[2])
        send(7, pts_ref, around.at[block], beside(step))
    around[13] = pts_ref[...]
    fetch(0).wait()
    for x in range(8):
        point = near[x].T
        owner = point >> 9
        offset_z = (owner & 7) - gz + 1
        offset_y = ((owner >> 3) & 3) - gy + 1
        offset_x = (owner >> 5) - gx + 1
        block = (offset_x * 3 + offset_y) * 3 + offset_z
        block_ids[pl.ds(4 * x, 4)] = block.reshape(4, 8, 128)
        slot_ids[pl.ds(4 * x, 4)] = (point & 511).reshape(4, 8, 128)
    pl.semaphore_wait(heard.at[0], len(near_steps))
    tell(1, flat_steps)
    for n in range(1, 5):
        fetch(n).wait()
    own_y = iota((128, 512), 0) // 8 == iota((128, 512), 1) % 128 // 8
    for q in range(NZ):
        part = jnp.concatenate([fzc_ref[pl.ds(8 * q, 8), :]] * 16, axis=0)
        upper, lower = split_two(jnp.where(own_y, part, 0.0))
        fzh[pl.ds(128 * q, 128), :] = upper
        fzl[pl.ds(128 * q, 128), :] = lower
    own_y = iota((128, 1024), 0) // 8 == iota((128, 1024), 1) % 128 // 8
    for q in range(NY):
        part = jnp.concatenate([izc_ref[pl.ds(8 * q, 8), :]] * 16, axis=0)
        iz[pl.ds(128 * q, 128), :] = jnp.where(own_y, part, 0.0).astype(BF16)
    part = jnp.concatenate(
        [jnp.broadcast_to(fxc_ref[pl.ds(n, 1), :], (8, 128)) for n in range(16)], axis=0
    )
    row, lane = iota((128, 128), 0), iota((128, 128), 1)
    fxh[...], fxl[...] = split_two(jnp.where(row % 8 == lane % 8, part, 0.0))
    part = jnp.concatenate(
        [jnp.broadcast_to(ixc_ref[pl.ds(n, 1), :], (8, 256)) for n in range(8)], axis=0
    )
    ixh[...], ixl[...] = split_two(jnp.where(iota((64, 256), 0) % 8 == iota((64, 256), 1) % 8, part, 0.0))
    pl.semaphore_wait(heard.at[1], len(flat_steps))
    tell(2, flat_steps)
    arrived(7, around, 26)
    for b in range(27):
        for t in range(4):
            block = around[b, pl.ds(t, 6, stride=4), :]
            lookup[4 * b + t, 0:6, :] = block
            place = block[0:3]
            upper = place.astype(BF16).astype(F32)
            table_rows[pl.ds(9 * b, 9), pl.ds(128 * t, 128)] = jnp.concatenate(
                [upper, place - upper, block[3:6]], axis=0
            )
    tab[...] = table_rows[...].astype(BF16)
    low_ids = iota((64, 128), 0)

    def step(t, masked_out, masked_in, pair_out, pair_in, hid_out, hid_in):
        early = jnp.minimum(t, CHUNKS - 1)
        middle = jnp.clip(t - 1, 0, CHUNKS - 1)
        late = jnp.maximum(t - 2, 0)
        slots, owners = slot_ids[early], block_ids[early]
        centre = centres[early // 4]
        base = jnp.concatenate([pre[middle // 4]] * 2, axis=1)
        valid = jnp.where(t >= 2, valid_slots[late // 4], 0.0)[0:1]
        first = (late % 4 * 8).astype(F32)
        total = jnp.zeros((KH, 128), F32)
        for part in range(4):
            span = pl.ds(part * PART, PART)
            by_lanes = 2 * part in BY_LANES
            if by_lanes:
                ahead = dot(win_few[...], pair_in[...])
            else:
                hot = []
                for s in (2 * part, 2 * part + 1):
                    chosen = jnp.broadcast_to(slots[s : s + 1], (8, 128))
                    low = jnp.broadcast_to((chosen & 63)[0:1], (64, 128))
                    low = jnp.where(low == low_ids, 1.0, 0.0).astype(BF16)
                    high = chosen >> 6
                    for n in range(8):
                        here = jnp.where(high == n, 1.0, 0.0)
                        here = jnp.concatenate([here] * 8, axis=0).astype(BF16)
                        hot.append(low * here)
                hot = [jnp.concatenate(hot[:8], axis=0), jnp.concatenate(hot[8:], axis=0)]
                found = dot(tab[...], jnp.concatenate(hot, axis=1))
                ahead = dot(win[...], masked_in[:, span]) + base
            last = dot(wmid[...], hid_in[:, span])
            hid_out[:, span] = twice_gelu(ahead)
            last = twice_gelu(last).astype(F32)
            for n in range(2):
                used = valid > first + (2 * part + n)
                total = total + jnp.where(used, last[:, n * 128 : (n + 1) * 128], 0.0)
            if by_lanes:
                for n in range(2):
                    s = 2 * part + n
                    chosen = jnp.broadcast_to(slots[s : s + 1], (8, 128))
                    block = jnp.broadcast_to(owners[s : s + 1], (8, 128))
                    pair = looked_up(lookup, chosen, block) + centre
                    pair_out[:, pl.ds(n * 128, 128)] = pair.astype(BF16)
            else:
                for n in range(2):
                    s = 2 * part + n
                    chosen = jnp.broadcast_to(owners[s : s + 1], (256, 128))
                    kept = jnp.where(rowblk[...] == chosen, found[:, n * 128 : (n + 1) * 128], 0.0)
                    masked_out[:, pl.ds(s * 128, 128)] = kept.astype(BF16)
        acc[late // 4] += total

    for unset in (masked_a, masked_b):
        unset[...] = jnp.zeros((256, 1024), BF16)
    for unset in (pair_a, pair_b):
        unset[...] = jnp.zeros((8, 256), BF16)
    for unset in (hid_a, hid_b):
        unset[...] = jnp.zeros((KH, 1024), BF16)

    def two_steps(tt, carry):
        step(2 * tt, masked_a, masked_b, pair_a, pair_b, hid_a, hid_b)
        step(2 * tt + 1, masked_b, masked_a, pair_b, pair_a, hid_b, hid_a)
        return carry

    def finish(slabs):
        for x in slabs:
            upper, lower = split_two(0.5 * acc[x])
            values = dot(kout_ref[...], upper) + dot(kout_ref[...], lower)
            latent = (values / valid_slots[x, 0:1]).astype(BF16)
            skip_ref[x] = dot_first(wskip_ref[...], latent)
            lat_ref[x] = latent.astype(F32)
        span = pl.ds(8 * slabs[0], 8 * len(slabs))
        for q in range(NZ):
            ready = lat_ref[slabs[0] : slabs[-1] + 1, pl.ds(8 * q, 8), :]
            s1[q, span, :] = ready.reshape(8 * len(slabs), 128).astype(BF16)
        r1[gz, span, :] = s1[gz, span, :]
        return span

    lax.fori_loop(0, 13, two_steps, 0)
    span = finish(range(6))
    pl.semaphore_wait(heard.at[2], len(flat_steps))
    for d in far_z:
        peer = along_z(d)
        send(0, s1.at[peer[2], span], r1.at[gz, span], peer)
    lax.fori_loop(13, CHUNKS // 2 + 1, two_steps, 0)
    span = finish(range(6, 8))
    for d in far_z:
        peer = along_z(d)
        send(8, s1.at[peer[2], span], r1.at[gz, span], peer)
    row, lane = iota((128, 128), 0), iota((128, 128), 1)
    row_i, lane_i = row // 8 % 8 * 2 + row // 64, lane // 8 % 8 * 2 + lane // 64
    mirror = (row % 8 == lane % 8) & (row_i != 8) & (lane_i == (16 - row_i) % 16)
    mirror = jnp.where(mirror, 1.0, 0.0).astype(BF16)
    row_j, lane_j = row // 16 * 2 + row // 4 % 2, lane // 16 * 2 + lane // 4 % 2
    flip = (row % 4 == 0) & (lane % 4 == 0) & (row // 8 % 2 == lane // 8 % 2)
    flip = flip & (lane_j != 8) & (row_j == (16 - lane_j) % 16)
    flip = jnp.where(flip, jnp.where(lane // 8 % 2 == 0, 1.0, -1.0), 0.0).astype(BF16)
    pick = jnp.where(iota((16, 128), 1) % 16 == iota((16, 128), 0), 1.0, 0.0).astype(BF16)
    own_channel = iota((64, 128), 0) % 8 == iota((64, 128), 1) // 16
    own_mode = iota((32, 1024), 1) // CH == iota((32, 1024), 0) % MODES
    for n in range(5, 10):
        fetch(n).wait()
    for n, span in ((0, pl.ds(0, 48)), (8, pl.ds(48, 16))):
        part = r1.at[pl.ds(0, NZ - 1), span]
        pltpu.make_async_copy(part, part, recv_sem.at[n]).wait()
    line = jnp.concatenate([r1[q] for q in range(NZ)], axis=1)
    deep = dot(line, fzh[...]) + dot(line, fzl[...])
    for q in range(NY):
        s2[q] = deep[:, q * 128 : (q + 1) * 128]
    for d in range(1, NY):
        peer = along_y(d)
        send(1, s2.at[peer[1]], r2.at[gy], peer)
    r2[gy] = s2[gy]
    arrived(1, r2, NY - 1)
    upper, lower = split_two(jnp.concatenate([r2[q] for q in range(NY)], axis=1))
    flat = dot(upper, fyh_ref[...]) + dot(upper, fyl_ref[...]) + dot(lower, fyh_ref[...])
    real = iota((64, 128), 1) // 8 % 2 == 0
    turned = jnp.where(real, pltpu.roll(flat, 120, axis=1), -pltpu.roll(flat, 8, axis=1))
    upper, lower = split_two(jnp.concatenate([flat, turned], axis=0))
    share = block_swap(dot(fxh[...], upper) + dot(fxl[...], upper) + dot(fxh[...], lower))
    for i in range(2):
        s4[:, i, :] = share[64 * i : 64 * i + 64]
    for peer in plane:
        send(2, s4.at[peer[2] * NX + peer[0]], r4.at[me], peer)
    r4[me] = s4[me]
    arrived(2, r4, 63)
    for q in range(NZ):
        pair = r4[q * NX]
        for n in range(1, NX):
            pair = pair + r4[q * NX + n]
        grid[pl.ds(2 * q, 2), :] = pair
    found = []
    for i in range(2):
        values = jnp.concatenate(
            [jnp.broadcast_to(grid[pl.ds(2 * q + i, 1), :], (8, 128)) for q in range(NZ)], axis=0
        )
        values = jnp.where(own_channel, values, 0.0).astype(BF16)
        found.append(
            lax.dot_general(
                pick,
                jnp.concatenate([values, values], axis=0),
                (((1,), (1,)), ((), ())),
                preferred_element_type=F32,
            )
        )
    rows = jnp.concatenate(
        [found[0][0:8], found[1][0:8], found[0][8:16], found[1][8:16]], axis=0
    )
    spread = jnp.where(own_mode, jnp.concatenate([rows] * 8, axis=1), 0.0).astype(BF16)
    by_real, by_imag = dot(spread, w_ref[0:1024]), dot(spread, w_ref[1024:2048])
    mixed_real = by_real[0:16] - by_imag[16:32]
    mixed_imag = by_imag[0:16] + by_real[16:32]
    for i in range(2):
        mine = jnp.concatenate(
            [mixed_real[8 * i : 8 * i + 8], mixed_imag[8 * i : 8 * i + 8]], axis=0
        ).astype(BF16)
        placed = jnp.where(own_channel, dot_first(mine, pick), 0.0).astype(BF16)
        s5[:, i, :] = dot(gather, placed)
    for peer in plane:
        send(3, s5.at[peer[2]], r5.at[me], peer)
    r5[me] = s5[gz]
    arrived(3, r5, 63)
    values = block_swap(jnp.concatenate([r5[:, i, :] for i in range(2)], axis=0))
    is_mean = (row < 8) & ((lane == 0) | (lane == 8)) & (gy == 0)
    values = jnp.where(is_mean, 0.0, values)
    exact = values.astype(BF16)
    real = lane // 8 % 2 == 0
    turned = jnp.where(real, -pltpu.roll(values, 120, axis=1), pltpu.roll(values, 8, axis=1))
    stacked = jnp.concatenate([exact, turned.astype(BF16)], axis=0)
    plain = (dot(ixh[...], stacked) + dot(ixl[...], stacked)).astype(BF16)
    flat = dot(plain, iyh_ref[...]) + dot(plain, iyl_ref[...])
    for q in range(NY):
        s7[q] = flat[:, q * 128 : (q + 1) * 128].astype(BF16)
    for d in range(1, NY):
        peer = along_y(d)
        send(4, s7.at[peer[1]], r7.at[gy], peer)
    r7[gy] = s7[gy]
    weight = jnp.where((lane % 4 == 0) & (gy == 0), 0.5, 2.0)
    pairs = dot(dot(mirror, exact).astype(BF16), flip)
    pairs = jnp.where(gy == 0, 0.5 * pairs, 0.0)
    power = jnp.sum(values * (weight * values + pairs), axis=1, keepdims=True)
    power = jnp.sum(power.reshape(16, 8, 1), axis=0)
    sv[...] = jnp.broadcast_to(power, (8, 128))
    for d in range(1, NY):
        send(5, sv, rv.at[gy], along_y(d))
    rv[gy] = sv[...]
    arrived(4, r7, NY - 1)
    line = jnp.concatenate([r7[q] for q in range(NY)], axis=1)
    depth = dot(line, iz[...])
    arrived(5, rv, NY - 1)
    power = (rv[0] + rv[1]) + (rv[2] + rv[3])
    scale = 1.0 / jnp.sqrt(power * (1.0 / float(GRID) ** 6) + 1.0)
    scale = jnp.concatenate([scale] * 8, axis=0)
    for q in range(NZ):
        s8[q] = (depth[:, q * 128 : (q + 1) * 128] * scale).astype(BF16)
    for d in far_z:
        peer = along_z(d)
        send(6, s8.at[peer[2]], r8.at[gz], peer)
    r8[gz] = s8[gz]
    arrived(6, r8, NZ - 1)
    wide[...] = r8[...].astype(F32)
    for x in range(8):
        out_ref[x] = gelu(wide[:, pl.ds(8 * x, 8), :].reshape(CH, 128) + skip_ref[x]).T
    for n, span in ((0, pl.ds(0, 48)), (8, pl.ds(48, 16))):
        part = r1.at[pl.ds(0, NZ - 1), span]
        pltpu.make_async_copy(part, part, send_sem.at[n]).wait()
    left(1, r2, NY - 1)
    left(2, r4, 63)
    left(3, r5, 63)
    left(4, r7, NY - 1)
    left(5, rv, NY - 1)
    left(6, r8, NZ - 1)
    left(7, around, 26)


def whole(points, counts, kin, kmid, kout, wskip, near, weights):
    fz, fy, fx, ix, iy, iz = transform_tables()
    tables = [wide_table(fz), *two_tables(fy), wide_table(fx), wide_table(ix)]
    tables += [*two_tables(iy), wide_table(iz)]
    vmem, anywhere = (pl.BlockSpec(memory_space=m) for m in (pltpu.VMEM, pl.ANY))
    v = pltpu.VMEM
    return pl.pallas_call(
        whole_kernel,
        out_shape=jax.ShapeDtypeStruct((8, 128, CH), F32),
        in_specs=[anywhere] * (8 + len(tables)),
        out_specs=vmem,
        scratch_shapes=[
            v((24, 128), F32), v((64, 16), jnp.int32), v((6, KH), BF16), v((KH, KH), BF16),
            v((CH, KH), BF16), v((CH, CH), BF16),
            v((8, 128, NB), jnp.int32), v((2048, CH), BF16),
            v((GRID, 512), F32), v((512, 128), BF16), v((512, 128), BF16),
            v((16, 128), F32), v((8, 256), F32), v((128, 512), BF16), v((128, 512), BF16),
            v((32, 1024), F32),
            v((27, 24, 128), F32), v((256, PTS), F32), v((256, PTS), BF16),
            v((CHUNKS, 8, 128), jnp.int32), v((CHUNKS, 8, 128), jnp.int32), v((8, 8, 128), F32),
            v((108, 8, 128), F32), v((8, 8, 128), F32), v((KH, 8), BF16),
            v((8, 256), BF16), v((8, 256), BF16),
            v((8, KH, 128), F32), v((256, 128), jnp.int32),
            v((KH, 256), BF16), v((KH, KH), BF16),
            v((256, 1024), BF16), v((256, 1024), BF16), v((KH, 1024), BF16), v((KH, 1024), BF16),
            v((8, KH, 128), F32), v((8, CH, 128), F32), v((8, CH, 128), F32),
            v((128, 128), BF16), v((128, 128), BF16), v((64, 256), BF16), v((64, 256), BF16),
            v((NZ, 64, 128), BF16), v((NZ, 64, 128), BF16),
            v((NY, 64, 128), F32), v((NY, 64, 128), F32),
            v((CH, 2, 128), F32), v((CH, 2, 128), F32),
            v((NZ, 2, 128), F32), v((CH, 2, 128), F32),
            v((NY, 64, 128), BF16), v((NY, 64, 128), BF16),
            v((8, 128), F32), v((NY, 8, 128), F32),
            v((NZ, 64, 128), BF16), v((NZ, 64, 128), BF16),
            v((1024, 512), BF16), v((1024, 512), BF16), v((512, 1024), BF16),
            v((MODES, 128), F32), v((NZ, 64, 128), F32),
            pltpu.SemaphoreType.DMA((9,)), pltpu.SemaphoreType.DMA((9,)),
            pltpu.SemaphoreType.DMA((16,)), pltpu.SemaphoreType.REGULAR((3,)),
        ],
        compiler_params=pltpu.CompilerParams(collective_id=0, has_side_effects=True),
        name="whole",
    )(points, counts, kin, kmid, kout, wskip, near, weights, *tables)


def body(point_data, neighbours, counts, kernel_in, kernel_mid, kernel_out, spectral, skip_weight):
    out = whole(
        point_data.reshape(24, 128),
        jnp.swapaxes(counts[0], 1, 2).reshape(64, 16),
        kernel_in,
        kernel_mid,
        kernel_out.T,
        skip_weight,
        neighbours.reshape(8, 128, NB),
        spectral.reshape(2048, CH),
    )
    return out.reshape(1, 8, 16, 8, CH)


def solution(mesh):
    cells = P(None, "gx", "gy", "gz", None)
    return jax.shard_map(
        body,
        mesh=mesh,
        in_specs=(
            P(None, None, ("gx", "gy", "gz")),
            cells,
            P(None, "gx", "gy", "gz"),
            P(),
            P(),
            P(),
            P(None, "gz", "gx", "gy", None, None),
            P(),
        ),
        out_specs=cells,
        check_vma=False,
    )
```

```python
import functools
import math

import jax
import jax.numpy as jnp
import numpy as np
from jax import lax
from jax.experimental import pallas as pl
from jax.experimental.pallas import tpu as pltpu
from jax.sharding import PartitionSpec as P

GRID = 64
MODES = 16
NB = 32
KH = 80
CH = 64
PTS = 512
NX, NY, NZ = 8, 4, 8
F32 = jnp.float32
BF16 = jnp.bfloat16
MESH_ID = pl.DeviceIdType.MESH


def dot(a, b):
    return jnp.dot(a, b, preferred_element_type=F32)


def gelu(v):
    inner = v * (0.7978845608028654 + 0.035677408136300125 * (v * v))
    half = 0.5 * v
    return half + half * jnp.tanh(inner)


def split_two(values):
    upper = values.astype(BF16)
    return upper, (values - upper.astype(F32)).astype(BF16)


def dot_first(a, b):
    return lax.dot_general(a, b, (((0,), (0,)), ((), ())), preferred_element_type=F32)


def twice_gelu(v):
    v = v.astype(BF16)
    inner = v * (BF16(0.7978845608028654) + BF16(0.035677408136300125) * (v * v))
    return v + v * jnp.tanh(inner)


def looked_up(lookup, chosen, block):
    low = chosen & 127
    odd, upper = (chosen & 128) != 0, (chosen & 256) != 0
    bits = [(block & (1 << n)) != 0 for n in range(5)]

    def tile(n):
        return jnp.take_along_axis(lookup[n], low, axis=1, mode="promise_in_bounds")

    def tree(first, level):
        if level < 0:
            near, far = (
                jnp.where(odd, tile(4 * first + n + 1), tile(4 * first + n)) for n in (0, 2)
            )
            return jnp.where(upper, far, near)
        left = tree(first, level - 1)
        if first + (1 << level) >= 27:
            return left
        return jnp.where(bits[level], tree(first + (1 << level), level - 1), left)

    return tree(0, 4)


CHUNKS = 32
BY_LANES = (6, 7)
PART = 256
ROWS = 176


@functools.cache
def transform_tables():
    m = np.arange(GRID)
    centred = np.where(np.arange(MODES) < MODES // 2, np.arange(MODES), np.arange(MODES) - MODES)
    third = np.arange(MODES)

    def angles(f):
        return 2.0 * np.pi * ((f[:, None] * m[None, :]) % GRID) / GRID

    cos_c, sin_c = np.cos(angles(centred)), np.sin(angles(centred))
    cos_t, sin_t = np.cos(angles(third)), np.sin(angles(third))
    eye_k = np.eye(4)
    both = np.stack([cos_t, -sin_t], axis=-1)
    fz = np.broadcast_to(
        both.reshape(4, 4, GRID, 2).transpose(2, 0, 1, 3)[:, :, None], (GRID, 4, 16, 4, 2)
    ).reshape(GRID, 512)
    turn = np.stack([np.stack([cos_c, -sin_c], -1), np.stack([sin_c, cos_c], -1)], -2)
    fy = np.einsum("jcpyro,kl->pykrjocl", turn.reshape(8, 2, NY, 16, 2, 2), eye_k).reshape(512, 128)
    first = np.stack([cos_c, sin_c]).reshape(2, 8, 2, NX, 8)
    fx = np.broadcast_to(
        first.transpose(3, 2, 1, 0, 4)[..., None], (NX, 2, 8, 2, 8, 8)
    ).reshape(NX, 16, 128)
    ix = np.broadcast_to(
        first.transpose(3, 4, 0, 2, 1)[..., None], (NX, 8, 2, 2, 8, 8)
    ).reshape(NX, 8, 256)
    back = np.stack([np.stack([cos_c, sin_c], -1), np.stack([-sin_c, cos_c], -1)], -2)
    iy = np.einsum("jcqyro,kl->jrckqylo", back.reshape(8, 2, NY, 16, 2, 2), eye_k).reshape(128, 512)
    weight = np.where(third == 0, 1.0, 2.0)[:, None, None] / GRID**3
    iz = np.broadcast_to(
        (both * weight).transpose(0, 2, 1).reshape(32, NZ, 1, 8), (32, NZ, 16, 8)
    ).reshape(32, 1024)
    return fz, fy, fx, ix, iy, iz


def two_tables(table):
    import ml_dtypes

    upper = table.astype(np.float32).astype(ml_dtypes.bfloat16)
    lower = (table - upper.astype(np.float64)).astype(np.float32).astype(ml_dtypes.bfloat16)
    return jnp.asarray(upper), jnp.asarray(lower)


def wide_table(table):
    return jnp.asarray(np.ascontiguousarray(table, dtype=np.float32))


def iota(shape, dim):
    return lax.broadcasted_iota(jnp.int32, shape, dim)


def block_swap(x):
    row, lane = iota(x.shape, 0), iota(x.shape, 1) // 16
    for bit in (1, 2, 4):
        high, right = (row & bit) != 0, (lane & bit) != 0
        down = pltpu.roll(pltpu.roll(x, bit, axis=0), 128 - 16 * bit, axis=1)
        up = pltpu.roll(pltpu.roll(x, x.shape[0] - bit, axis=0), 16 * bit, axis=1)
        x = jnp.where(high == right, x, jnp.where(high, down, up))
    return x


def whole_kernel(
    pts_hbm, cnt_hbm, kin_hbm, kmid_hbm, kout_hbm, wskip_hbm, near_hbm, w_hbm, fzc_hbm, fyh_hbm, fyl_hbm, fxc_hbm, ixc_hbm, iyh_hbm, iyl_hbm, izc_hbm,
    out_ref,
    pts_ref, cnt_ref, kin_ref, kmid_ref, kout_ref, wskip_ref, near, w_ref, fzc_ref, fyh_ref, fyl_ref, fxc_ref, ixc_ref, iyh_ref, iyl_ref, izc_ref,
    around, table_rows, tab, slot_ids, block_ids, valid_slots,
    lookup, centres, win_few, pair_a, pair_b, pre, rowblk, win, wmid,
    masked_a, masked_b, hid_a, hid_b, acc, lat_ref, skip_ref, fxh, fxl, ixh, ixl,
    s1, r1, s2, r2, s4, r4, s5, r5, s7, r7, sv, rv, s8, r8, fzh, fzl, iz, grid, wide,
    result, send_sem, recv_sem, in_sem, heard, out_sem,
):
    gx, gy, gz = lax.axis_index("gx"), lax.axis_index("gy"), lax.axis_index("gz")
    me = gz * NX + gx
    barrier = pltpu.get_barrier_semaphore()
    fetched = [
        (near_hbm, near), (fzc_hbm, fzc_ref), (fxc_hbm.at[gx], fxc_ref), (ixc_hbm.at[gx], ixc_ref),
        (izc_hbm, izc_ref), (fyh_hbm, fyh_ref), (fyl_hbm, fyl_ref), (iyh_hbm, iyh_ref),
        (iyl_hbm, iyl_ref), (w_hbm, w_ref), (kin_hbm, kin_ref), (kmid_hbm, kmid_ref),
        (cnt_hbm, cnt_ref), (pts_hbm, pts_ref), (kout_hbm, kout_ref), (wskip_hbm, wskip_ref),
    ]

    def fetch(n):
        return pltpu.make_async_copy(fetched[n][0], fetched[n][1], in_sem.at[n])

    for n in (13, 10, 11, 12, 0, 14, 15, *range(1, 10)):
        fetch(n).start()

    def along_y(d):
        return (gx, lax.rem(gy + d, NY), gz)

    def along_z(d):
        return (gx, gy, lax.rem(gz + d, NZ))

    far_z = (4, 3, 5, 2, 6, 1, 7)

    def beside(step):
        return tuple(lax.rem(p + d + n, n) for p, d, n in zip((gx, gy, gz), step, (NX, NY, NZ)))

    plane = [
        (lax.rem(gx + dx, NX), gy, lax.rem(gz + dz, NZ))
        for dx, dz in sorted(
            ((dx, dz) for dx in range(NX) for dz in range(NZ) if (dx, dz) != (0, 0)),
            key=lambda d: -2 * min(d[0], NX - d[0]) - min(d[1], NZ - d[1]),
        )
    ]
    steps = [
        (dx, dy, dz)
        for dx in (-1, 0, 1)
        for dy in (-1, 0, 1)
        for dz in (-1, 0, 1)
        if (dx, dy, dz) != (0, 0, 0)
    ]
    flat_steps = [s for s in steps if s[1] == 0]
    near_steps = flat_steps + [(0, -1, 0), (0, 1, 0)]

    def tell(n, whom):
        for s in whom:
            pl.semaphore_signal(
                heard.at[n], inc=1, device_id=beside(s), device_id_type=MESH_ID
            )

    for s in steps:
        pl.semaphore_signal(barrier, inc=1, device_id=beside(s), device_id_type=MESH_ID)

    for n in range(10, 16):
        fetch(n).wait()
    rowblk[...] = iota((ROWS, 128), 0) // 6
    col = iota((6, ROWS), 1)
    chosen = (col % 6 == iota((6, ROWS), 0)) & (col < 162)
    chosen = jnp.where(chosen, 1.0, 0.0).astype(BF16)
    win[...] = dot_first(kin_ref[...], chosen).astype(BF16)
    eye = jnp.where(iota((KH, KH), 0) == iota((KH, KH), 1), 0.5, 0.0).astype(BF16)
    wmid[...] = dot_first(kmid_ref[...], eye).astype(BF16)
    few = jnp.where(iota((6, 8), 0) == iota((6, 8), 1), 1.0, 0.0).astype(BF16)
    win_few[...] = dot_first(kin_ref[...], few).astype(BF16)
    row, lane = iota((8, 128), 0), iota((8, 128), 1)
    index_y, index_z = lane // 8 - 8, lane % 8 - 4
    for x in range(8):
        index = jnp.where(row == 0, x - 4, jnp.where(row == 1, index_y, index_z))
        centre = jnp.where(row < 3, -(index.astype(F32) + 0.5) / GRID, 0.0)
        centres[x] = centre
        pre[x] = dot_first(kin_ref[...], centre[0:6].astype(BF16))
    by_row = jnp.where(iota((16, 128), 1) // 8 == iota((16, 128), 0), 1.0, 0.0).astype(BF16)
    spread = dot(cnt_ref[...].astype(F32).astype(BF16), by_row)
    spread = jnp.where(iota((64, 128), 0) % 8 == iota((64, 128), 1) % 8, spread, 0.0)
    gather = jnp.where(iota((8, 64), 1) // 8 == iota((8, 64), 0), 1.0, 0.0).astype(BF16)
    spread = dot(gather, spread.astype(BF16))
    for x in range(8):
        valid_slots[x] = jnp.broadcast_to(spread[x : x + 1], (8, 128))
    acc[...] = jnp.zeros((8, KH, 128), F32)
    table_rows[pl.ds(ROWS - 16, 16), :] = jnp.zeros((16, PTS), F32)
    row = iota((6, 128), 0)
    middle = jnp.where(row == 0, gx * 8 + 4, jnp.where(row == 1, gy * 16 + 8, gz * 8 + 4))
    middle = jnp.where(row < 3, middle.astype(F32) / GRID, 0.0)
    lookup[:, 6:8, :] = jnp.zeros((108, 2, 128), F32)
    pl.semaphore_wait(barrier, len(steps))
    tell(0, near_steps)

    def send(n, source, target, peer):
        pltpu.make_async_remote_copy(
            src_ref=source,
            dst_ref=target,
            send_sem=send_sem.at[n],
            recv_sem=recv_sem.at[n],
            device_id=peer,
            device_id_type=MESH_ID,
        ).start()

    def arrived(n, buffer, count):
        part = buffer.at[pl.ds(0, count)]
        pltpu.make_async_copy(part, part, recv_sem.at[n]).wait()

    def left(n, buffer, count):
        part = buffer.at[pl.ds(0, count)]
        pltpu.make_async_copy(part, part, send_sem.at[n]).wait()

    for step in steps:
        block = ((1 - step[0]) * 3 + (1 - step[1])) * 3 + (1 - step[2])
        send(7, pts_ref, around.at[block], beside(step))
    around[13] = pts_ref[...]
    fetch(0).wait()
    for x in range(8):
        point = near[x].T
        owner = point >> 9
        offset_z = (owner & 7) - gz + 1
        offset_y = ((owner >> 3) & 3) - gy + 1
        offset_x = (owner >> 5) - gx + 1
        block = (offset_x * 3 + offset_y) * 3 + offset_z
        block_ids[pl.ds(4 * x, 4)] = block.reshape(4, 8, 128)
        slot_ids[pl.ds(4 * x, 4)] = (point & 511).reshape(4, 8, 128)
    pl.semaphore_wait(heard.at[0], len(near_steps))
    tell(1, flat_steps)
    for n in range(1, 5):
        fetch(n).wait()
    own_y = iota((128, 512), 0) // 8 == iota((128, 512), 1) % 128 // 8
    for q in range(NZ):
        part = jnp.concatenate([fzc_ref[pl.ds(8 * q, 8), :]] * 16, axis=0)
        upper, lower = split_two(jnp.where(own_y, part, 0.0))
        fzh[pl.ds(128 * q, 128), :] = upper
        fzl[pl.ds(128 * q, 128), :] = lower
    own_y = iota((128, 1024), 0) // 8 == iota((128, 1024), 1) % 128 // 8
    for q in range(NY):
        part = jnp.concatenate([izc_ref[pl.ds(8 * q, 8), :]] * 16, axis=0)
        iz[pl.ds(128 * q, 128), :] = jnp.where(own_y, part, 0.0).astype(BF16)
    part = jnp.concatenate(
        [jnp.broadcast_to(fxc_ref[pl.ds(n, 1), :], (8, 128)) for n in range(16)], axis=0
    )
    row, lane = iota((128, 128), 0), iota((128, 128), 1)
    fxh[...], fxl[...] = split_two(jnp.where(row % 8 == lane % 8, part, 0.0))
    part = jnp.concatenate(
        [jnp.broadcast_to(ixc_ref[pl.ds(n, 1), :], (8, 256)) for n in range(8)], axis=0
    )
    ixh[...], ixl[...] = split_two(jnp.where(iota((64, 256), 0) % 8 == iota((64, 256), 1) % 8, part, 0.0))
    pl.semaphore_wait(heard.at[1], len(flat_steps))
    tell(2, flat_steps)
    arrived(7, around, 26)
    for b in range(27):
        for t in range(4):
            block = around[b, pl.ds(t, 6, stride=4), :] - middle
            lookup[4 * b + t, 0:6, :] = block
            table_rows[pl.ds(6 * b, 6), pl.ds(128 * t, 128)] = block
    tab[...] = table_rows[...].astype(BF16)
    low_ids = iota((64, 128), 0)

    def step(t, masked_out, masked_in, pair_out, pair_in, hid_out, hid_in):
        early = jnp.minimum(t, CHUNKS - 1)
        middle = jnp.clip(t - 1, 0, CHUNKS - 1)
        late = jnp.maximum(t - 2, 0)
        slots, owners = slot_ids[early], block_ids[early]
        centre = centres[early // 4]
        base = jnp.concatenate([pre[middle // 4]] * 2, axis=1)
        valid = jnp.where(t >= 2, valid_slots[late // 4], 0.0)[0:1]
        first = (late % 4 * 8).astype(F32)
        total = jnp.zeros((KH, 128), F32)
        for part in range(4):
            span = pl.ds(part * PART, PART)
            by_lanes = 2 * part in BY_LANES
            if by_lanes:
                ahead = dot(win_few[...], pair_in[...])
            else:
                hot = []
                for s in (2 * part, 2 * part + 1):
                    chosen = jnp.broadcast_to(slots[s : s + 1], (8, 128))
                    low = jnp.broadcast_to((chosen & 63)[0:1], (64, 128))
                    low = jnp.where(low == low_ids, 1.0, 0.0).astype(BF16)
                    high = chosen >> 6
                    for n in range(8):
                        here = jnp.where(high == n, 1.0, 0.0)
                        here = jnp.concatenate([here] * 8, axis=0).astype(BF16)
                        hot.append(low * here)
                hot = [jnp.concatenate(hot[:8], axis=0), jnp.concatenate(hot[8:], axis=0)]
                found = dot(tab[...], jnp.concatenate(hot, axis=1))
                ahead = dot(win[...], masked_in[:, span]) + base
            last = dot(wmid[...], hid_in[:, span])
            hid_out[:, span] = twice_gelu(ahead)
            last = twice_gelu(last).astype(F32)
            for n in range(2):
                used = valid > first + (2 * part + n)
                total = total + jnp.where(used, last[:, n * 128 : (n + 1) * 128], 0.0)
            if by_lanes:
                for n in range(2):
                    s = 2 * part + n
                    chosen = jnp.broadcast_to(slots[s : s + 1], (8, 128))
                    block = jnp.broadcast_to(owners[s : s + 1], (8, 128))
                    pair = looked_up(lookup, chosen, block) + centre
                    pair_out[:, pl.ds(n * 128, 128)] = pair.astype(BF16)
            else:
                for n in range(2):
                    s = 2 * part + n
                    chosen = jnp.broadcast_to(owners[s : s + 1], (ROWS, 128))
                    kept = jnp.where(rowblk[...] == chosen, found[:, n * 128 : (n + 1) * 128], 0.0)
                    masked_out[:, pl.ds(s * 128, 128)] = kept.astype(BF16)
        acc[late // 4] += total

    for unset in (masked_a, masked_b):
        unset[...] = jnp.zeros((ROWS, 1024), BF16)
    for unset in (pair_a, pair_b):
        unset[...] = jnp.zeros((8, 256), BF16)
    for unset in (hid_a, hid_b):
        unset[...] = jnp.zeros((KH, 1024), BF16)

    def two_steps(tt, carry):
        step(2 * tt, masked_a, masked_b, pair_a, pair_b, hid_a, hid_b)
        step(2 * tt + 1, masked_b, masked_a, pair_b, pair_a, hid_b, hid_a)
        return carry

    def finish(slabs):
        for x in slabs:
            upper, lower = split_two(0.5 * acc[x])
            values = dot(kout_ref[...], upper) + dot(kout_ref[...], lower)
            latent = (values / valid_slots[x, 0:1]).astype(BF16)
            skip_ref[x] = dot_first(wskip_ref[...], latent)
            lat_ref[x] = latent.astype(F32)
        span = pl.ds(8 * slabs[0], 8 * len(slabs))
        for q in range(NZ):
            ready = lat_ref[slabs[0] : slabs[-1] + 1, pl.ds(8 * q, 8), :]
            s1[q, span, :] = ready.reshape(8 * len(slabs), 128).astype(BF16)
        r1[gz, span, :] = s1[gz, span, :]
        return span

    lax.fori_loop(0, 13, two_steps, 0)
    span = finish(range(6))
    pl.semaphore_wait(heard.at[2], len(flat_steps))
    for d in far_z:
        peer = along_z(d)
        send(0, s1.at[peer[2], span], r1.at[gz, span], peer)
    lax.fori_loop(13, CHUNKS // 2 + 1, two_steps, 0)
    span = finish(range(6, 8))
    for d in far_z:
        peer = along_z(d)
        send(8, s1.at[peer[2], span], r1.at[gz, span], peer)
    row, lane = iota((128, 128), 0), iota((128, 128), 1)
    row_i, lane_i = row // 8 % 8 * 2 + row // 64, lane // 8 % 8 * 2 + lane // 64
    mirror = (row % 8 == lane % 8) & (row_i != 8) & (lane_i == (16 - row_i) % 16)
    mirror = jnp.where(mirror, 1.0, 0.0).astype(BF16)
    row_j, lane_j = row // 16 * 2 + row // 4 % 2, lane // 16 * 2 + lane // 4 % 2
    flip = (row % 4 == 0) & (lane % 4 == 0) & (row // 8 % 2 == lane // 8 % 2)
    flip = flip & (lane_j != 8) & (row_j == (16 - lane_j) % 16)
    flip = jnp.where(flip, jnp.where(lane // 8 % 2 == 0, 1.0, -1.0), 0.0).astype(BF16)
    pick = jnp.where(iota((16, 128), 1) % 16 == iota((16, 128), 0), 1.0, 0.0).astype(BF16)
    own_channel = iota((64, 128), 0) % 8 == iota((64, 128), 1) // 16
    own_mode = iota((32, 1024), 1) // CH == iota((32, 1024), 0) % MODES
    for n in range(5, 10):
        fetch(n).wait()
    for n, span in ((0, pl.ds(0, 48)), (8, pl.ds(48, 16))):
        part = r1.at[pl.ds(0, NZ - 1), span]
        pltpu.make_async_copy(part, part, recv_sem.at[n]).wait()
    line = jnp.concatenate([r1[q] for q in range(NZ)], axis=1)
    deep = dot(line, fzh[...]) + dot(line, fzl[...])
    for q in range(NY):
        s2[q] = deep[:, q * 128 : (q + 1) * 128]
    for d in range(1, NY):
        peer = along_y(d)
        send(1, s2.at[peer[1]], r2.at[gy], peer)
    r2[gy] = s2[gy]
    arrived(1, r2, NY - 1)
    upper, lower = split_two(jnp.concatenate([r2[q] for q in range(NY)], axis=1))
    flat = dot(upper, fyh_ref[...]) + dot(upper, fyl_ref[...]) + dot(lower, fyh_ref[...])
    real = iota((64, 128), 1) // 8 % 2 == 0
    turned = jnp.where(real, pltpu.roll(flat, 120, axis=1), -pltpu.roll(flat, 8, axis=1))
    upper, lower = split_two(jnp.concatenate([flat, turned], axis=0))
    share = block_swap(dot(fxh[...], upper) + dot(fxl[...], upper) + dot(fxh[...], lower))
    for i in range(2):
        s4[:, i, :] = share[64 * i : 64 * i + 64]
    for peer in plane:
        send(2, s4.at[peer[2] * NX + peer[0]], r4.at[me], peer)
    r4[me] = s4[me]
    arrived(2, r4, 63)
    for q in range(NZ):
        pair = r4[q * NX]
        for n in range(1, NX):
            pair = pair + r4[q * NX + n]
        grid[pl.ds(2 * q, 2), :] = pair
    found = []
    for i in range(2):
        values = jnp.concatenate(
            [jnp.broadcast_to(grid[pl.ds(2 * q + i, 1), :], (8, 128)) for q in range(NZ)], axis=0
        )
        values = jnp.where(own_channel, values, 0.0).astype(BF16)
        found.append(
            lax.dot_general(
                pick,
                jnp.concatenate([values, values], axis=0),
                (((1,), (1,)), ((), ())),
                preferred_element_type=F32,
            )
        )
    rows = jnp.concatenate(
        [found[0][0:8], found[1][0:8], found[0][8:16], found[1][8:16]], axis=0
    )
    spread = jnp.where(own_mode, jnp.concatenate([rows] * 8, axis=1), 0.0).astype(BF16)
    by_real, by_imag = dot(spread, w_ref[0:1024]), dot(spread, w_ref[1024:2048])
    mixed_real = by_real[0:16] - by_imag[16:32]
    mixed_imag = by_imag[0:16] + by_real[16:32]
    for i in range(2):
        mine = jnp.concatenate(
            [mixed_real[8 * i : 8 * i + 8], mixed_imag[8 * i : 8 * i + 8]], axis=0
        ).astype(BF16)
        placed = jnp.where(own_channel, dot_first(mine, pick), 0.0).astype(BF16)
        s5[:, i, :] = dot(gather, placed)
    for peer in plane:
        send(3, s5.at[peer[2]], r5.at[me], peer)
    r5[me] = s5[gz]
    arrived(3, r5, 63)
    values = block_swap(jnp.concatenate([r5[:, i, :] for i in range(2)], axis=0))
    is_mean = (row < 8) & ((lane == 0) | (lane == 8)) & (gy == 0)
    values = jnp.where(is_mean, 0.0, values)
    exact = values.astype(BF16)
    real = lane // 8 % 2 == 0
    turned = jnp.where(real, -pltpu.roll(values, 120, axis=1), pltpu.roll(values, 8, axis=1))
    stacked = jnp.concatenate([exact, turned.astype(BF16)], axis=0)
    plain = (dot(ixh[...], stacked) + dot(ixl[...], stacked)).astype(BF16)
    flat = dot(plain, iyh_ref[...]) + dot(plain, iyl_ref[...])
    for q in range(NY):
        s7[q] = flat[:, q * 128 : (q + 1) * 128].astype(BF16)
    halves = [pl.ds(32 * h, 32) for h in range(2)]
    for h, span in enumerate(halves):
        for d in (2, 1, 3):
            peer = along_y(d)
            send((4, 9)[h], s7.at[peer[1], span], r7.at[gy, span], peer)
    r7[gy] = s7[gy]
    weight = jnp.where((lane % 4 == 0) & (gy == 0), 0.5, 2.0)
    pairs = dot(dot(mirror, exact).astype(BF16), flip)
    pairs = jnp.where(gy == 0, 0.5 * pairs, 0.0)
    power = jnp.sum(values * (weight * values + pairs), axis=1, keepdims=True)
    power = jnp.sum(power.reshape(16, 8, 1), axis=0)
    sv[...] = jnp.broadcast_to(power, (8, 128))
    for d in range(1, NY):
        send(5, sv, rv.at[gy], along_y(d))
    rv[gy] = sv[...]
    def both_waits(sems, n, buffer, count, span):
        part = buffer.at[pl.ds(0, count), span]
        pltpu.make_async_copy(part, part, sems.at[n]).wait()

    for h, span in enumerate(halves):
        both_waits(recv_sem, (4, 9)[h], r7, NY - 1, span)
        line = jnp.concatenate([r7[q, span, :] for q in range(NY)], axis=1)
        depth = dot(line, iz[...])
        if h == 0:
            arrived(5, rv, NY - 1)
            power = (rv[0] + rv[1]) + (rv[2] + rv[3])
            scale = 1.0 / jnp.sqrt(power * (1.0 / float(GRID) ** 6) + 1.0)
            scale = jnp.concatenate([scale] * 4, axis=0)
        for q in range(NZ):
            s8[q, span, :] = (depth[:, q * 128 : (q + 1) * 128] * scale).astype(BF16)
        for d in far_z:
            peer = along_z(d)
            send((6, 10)[h], s8.at[peer[2], span], r8.at[gz, span], peer)
        r8[gz, span, :] = s8[gz, span, :]

    def put(x):
        return pltpu.make_async_copy(result.at[x], out_ref.at[x], out_sem.at[x])

    for h, span in enumerate(halves):
        both_waits(recv_sem, (6, 10)[h], r8, NZ - 1, span)
        wide[:, span, :] = r8[:, span, :].astype(F32)
        for x in range(4 * h, 4 * h + 4):
            result[x] = gelu(wide[:, pl.ds(8 * x, 8), :].reshape(CH, 128) + skip_ref[x]).T
            put(x).start()
    for n, span in ((0, pl.ds(0, 48)), (8, pl.ds(48, 16))):
        part = r1.at[pl.ds(0, NZ - 1), span]
        pltpu.make_async_copy(part, part, send_sem.at[n]).wait()
    left(1, r2, NY - 1)
    left(2, r4, 63)
    left(3, r5, 63)
    for h, span in enumerate(halves):
        both_waits(send_sem, (4, 9)[h], r7, NY - 1, span)
        both_waits(send_sem, (6, 10)[h], r8, NZ - 1, span)
    for x in range(8):
        put(x).wait()
    left(5, rv, NY - 1)
    left(7, around, 26)


def whole(points, counts, kin, kmid, kout, wskip, near, weights):
    fz, fy, fx, ix, iy, iz = transform_tables()
    tables = [wide_table(fz), *two_tables(fy), wide_table(fx), wide_table(ix)]
    tables += [*two_tables(iy), wide_table(iz)]
    anywhere = pl.BlockSpec(memory_space=pl.ANY)
    v = pltpu.VMEM
    return pl.pallas_call(
        whole_kernel,
        out_shape=jax.ShapeDtypeStruct((8, 128, CH), F32),
        in_specs=[anywhere] * (8 + len(tables)),
        out_specs=anywhere,
        scratch_shapes=[
            v((24, 128), F32), v((64, 16), jnp.int32), v((6, KH), BF16), v((KH, KH), BF16),
            v((CH, KH), BF16), v((CH, CH), BF16),
            v((8, 128, NB), jnp.int32), v((2048, CH), BF16),
            v((GRID, 512), F32), v((512, 128), BF16), v((512, 128), BF16),
            v((16, 128), F32), v((8, 256), F32), v((128, 512), BF16), v((128, 512), BF16),
            v((32, 1024), F32),
            v((27, 24, 128), F32), v((ROWS, PTS), F32), v((ROWS, PTS), BF16),
            v((CHUNKS, 8, 128), jnp.int32), v((CHUNKS, 8, 128), jnp.int32), v((8, 8, 128), F32),
            v((108, 8, 128), F32), v((8, 8, 128), F32), v((KH, 8), BF16),
            v((8, 256), BF16), v((8, 256), BF16),
            v((8, KH, 128), F32), v((ROWS, 128), jnp.int32),
            v((KH, ROWS), BF16), v((KH, KH), BF16),
            v((ROWS, 1024), BF16), v((ROWS, 1024), BF16), v((KH, 1024), BF16), v((KH, 1024), BF16),
            v((8, KH, 128), F32), v((8, CH, 128), F32), v((8, CH, 128), F32),
            v((128, 128), BF16), v((128, 128), BF16), v((64, 256), BF16), v((64, 256), BF16),
            v((NZ, 64, 128), BF16), v((NZ, 64, 128), BF16),
            v((NY, 64, 128), F32), v((NY, 64, 128), F32),
            v((CH, 2, 128), F32), v((CH, 2, 128), F32),
            v((NZ, 2, 128), F32), v((CH, 2, 128), F32),
            v((NY, 64, 128), BF16), v((NY, 64, 128), BF16),
            v((8, 128), F32), v((NY, 8, 128), F32),
            v((NZ, 64, 128), BF16), v((NZ, 64, 128), BF16),
            v((1024, 512), BF16), v((1024, 512), BF16), v((512, 1024), BF16),
            v((MODES, 128), F32), v((NZ, 64, 128), F32),
            v((8, 128, CH), F32), pltpu.SemaphoreType.DMA((11,)), pltpu.SemaphoreType.DMA((11,)),
            pltpu.SemaphoreType.DMA((16,)), pltpu.SemaphoreType.REGULAR((3,)),
            pltpu.SemaphoreType.DMA((8,)),
        ],
        compiler_params=pltpu.CompilerParams(collective_id=0, has_side_effects=True),
        name="whole",
    )(points, counts, kin, kmid, kout, wskip, near, weights, *tables)


def body(point_data, neighbours, counts, kernel_in, kernel_mid, kernel_out, spectral, skip_weight):
    out = whole(
        point_data.reshape(24, 128),
        jnp.swapaxes(counts[0], 1, 2).reshape(64, 16),
        kernel_in,
        kernel_mid,
        kernel_out.T,
        skip_weight,
        neighbours.reshape(8, 128, NB),
        spectral.reshape(2048, CH),
    )
    return out.reshape(1, 8, 16, 8, CH)


def solution(mesh):
    cells = P(None, "gx", "gy", "gz", None)
    return jax.shard_map(
        body,
        mesh=mesh,
        in_specs=(
            P(None, None, ("gx", "gy", "gz")),
            cells,
            P(None, "gx", "gy", "gz"),
            P(),
            P(),
            P(),
            P(None, "gz", "gx", "gy", None, None),
            P(),
        ),
        out_specs=cells,
        check_vma=False,
    )
```

```python
import functools
import math

import jax
import jax.numpy as jnp
import numpy as np
from jax import lax
from jax.experimental import pallas as pl
from jax.experimental.pallas import tpu as pltpu
from jax.sharding import PartitionSpec as P

GRID = 64
MODES = 16
NB = 32
KH = 80
CH = 64
PTS = 512
NX, NY, NZ = 8, 4, 8
F32 = jnp.float32
BF16 = jnp.bfloat16
MESH_ID = pl.DeviceIdType.MESH


def dot(a, b):
    return jnp.dot(a, b, preferred_element_type=F32)


def gelu(v):
    inner = v * (0.7978845608028654 + 0.035677408136300125 * (v * v))
    half = 0.5 * v
    return half + half * jnp.tanh(inner)


def split_two(values):
    upper = values.astype(BF16)
    return upper, (values - upper.astype(F32)).astype(BF16)


def dot_first(a, b):
    return lax.dot_general(a, b, (((0,), (0,)), ((), ())), preferred_element_type=F32)


def twice_gelu(v):
    v = v.astype(BF16)
    inner = v * (BF16(0.7978845608028654) + BF16(0.035677408136300125) * (v * v))
    return v + v * jnp.tanh(inner)


def looked_up(lookup, chosen, block):
    low = chosen & 127
    odd, upper = (chosen & 128) != 0, (chosen & 256) != 0
    bits = [(block & (1 << n)) != 0 for n in range(5)]

    def tile(n):
        return jnp.take_along_axis(lookup[n], low, axis=1, mode="promise_in_bounds")

    def tree(first, level):
        if level < 0:
            near, far = (
                jnp.where(odd, tile(4 * first + n + 1), tile(4 * first + n)) for n in (0, 2)
            )
            return jnp.where(upper, far, near)
        left = tree(first, level - 1)
        if first + (1 << level) >= 27:
            return left
        return jnp.where(bits[level], tree(first + (1 << level), level - 1), left)

    return tree(0, 4)


CHUNKS = 32
BY_LANES = (6, 7)
PART = 256
ROWS = 176


@functools.cache
def transform_tables():
    m = np.arange(GRID)
    centred = np.where(np.arange(MODES) < MODES // 2, np.arange(MODES), np.arange(MODES) - MODES)
    third = np.arange(MODES)

    def angles(f):
        return 2.0 * np.pi * ((f[:, None] * m[None, :]) % GRID) / GRID

    cos_c, sin_c = np.cos(angles(centred)), np.sin(angles(centred))
    cos_t, sin_t = np.cos(angles(third)), np.sin(angles(third))
    eye_k = np.eye(4)
    both = np.stack([cos_t, -sin_t], axis=-1)
    fz = np.broadcast_to(
        both.reshape(4, 4, GRID, 2).transpose(2, 0, 1, 3)[:, :, None], (GRID, 4, 16, 4, 2)
    ).reshape(GRID, 512)
    turn = np.stack([np.stack([cos_c, -sin_c], -1), np.stack([sin_c, cos_c], -1)], -2)
    fy = np.einsum("jcpyro,kl->pykrjocl", turn.reshape(8, 2, NY, 16, 2, 2), eye_k).reshape(512, 128)
    first = np.stack([cos_c, sin_c]).reshape(2, 8, 2, NX, 8)
    fx = np.broadcast_to(
        first.transpose(3, 2, 1, 0, 4)[..., None], (NX, 2, 8, 2, 8, 8)
    ).reshape(NX, 16, 128)
    ix = np.broadcast_to(
        first.transpose(3, 4, 0, 2, 1)[..., None], (NX, 8, 2, 2, 8, 8)
    ).reshape(NX, 8, 256)
    back = np.stack([np.stack([cos_c, sin_c], -1), np.stack([-sin_c, cos_c], -1)], -2)
    iy = np.einsum("jcqyro,kl->jrckqylo", back.reshape(8, 2, NY, 16, 2, 2), eye_k).reshape(128, 512)
    weight = np.where(third == 0, 1.0, 2.0)[:, None, None] / GRID**3
    iz = np.broadcast_to(
        (both * weight).transpose(0, 2, 1).reshape(32, NZ, 1, 8), (32, NZ, 16, 8)
    ).reshape(32, 1024)
    return fz, fy, fx, ix, iy, iz


def two_tables(table):
    import ml_dtypes

    upper = table.astype(np.float32).astype(ml_dtypes.bfloat16)
    lower = (table - upper.astype(np.float64)).astype(np.float32).astype(ml_dtypes.bfloat16)
    return jnp.asarray(upper), jnp.asarray(lower)


def wide_table(table):
    return jnp.asarray(np.ascontiguousarray(table, dtype=np.float32))


def iota(shape, dim):
    return lax.broadcasted_iota(jnp.int32, shape, dim)


def block_swap(x):
    row, lane = iota(x.shape, 0), iota(x.shape, 1) // 16
    for bit in (1, 2, 4):
        high, right = (row & bit) != 0, (lane & bit) != 0
        down = pltpu.roll(pltpu.roll(x, bit, axis=0), 128 - 16 * bit, axis=1)
        up = pltpu.roll(pltpu.roll(x, x.shape[0] - bit, axis=0), 16 * bit, axis=1)
        x = jnp.where(high == right, x, jnp.where(high, down, up))
    return x


def whole_kernel(
    pts_hbm, cnt_hbm, kin_hbm, kmid_hbm, kout_hbm, wskip_hbm, near_hbm, w_hbm, fzc_hbm, fyh_hbm, fyl_hbm, fxc_hbm, ixc_hbm, iyh_hbm, iyl_hbm, izc_hbm,
    out_ref,
    pts_ref, cnt_ref, kin_ref, kmid_ref, kout_ref, wskip_ref, near, w_ref, fzc_ref, fyh_ref, fyl_ref, fxc_ref, ixc_ref, iyh_ref, iyl_ref, izc_ref,
    around, table_rows, tab, slot_ids, block_ids, valid_slots,
    lookup, centres, win_few, pair_a, pair_b, pre, rowblk, win, wmid,
    masked_a, masked_b, hid_a, hid_b, acc, lat_ref, skip_ref, fxh, fxl, ixh, ixl,
    s1, r1, s2, r2, s4, r4, s5, r5, s7, r7, sv, rv, s8, r8, fzh, fzl, iz, grid, wide,
    result, send_sem, recv_sem, in_sem, heard, out_sem,
):
    gx, gy, gz = lax.axis_index("gx"), lax.axis_index("gy"), lax.axis_index("gz")
    me = gz * NX + gx
    barrier = pltpu.get_barrier_semaphore()
    fetched = [
        (near_hbm, near), (fzc_hbm, fzc_ref), (fxc_hbm.at[gx], fxc_ref), (ixc_hbm.at[gx], ixc_ref),
        (izc_hbm, izc_ref), (fyh_hbm, fyh_ref), (fyl_hbm, fyl_ref), (iyh_hbm, iyh_ref),
        (iyl_hbm, iyl_ref), (w_hbm, w_ref), (kin_hbm, kin_ref), (kmid_hbm, kmid_ref),
        (cnt_hbm, cnt_ref), (pts_hbm, pts_ref), (kout_hbm, kout_ref), (wskip_hbm, wskip_ref),
    ]

    def fetch(n):
        return pltpu.make_async_copy(fetched[n][0], fetched[n][1], in_sem.at[n])

    for n in (13, 10, 11, 12, 0, 14, 15, *range(1, 10)):
        fetch(n).start()

    def along_y(d):
        return (gx, lax.rem(gy + d, NY), gz)

    def along_z(d):
        return (gx, gy, lax.rem(gz + d, NZ))

    far_z = (4, 3, 5, 2, 6, 1, 7)

    def beside(step):
        return tuple(lax.rem(p + d + n, n) for p, d, n in zip((gx, gy, gz), step, (NX, NY, NZ)))

    plane = [
        (lax.rem(gx + dx, NX), gy, lax.rem(gz + dz, NZ))
        for dx, dz in sorted(
            ((dx, dz) for dx in range(NX) for dz in range(NZ) if (dx, dz) != (0, 0)),
            key=lambda d: -2 * min(d[0], NX - d[0]) - min(d[1], NZ - d[1]),
        )
    ]
    steps = [
        (dx, dy, dz)
        for dx in (-1, 0, 1)
        for dy in (-1, 0, 1)
        for dz in (-1, 0, 1)
        if (dx, dy, dz) != (0, 0, 0)
    ]
    flat_steps = [s for s in steps if s[1] == 0]
    near_steps = flat_steps + [(0, -1, 0), (0, 1, 0)]

    def tell(n, whom):
        for s in whom:
            pl.semaphore_signal(
                heard.at[n], inc=1, device_id=beside(s), device_id_type=MESH_ID
            )

    for s in steps:
        pl.semaphore_signal(barrier, inc=1, device_id=beside(s), device_id_type=MESH_ID)

    for n in range(10, 16):
        fetch(n).wait()
    rowblk[...] = iota((ROWS, 128), 0) // 6
    col = iota((6, ROWS), 1)
    chosen = (col % 6 == iota((6, ROWS), 0)) & (col < 162)
    chosen = jnp.where(chosen, 1.0, 0.0).astype(BF16)
    win[...] = dot_first(kin_ref[...], chosen).astype(BF16)
    eye = jnp.where(iota((KH, KH), 0) == iota((KH, KH), 1), 0.5, 0.0).astype(BF16)
    wmid[...] = dot_first(kmid_ref[...], eye).astype(BF16)
    few = jnp.where(iota((6, 8), 0) == iota((6, 8), 1), 1.0, 0.0).astype(BF16)
    win_few[...] = dot_first(kin_ref[...], few).astype(BF16)
    row, lane = iota((8, 128), 0), iota((8, 128), 1)
    index_y, index_z = lane // 8 - 8, lane % 8 - 4
    for x in range(8):
        index = jnp.where(row == 0, x - 4, jnp.where(row == 1, index_y, index_z))
        centre = jnp.where(row < 3, -(index.astype(F32) + 0.5) / GRID, 0.0)
        centres[x] = centre
        pre[x] = dot_first(kin_ref[...], centre[0:6].astype(BF16))
    by_row = jnp.where(iota((16, 128), 1) // 8 == iota((16, 128), 0), 1.0, 0.0).astype(BF16)
    spread = dot(cnt_ref[...].astype(F32).astype(BF16), by_row)
    spread = jnp.where(iota((64, 128), 0) % 8 == iota((64, 128), 1) % 8, spread, 0.0)
    gather = jnp.where(iota((8, 64), 1) // 8 == iota((8, 64), 0), 1.0, 0.0).astype(BF16)
    spread = dot(gather, spread.astype(BF16))
    for x in range(8):
        valid_slots[x] = jnp.broadcast_to(spread[x : x + 1], (8, 128))
    acc[...] = jnp.zeros((8, KH, 128), F32)
    table_rows[pl.ds(ROWS - 16, 16), :] = jnp.zeros((16, PTS), F32)
    row = iota((6, 128), 0)
    middle = jnp.where(row == 0, gx * 8 + 4, jnp.where(row == 1, gy * 16 + 8, gz * 8 + 4))
    middle = jnp.where(row < 3, middle.astype(F32) / GRID, 0.0)
    lookup[:, 6:8, :] = jnp.zeros((108, 2, 128), F32)
    pl.semaphore_wait(barrier, len(steps))
    tell(0, near_steps)

    def send(n, source, target, peer):
        pltpu.make_async_remote_copy(
            src_ref=source,
            dst_ref=target,
            send_sem=send_sem.at[n],
            recv_sem=recv_sem.at[n],
            device_id=peer,
            device_id_type=MESH_ID,
        ).start()

    def arrived(n, buffer, count):
        part = buffer.at[pl.ds(0, count)]
        pltpu.make_async_copy(part, part, recv_sem.at[n]).wait()

    def left(n, buffer, count):
        part = buffer.at[pl.ds(0, count)]
        pltpu.make_async_copy(part, part, send_sem.at[n]).wait()

    for step in steps:
        block = ((1 - step[0]) * 3 + (1 - step[1])) * 3 + (1 - step[2])
        send(7, pts_ref, around.at[block], beside(step))
    around[13] = pts_ref[...]
    fetch(0).wait()
    for x in range(8):
        point = near[x].T
        owner = point >> 9
        offset_z = (owner & 7) - gz + 1
        offset_y = ((owner >> 3) & 3) - gy + 1
        offset_x = (owner >> 5) - gx + 1
        block = (offset_x * 3 + offset_y) * 3 + offset_z
        block_ids[pl.ds(4 * x, 4)] = block.reshape(4, 8, 128)
        slot_ids[pl.ds(4 * x, 4)] = (point & 511).reshape(4, 8, 128)
    pl.semaphore_wait(heard.at[0], len(near_steps))
    tell(1, flat_steps)
    for n in range(1, 5):
        fetch(n).wait()
    own_y = iota((128, 512), 0) // 8 == iota((128, 512), 1) % 128 // 8
    for q in range(NZ):
        part = jnp.concatenate([fzc_ref[pl.ds(8 * q, 8), :]] * 16, axis=0)
        upper, lower = split_two(jnp.where(own_y, part, 0.0))
        fzh[pl.ds(128 * q, 128), :] = upper
        fzl[pl.ds(128 * q, 128), :] = lower
    own_y = iota((128, 1024), 0) // 8 == iota((128, 1024), 1) % 128 // 8
    for q in range(NY):
        part = jnp.concatenate([izc_ref[pl.ds(8 * q, 8), :]] * 16, axis=0)
        iz[pl.ds(128 * q, 128), :] = jnp.where(own_y, part, 0.0).astype(BF16)
    part = jnp.concatenate(
        [jnp.broadcast_to(fxc_ref[pl.ds(n, 1), :], (8, 128)) for n in range(16)], axis=0
    )
    row, lane = iota((128, 128), 0), iota((128, 128), 1)
    fxh[...], fxl[...] = split_two(jnp.where(row % 8 == lane % 8, part, 0.0))
    part = jnp.concatenate(
        [jnp.broadcast_to(ixc_ref[pl.ds(n, 1), :], (8, 256)) for n in range(8)], axis=0
    )
    ixh[...], ixl[...] = split_two(jnp.where(iota((64, 256), 0) % 8 == iota((64, 256), 1) % 8, part, 0.0))
    pl.semaphore_wait(heard.at[1], len(flat_steps))
    tell(2, flat_steps)
    arrived(7, around, 26)
    for b in range(27):
        for t in range(4):
            block = around[b, pl.ds(t, 6, stride=4), :] - middle
            lookup[4 * b + t, 0:6, :] = block
            table_rows[pl.ds(6 * b, 6), pl.ds(128 * t, 128)] = block
    tab[...] = table_rows[...].astype(BF16)
    low_ids = iota((64, 128), 0)

    def step(t, masked_out, masked_in, pair_out, pair_in, hid_out, hid_in, stages="ghs"):
        if "g" in stages:
            slots, owners = slot_ids[t], block_ids[t]
            centre = centres[t // 4]
        if "h" in stages:
            base = jnp.concatenate([pre[(t - 1) // 4]] * 2, axis=1)
        if "s" in stages:
            slab = (t - 2) // 4
            valid = valid_slots[slab][0:1]
            first = lax.convert_element_type((t - 2) % 4 * 8, F32)
            total = jnp.zeros((KH, 128), F32)
        for part in range(4):
            span = pl.ds(part * PART, PART)
            by_lanes = 2 * part in BY_LANES
            if "g" in stages and not by_lanes:
                hot = []
                for s in (2 * part, 2 * part + 1):
                    chosen = jnp.broadcast_to(slots[s : s + 1], (8, 128))
                    low = jnp.broadcast_to((chosen & 63)[0:1], (64, 128))
                    low = jnp.where(low == low_ids, 1.0, 0.0).astype(BF16)
                    high = chosen >> 6
                    for n in range(8):
                        here = jnp.where(high == n, 1.0, 0.0)
                        here = jnp.concatenate([here] * 8, axis=0).astype(BF16)
                        hot.append(low * here)
                hot = [jnp.concatenate(hot[:8], axis=0), jnp.concatenate(hot[8:], axis=0)]
                found = dot(tab[...], jnp.concatenate(hot, axis=1))
            if "h" in stages:
                if by_lanes:
                    ahead = dot(win_few[...], pair_in[...])
                else:
                    ahead = dot(win[...], masked_in[:, span]) + base
            if "s" in stages:
                last = dot(wmid[...], hid_in[:, span])
            if "h" in stages:
                hid_out[:, span] = twice_gelu(ahead)
            if "s" in stages:
                last = twice_gelu(last).astype(F32)
                for n in range(2):
                    used = valid > first + (2 * part + n)
                    total = total + jnp.where(used, last[:, n * 128 : (n + 1) * 128], 0.0)
            if "g" not in stages:
                continue
            for n in range(2):
                s = 2 * part + n
                if by_lanes:
                    chosen = jnp.broadcast_to(slots[s : s + 1], (8, 128))
                    block = jnp.broadcast_to(owners[s : s + 1], (8, 128))
                    pair = looked_up(lookup, chosen, block) + centre
                    pair_out[:, pl.ds(n * 128, 128)] = pair.astype(BF16)
                else:
                    chosen = jnp.broadcast_to(owners[s : s + 1], (ROWS, 128))
                    kept = jnp.where(rowblk[...] == chosen, found[:, n * 128 : (n + 1) * 128], 0.0)
                    masked_out[:, pl.ds(s * 128, 128)] = kept.astype(BF16)
        if "s" in stages:
            acc[slab] += total

    even = (masked_a, masked_b, pair_a, pair_b, hid_a, hid_b)
    odd = (masked_b, masked_a, pair_b, pair_a, hid_b, hid_a)

    def two_steps(tt, carry):
        step(2 * tt, *even)
        step(2 * tt + 1, *odd)
        return carry

    def finish(slabs):
        for x in slabs:
            upper, lower = split_two(0.5 * acc[x])
            values = dot(kout_ref[...], upper) + dot(kout_ref[...], lower)
            latent = (values / valid_slots[x, 0:1]).astype(BF16)
            skip_ref[x] = dot_first(wskip_ref[...], latent)
            lat_ref[x] = latent.astype(F32)
        span = pl.ds(8 * slabs[0], 8 * len(slabs))
        for q in range(NZ):
            ready = lat_ref[slabs[0] : slabs[-1] + 1, pl.ds(8 * q, 8), :]
            s1[q, span, :] = ready.reshape(8 * len(slabs), 128).astype(BF16)
        r1[gz, span, :] = s1[gz, span, :]
        return span

    step(0, *even, "g")
    step(1, *odd, "gh")
    lax.fori_loop(1, 13, two_steps, 0)
    span = finish(range(6))
    pl.semaphore_wait(heard.at[2], len(flat_steps))
    for d in far_z:
        peer = along_z(d)
        send(0, s1.at[peer[2], span], r1.at[gz, span], peer)
    lax.fori_loop(13, CHUNKS // 2, two_steps, 0)
    step(CHUNKS, *even, "hs")
    step(CHUNKS + 1, *odd, "s")
    span = finish(range(6, 8))
    for d in far_z:
        peer = along_z(d)
        send(8, s1.at[peer[2], span], r1.at[gz, span], peer)
    row, lane = iota((128, 128), 0), iota((128, 128), 1)
    row_i, lane_i = row // 8 % 8 * 2 + row // 64, lane // 8 % 8 * 2 + lane // 64
    mirror = (row % 8 == lane % 8) & (row_i != 8) & (lane_i == (16 - row_i) % 16)
    mirror = jnp.where(mirror, 1.0, 0.0).astype(BF16)
    row_j, lane_j = row // 16 * 2 + row // 4 % 2, lane // 16 * 2 + lane // 4 % 2
    flip = (row % 4 == 0) & (lane % 4 == 0) & (row // 8 % 2 == lane // 8 % 2)
    flip = flip & (lane_j != 8) & (row_j == (16 - lane_j) % 16)
    flip = jnp.where(flip, jnp.where(lane // 8 % 2 == 0, 1.0, -1.0), 0.0).astype(BF16)
    pick = jnp.where(iota((16, 128), 1) % 16 == iota((16, 128), 0), 1.0, 0.0).astype(BF16)
    own_channel = iota((64, 128), 0) % 8 == iota((64, 128), 1) // 16
    own_mode = iota((32, 1024), 1) // CH == iota((32, 1024), 0) % MODES
    for n in range(5, 10):
        fetch(n).wait()
    for n, span in ((0, pl.ds(0, 48)), (8, pl.ds(48, 16))):
        part = r1.at[pl.ds(0, NZ - 1), span]
        pltpu.make_async_copy(part, part, recv_sem.at[n]).wait()
    line = jnp.concatenate([r1[q] for q in range(NZ)], axis=1)
    deep = dot(line, fzh[...]) + dot(line, fzl[...])
    for q in range(NY):
        s2[q] = deep[:, q * 128 : (q + 1) * 128]
    for d in range(1, NY):
        peer = along_y(d)
        send(1, s2.at[peer[1]], r2.at[gy], peer)
    r2[gy] = s2[gy]
    arrived(1, r2, NY - 1)
    upper, lower = split_two(jnp.concatenate([r2[q] for q in range(NY)], axis=1))
    flat = dot(upper, fyh_ref[...]) + dot(upper, fyl_ref[...]) + dot(lower, fyh_ref[...])
    real = iota((64, 128), 1) // 8 % 2 == 0
    turned = jnp.where(real, pltpu.roll(flat, 120, axis=1), -pltpu.roll(flat, 8, axis=1))
    upper, lower = split_two(jnp.concatenate([flat, turned], axis=0))
    share = block_swap(dot(fxh[...], upper) + dot(fxl[...], upper) + dot(fxh[...], lower))
    for i in range(2):
        s4[:, i, :] = share[64 * i : 64 * i + 64]
    for peer in plane:
        send(2, s4.at[peer[2] * NX + peer[0]], r4.at[me], peer)
    r4[me] = s4[me]
    arrived(2, r4, 63)
    for q in range(NZ):
        pair = r4[q * NX]
        for n in range(1, NX):
            pair = pair + r4[q * NX + n]
        grid[pl.ds(2 * q, 2), :] = pair
    found = []
    for i in range(2):
        values = jnp.concatenate(
            [jnp.broadcast_to(grid[pl.ds(2 * q + i, 1), :], (8, 128)) for q in range(NZ)], axis=0
        )
        values = jnp.where(own_channel, values, 0.0).astype(BF16)
        found.append(
            lax.dot_general(
                pick,
                jnp.concatenate([values, values], axis=0),
                (((1,), (1,)), ((), ())),
                preferred_element_type=F32,
            )
        )
    rows = jnp.concatenate(
        [found[0][0:8], found[1][0:8], found[0][8:16], found[1][8:16]], axis=0
    )
    spread = jnp.where(own_mode, jnp.concatenate([rows] * 8, axis=1), 0.0).astype(BF16)
    by_real, by_imag = dot(spread, w_ref[0:1024]), dot(spread, w_ref[1024:2048])
    mixed_real = by_real[0:16] - by_imag[16:32]
    mixed_imag = by_imag[0:16] + by_real[16:32]
    for i in range(2):
        mine = jnp.concatenate(
            [mixed_real[8 * i : 8 * i + 8], mixed_imag[8 * i : 8 * i + 8]], axis=0
        ).astype(BF16)
        placed = jnp.where(own_channel, dot_first(mine, pick), 0.0).astype(BF16)
        s5[:, i, :] = dot(gather, placed)
    for peer in plane:
        send(3, s5.at[peer[2]], r5.at[me], peer)
    r5[me] = s5[gz]
    arrived(3, r5, 63)
    values = block_swap(jnp.concatenate([r5[:, i, :] for i in range(2)], axis=0))
    is_mean = (row < 8) & ((lane == 0) | (lane == 8)) & (gy == 0)
    values = jnp.where(is_mean, 0.0, values)
    exact = values.astype(BF16)
    real = lane // 8 % 2 == 0
    turned = jnp.where(real, -pltpu.roll(values, 120, axis=1), pltpu.roll(values, 8, axis=1))
    stacked = jnp.concatenate([exact, turned.astype(BF16)], axis=0)
    plain = (dot(ixh[...], stacked) + dot(ixl[...], stacked)).astype(BF16)
    flat = dot(plain, iyh_ref[...]) + dot(plain, iyl_ref[...])
    for q in range(NY):
        s7[q] = flat[:, q * 128 : (q + 1) * 128].astype(BF16)
    halves = [pl.ds(32 * h, 32) for h in range(2)]
    for h, span in enumerate(halves):
        for d in (2, 1, 3):
            peer = along_y(d)
            send((4, 9)[h], s7.at[peer[1], span], r7.at[gy, span], peer)
    r7[gy] = s7[gy]
    weight = jnp.where((lane % 4 == 0) & (gy == 0), 0.5, 2.0)
    pairs = dot(dot(mirror, exact).astype(BF16), flip)
    pairs = jnp.where(gy == 0, 0.5 * pairs, 0.0)
    power = jnp.sum(values * (weight * values + pairs), axis=1, keepdims=True)
    power = jnp.sum(power.reshape(16, 8, 1), axis=0)
    sv[...] = jnp.broadcast_to(power, (8, 128))
    for d in range(1, NY):
        send(5, sv, rv.at[gy], along_y(d))
    rv[gy] = sv[...]
    def both_waits(sems, n, buffer, count, span):
        part = buffer.at[pl.ds(0, count), span]
        pltpu.make_async_copy(part, part, sems.at[n]).wait()

    for h, span in enumerate(halves):
        both_waits(recv_sem, (4, 9)[h], r7, NY - 1, span)
        line = jnp.concatenate([r7[q, span, :] for q in range(NY)], axis=1)
        depth = dot(line, iz[...])
        if h == 0:
            arrived(5, rv, NY - 1)
            power = (rv[0] + rv[1]) + (rv[2] + rv[3])
            scale = 1.0 / jnp.sqrt(power * (1.0 / float(GRID) ** 6) + 1.0)
            scale = jnp.concatenate([scale] * 4, axis=0)
        for q in range(NZ):
            s8[q, span, :] = (depth[:, q * 128 : (q + 1) * 128] * scale).astype(BF16)
        for d in far_z:
            peer = along_z(d)
            send((6, 10)[h], s8.at[peer[2], span], r8.at[gz, span], peer)
        r8[gz, span, :] = s8[gz, span, :]

    def put(x):
        return pltpu.make_async_copy(result.at[x], out_ref.at[x], out_sem.at[x])

    for h, span in enumerate(halves):
        both_waits(recv_sem, (6, 10)[h], r8, NZ - 1, span)
        wide[:, span, :] = r8[:, span, :].astype(F32)
        for x in range(4 * h, 4 * h + 4):
            result[x] = gelu(wide[:, pl.ds(8 * x, 8), :].reshape(CH, 128) + skip_ref[x]).T
            put(x).start()
    for n, span in ((0, pl.ds(0, 48)), (8, pl.ds(48, 16))):
        part = r1.at[pl.ds(0, NZ - 1), span]
        pltpu.make_async_copy(part, part, send_sem.at[n]).wait()
    left(1, r2, NY - 1)
    left(2, r4, 63)
    left(3, r5, 63)
    for h, span in enumerate(halves):
        both_waits(send_sem, (4, 9)[h], r7, NY - 1, span)
        both_waits(send_sem, (6, 10)[h], r8, NZ - 1, span)
    for x in range(8):
        put(x).wait()
    left(5, rv, NY - 1)
    left(7, around, 26)


def whole(points, counts, kin, kmid, kout, wskip, near, weights):
    fz, fy, fx, ix, iy, iz = transform_tables()
    tables = [wide_table(fz), *two_tables(fy), wide_table(fx), wide_table(ix)]
    tables += [*two_tables(iy), wide_table(iz)]
    anywhere = pl.BlockSpec(memory_space=pl.ANY)
    v = pltpu.VMEM
    return pl.pallas_call(
        whole_kernel,
        out_shape=jax.ShapeDtypeStruct((8, 128, CH), F32),
        in_specs=[anywhere] * (8 + len(tables)),
        out_specs=anywhere,
        scratch_shapes=[
            v((24, 128), F32), v((64, 16), jnp.int32), v((6, KH), BF16), v((KH, KH), BF16),
            v((CH, KH), BF16), v((CH, CH), BF16),
            v((8, 128, NB), jnp.int32), v((2048, CH), BF16),
            v((GRID, 512), F32), v((512, 128), BF16), v((512, 128), BF16),
            v((16, 128), F32), v((8, 256), F32), v((128, 512), BF16), v((128, 512), BF16),
            v((32, 1024), F32),
            v((27, 24, 128), F32), v((ROWS, PTS), F32), v((ROWS, PTS), BF16),
            v((CHUNKS, 8, 128), jnp.int32), v((CHUNKS, 8, 128), jnp.int32), v((8, 8, 128), F32),
            v((108, 8, 128), F32), v((8, 8, 128), F32), v((KH, 8), BF16),
            v((8, 256), BF16), v((8, 256), BF16),
            v((8, KH, 128), F32), v((ROWS, 128), jnp.int32),
            v((KH, ROWS), BF16), v((KH, KH), BF16),
            v((ROWS, 1024), BF16), v((ROWS, 1024), BF16), v((KH, 1024), BF16), v((KH, 1024), BF16),
            v((8, KH, 128), F32), v((8, CH, 128), F32), v((8, CH, 128), F32),
            v((128, 128), BF16), v((128, 128), BF16), v((64, 256), BF16), v((64, 256), BF16),
            v((NZ, 64, 128), BF16), v((NZ, 64, 128), BF16),
            v((NY, 64, 128), F32), v((NY, 64, 128), F32),
            v((CH, 2, 128), F32), v((CH, 2, 128), F32),
            v((NZ, 2, 128), F32), v((CH, 2, 128), F32),
            v((NY, 64, 128), BF16), v((NY, 64, 128), BF16),
            v((8, 128), F32), v((NY, 8, 128), F32),
            v((NZ, 64, 128), BF16), v((NZ, 64, 128), BF16),
            v((1024, 512), BF16), v((1024, 512), BF16), v((512, 1024), BF16),
            v((MODES, 128), F32), v((NZ, 64, 128), F32),
            v((8, 128, CH), F32), pltpu.SemaphoreType.DMA((11,)), pltpu.SemaphoreType.DMA((11,)),
            pltpu.SemaphoreType.DMA((16,)), pltpu.SemaphoreType.REGULAR((3,)),
            pltpu.SemaphoreType.DMA((8,)),
        ],
        compiler_params=pltpu.CompilerParams(collective_id=0, has_side_effects=True),
        name="whole",
    )(points, counts, kin, kmid, kout, wskip, near, weights, *tables)


def body(point_data, neighbours, counts, kernel_in, kernel_mid, kernel_out, spectral, skip_weight):
    out = whole(
        point_data.reshape(24, 128),
        jnp.swapaxes(counts[0], 1, 2).reshape(64, 16),
        kernel_in,
        kernel_mid,
        kernel_out.T,
        skip_weight,
        neighbours.reshape(8, 128, NB),
        spectral.reshape(2048, CH),
    )
    return out.reshape(1, 8, 16, 8, CH)


def solution(mesh):
    cells = P(None, "gx", "gy", "gz", None)
    return jax.shard_map(
        body,
        mesh=mesh,
        in_specs=(
            P(None, None, ("gx", "gy", "gz")),
            cells,
            P(None, "gx", "gy", "gz"),
            P(),
            P(),
            P(),
            P(None, "gz", "gx", "gy", None, None),
            P(),
        ),
        out_specs=cells,
        check_vma=False,
    )
```

```python
import functools
import math

import jax
import jax.numpy as jnp
import numpy as np
from jax import lax
from jax.experimental import pallas as pl
from jax.experimental.pallas import tpu as pltpu
from jax.sharding import PartitionSpec as P

GRID = 64
MODES = 16
NB = 32
KH = 80
CH = 64
PTS = 512
NX, NY, NZ = 8, 4, 8
F32 = jnp.float32
BF16 = jnp.bfloat16
MESH_ID = pl.DeviceIdType.MESH


def dot(a, b):
    return jnp.dot(a, b, preferred_element_type=F32)


def gelu(v):
    inner = v * (0.7978845608028654 + 0.035677408136300125 * (v * v))
    half = 0.5 * v
    return half + half * jnp.tanh(inner)


def split_two(values):
    upper = values.astype(BF16)
    return upper, (values - upper.astype(F32)).astype(BF16)


def dot_first(a, b):
    return lax.dot_general(a, b, (((0,), (0,)), ((), ())), preferred_element_type=F32)


def twice_gelu(v):
    v = v.astype(BF16)
    inner = v * (BF16(0.7978845608028654) + BF16(0.035677408136300125) * (v * v))
    return v + v * jnp.tanh(inner)


def looked_up(lookup, chosen, block):
    low = chosen & 127
    odd, upper = (chosen & 128) != 0, (chosen & 256) != 0
    bits = [(block & (1 << n)) != 0 for n in range(5)]

    def tile(n):
        return jnp.take_along_axis(lookup[n], low, axis=1, mode="promise_in_bounds")

    def tree(first, level):
        if level < 0:
            near, far = (
                jnp.where(odd, tile(4 * first + n + 1), tile(4 * first + n)) for n in (0, 2)
            )
            return jnp.where(upper, far, near)
        left = tree(first, level - 1)
        if first + (1 << level) >= 27:
            return left
        return jnp.where(bits[level], tree(first + (1 << level), level - 1), left)

    return tree(0, 4)


CHUNKS = 32
BY_LANES = (6, 7)
PART = 256
ROWS = 176


@functools.cache
def transform_tables():
    m = np.arange(GRID)
    centred = np.where(np.arange(MODES) < MODES // 2, np.arange(MODES), np.arange(MODES) - MODES)
    third = np.arange(MODES)

    def angles(f):
        return 2.0 * np.pi * ((f[:, None] * m[None, :]) % GRID) / GRID

    cos_c, sin_c = np.cos(angles(centred)), np.sin(angles(centred))
    cos_t, sin_t = np.cos(angles(third)), np.sin(angles(third))
    eye_k = np.eye(4)
    both = np.stack([cos_t, -sin_t], axis=-1)
    fz = np.broadcast_to(
        both.reshape(4, 4, GRID, 2).transpose(2, 0, 1, 3)[:, :, None], (GRID, 4, 16, 4, 2)
    ).reshape(GRID, 512)
    turn = np.stack([np.stack([cos_c, -sin_c], -1), np.stack([sin_c, cos_c], -1)], -2)
    fy = np.einsum("jcpyro,kl->pykrjocl", turn.reshape(8, 2, NY, 16, 2, 2), eye_k).reshape(512, 128)
    first = np.stack([cos_c, sin_c]).reshape(2, 8, 2, NX, 8)
    fx = np.broadcast_to(
        first.transpose(3, 2, 1, 0, 4)[..., None], (NX, 2, 8, 2, 8, 8)
    ).reshape(NX, 16, 128)
    ix = np.broadcast_to(
        first.transpose(3, 4, 0, 2, 1)[..., None], (NX, 8, 2, 2, 8, 8)
    ).reshape(NX, 8, 256)
    back = np.stack([np.stack([cos_c, sin_c], -1), np.stack([-sin_c, cos_c], -1)], -2)
    iy = np.einsum("jcqyro,kl->jrckqylo", back.reshape(8, 2, NY, 16, 2, 2), eye_k).reshape(128, 512)
    weight = np.where(third == 0, 1.0, 2.0)[:, None, None] / GRID**3
    iz = np.broadcast_to(
        (both * weight).transpose(0, 2, 1).reshape(32, NZ, 1, 8), (32, NZ, 16, 8)
    ).reshape(32, 1024)
    return fz, fy, fx, ix, iy, iz


def two_tables(table):
    import ml_dtypes

    upper = table.astype(np.float32).astype(ml_dtypes.bfloat16)
    lower = (table - upper.astype(np.float64)).astype(np.float32).astype(ml_dtypes.bfloat16)
    return jnp.asarray(upper), jnp.asarray(lower)


def wide_table(table):
    return jnp.asarray(np.ascontiguousarray(table, dtype=np.float32))


def iota(shape, dim):
    return lax.broadcasted_iota(jnp.int32, shape, dim)


def block_swap(x):
    row, lane = iota(x.shape, 0), iota(x.shape, 1) // 16
    for bit in (1, 2, 4):
        high, right = (row & bit) != 0, (lane & bit) != 0
        down = pltpu.roll(pltpu.roll(x, bit, axis=0), 128 - 16 * bit, axis=1)
        up = pltpu.roll(pltpu.roll(x, x.shape[0] - bit, axis=0), 16 * bit, axis=1)
        x = jnp.where(high == right, x, jnp.where(high, down, up))
    return x


def whole_kernel(
    pts_hbm, cnt_hbm, kin_hbm, kmid_hbm, kout_hbm, wskip_hbm, near_hbm, w_hbm, fzc_hbm, fyh_hbm, fyl_hbm, fxc_hbm, ixc_hbm, iyh_hbm, iyl_hbm, izc_hbm,
    out_ref,
    pts_ref, cnt_ref, kin_ref, kmid_ref, kout_ref, wskip_ref, near, w_ref, fzc_ref, fyh_ref, fyl_ref, fxc_ref, ixc_ref, iyh_ref, iyl_ref, izc_ref,
    around, table_rows, tab, slot_ids, block_ids, valid_slots,
    lookup, centres, win_few, pair_a, pair_b, pre, rowblk, win, wmid,
    masked_a, masked_b, hid_a, hid_b, acc, lat_ref, skip_ref, fxh, fxl, ixh, ixl,
    s1, r1, s2, r2, s4, r4, s5, r5, s7, r7, sv, rv, s8, r8, fzh, fzl, iz, grid, wide,
    result, send_sem, recv_sem, in_sem, heard, out_sem,
):
    gx, gy, gz = lax.axis_index("gx"), lax.axis_index("gy"), lax.axis_index("gz")
    me = gz * NX + gx
    barrier = pltpu.get_barrier_semaphore()
    fetched = [
        (near_hbm, near), (fzc_hbm, fzc_ref), (fxc_hbm.at[gx], fxc_ref), (ixc_hbm.at[gx], ixc_ref),
        (izc_hbm, izc_ref), (fyh_hbm, fyh_ref), (fyl_hbm, fyl_ref), (iyh_hbm, iyh_ref),
        (iyl_hbm, iyl_ref), (w_hbm, w_ref), (kin_hbm, kin_ref), (kmid_hbm, kmid_ref),
        (cnt_hbm, cnt_ref), (pts_hbm, pts_ref), (kout_hbm, kout_ref), (wskip_hbm, wskip_ref),
    ]

    def fetch(n):
        return pltpu.make_async_copy(fetched[n][0], fetched[n][1], in_sem.at[n])

    for n in (13, 10, 11, 12, 0, 14, 15, *range(1, 10)):
        fetch(n).start()

    def along_y(d):
        return (gx, lax.rem(gy + d, NY), gz)

    def along_z(d):
        return (gx, gy, lax.rem(gz + d, NZ))

    far_z = (4, 3, 5, 2, 6, 1, 7)

    def beside(step):
        return tuple(lax.rem(p + d + n, n) for p, d, n in zip((gx, gy, gz), step, (NX, NY, NZ)))

    plane = [
        (lax.rem(gx + dx, NX), gy, lax.rem(gz + dz, NZ))
        for dx, dz in sorted(
            ((dx, dz) for dx in range(NX) for dz in range(NZ) if (dx, dz) != (0, 0)),
            key=lambda d: -2 * min(d[0], NX - d[0]) - min(d[1], NZ - d[1]),
        )
    ]
    steps = [
        (dx, dy, dz)
        for dx in (-1, 0, 1)
        for dy in (-1, 0, 1)
        for dz in (-1, 0, 1)
        if (dx, dy, dz) != (0, 0, 0)
    ]
    flat_steps = [s for s in steps if s[1] == 0]
    near_steps = flat_steps + [(0, -1, 0), (0, 1, 0)]

    def tell(n, whom):
        for s in whom:
            pl.semaphore_signal(
                heard.at[n], inc=1, device_id=beside(s), device_id_type=MESH_ID
            )

    for s in steps:
        pl.semaphore_signal(barrier, inc=1, device_id=beside(s), device_id_type=MESH_ID)

    for n in range(10, 16):
        fetch(n).wait()
    rowblk[...] = iota((ROWS, 128), 0) // 6
    col = iota((6, ROWS), 1)
    chosen = (col % 6 == iota((6, ROWS), 0)) & (col < 162)
    chosen = jnp.where(chosen, 1.0, 0.0).astype(BF16)
    win[...] = dot_first(kin_ref[...], chosen).astype(BF16)
    eye = jnp.where(iota((KH, KH), 0) == iota((KH, KH), 1), 0.5, 0.0).astype(BF16)
    wmid[...] = dot_first(kmid_ref[...], eye).astype(BF16)
    few = jnp.where(iota((6, 8), 0) == iota((6, 8), 1), 1.0, 0.0).astype(BF16)
    win_few[...] = dot_first(kin_ref[...], few).astype(BF16)
    row, lane = iota((8, 128), 0), iota((8, 128), 1)
    index_y, index_z = lane // 8 - 8, lane % 8 - 4
    for x in range(8):
        index = jnp.where(row == 0, x - 4, jnp.where(row == 1, index_y, index_z))
        centre = jnp.where(row < 3, -(index.astype(F32) + 0.5) / GRID, 0.0)
        centres[x] = centre
        pre[x] = dot_first(kin_ref[...], centre[0:6].astype(BF16))
    by_row = jnp.where(iota((16, 128), 1) // 8 == iota((16, 128), 0), 1.0, 0.0).astype(BF16)
    spread = dot(cnt_ref[...].astype(F32).astype(BF16), by_row)
    spread = jnp.where(iota((64, 128), 0) % 8 == iota((64, 128), 1) % 8, spread, 0.0)
    gather = jnp.where(iota((8, 64), 1) // 8 == iota((8, 64), 0), 1.0, 0.0).astype(BF16)
    spread = dot(gather, spread.astype(BF16))
    for x in range(8):
        valid_slots[x] = jnp.broadcast_to(spread[x : x + 1], (8, 128))
    acc[...] = jnp.zeros((8, KH, 128), F32)
    table_rows[pl.ds(ROWS - 16, 16), :] = jnp.zeros((16, PTS), F32)
    row = iota((6, 128), 0)
    middle = jnp.where(row == 0, gx * 8 + 4, jnp.where(row == 1, gy * 16 + 8, gz * 8 + 4))
    middle = jnp.where(row < 3, middle.astype(F32) / GRID, 0.0)
    lookup[:, 6:8, :] = jnp.zeros((108, 2, 128), F32)
    pl.semaphore_wait(barrier, len(steps))
    tell(0, near_steps)

    def send(n, source, target, peer):
        pltpu.make_async_remote_copy(
            src_ref=source,
            dst_ref=target,
            send_sem=send_sem.at[n],
            recv_sem=recv_sem.at[n],
            device_id=peer,
            device_id_type=MESH_ID,
        ).start()

    def arrived(n, buffer, count):
        part = buffer.at[pl.ds(0, count)]
        pltpu.make_async_copy(part, part, recv_sem.at[n]).wait()

    def left(n, buffer, count):
        part = buffer.at[pl.ds(0, count)]
        pltpu.make_async_copy(part, part, send_sem.at[n]).wait()

    for step in sorted(steps, key=lambda d: -sum(map(abs, d))):
        block = ((1 - step[0]) * 3 + (1 - step[1])) * 3 + (1 - step[2])
        send(7, pts_ref, around.at[block], beside(step))
    around[13] = pts_ref[...]
    fetch(0).wait()
    for x in range(8):
        point = near[x].T
        owner = point >> 9
        offset_z = (owner & 7) - gz + 1
        offset_y = ((owner >> 3) & 3) - gy + 1
        offset_x = (owner >> 5) - gx + 1
        block = (offset_x * 3 + offset_y) * 3 + offset_z
        block_ids[pl.ds(4 * x, 4)] = block.reshape(4, 8, 128)
        slot_ids[pl.ds(4 * x, 4)] = (point & 511).reshape(4, 8, 128)
    pl.semaphore_wait(heard.at[0], len(near_steps))
    tell(1, flat_steps)
    for n in range(1, 5):
        fetch(n).wait()
    own_y = iota((128, 512), 0) // 8 == iota((128, 512), 1) % 128 // 8
    for q in range(NZ):
        part = jnp.concatenate([fzc_ref[pl.ds(8 * q, 8), :]] * 16, axis=0)
        upper, lower = split_two(jnp.where(own_y, part, 0.0))
        fzh[pl.ds(128 * q, 128), :] = upper
        fzl[pl.ds(128 * q, 128), :] = lower
    own_y = iota((128, 1024), 0) // 8 == iota((128, 1024), 1) % 128 // 8
    for q in range(NY):
        part = jnp.concatenate([izc_ref[pl.ds(8 * q, 8), :]] * 16, axis=0)
        iz[pl.ds(128 * q, 128), :] = jnp.where(own_y, part, 0.0).astype(BF16)
    part = jnp.concatenate(
        [jnp.broadcast_to(fxc_ref[pl.ds(n, 1), :], (8, 128)) for n in range(16)], axis=0
    )
    row, lane = iota((128, 128), 0), iota((128, 128), 1)
    fxh[...], fxl[...] = split_two(jnp.where(row % 8 == lane % 8, part, 0.0))
    part = jnp.concatenate(
        [jnp.broadcast_to(ixc_ref[pl.ds(n, 1), :], (8, 256)) for n in range(8)], axis=0
    )
    ixh[...], ixl[...] = split_two(jnp.where(iota((64, 256), 0) % 8 == iota((64, 256), 1) % 8, part, 0.0))
    pl.semaphore_wait(heard.at[1], len(flat_steps))
    tell(2, flat_steps)
    arrived(7, around, 26)
    for b in range(27):
        for t in range(4):
            block = around[b, pl.ds(t, 6, stride=4), :] - middle
            lookup[4 * b + t, 0:6, :] = block
            table_rows[pl.ds(6 * b, 6), pl.ds(128 * t, 128)] = block
    tab[...] = table_rows[...].astype(BF16)
    low_ids = iota((64, 128), 0)

    def step(t, masked_out, masked_in, pair_out, pair_in, hid_out, hid_in, stages="ghs"):
        if "g" in stages:
            slots, owners = slot_ids[t], block_ids[t]
            centre = centres[t // 4]
        if "h" in stages:
            base = jnp.concatenate([pre[(t - 1) // 4]] * 2, axis=1)
        if "s" in stages:
            slab = (t - 2) // 4
            valid = valid_slots[slab][0:1]
            first = lax.convert_element_type((t - 2) % 4 * 8, F32)
            total = jnp.zeros((KH, 128), F32)
        for part in range(4):
            span = pl.ds(part * PART, PART)
            by_lanes = 2 * part in BY_LANES
            if "g" in stages and not by_lanes:
                hot = []
                for s in (2 * part, 2 * part + 1):
                    chosen = jnp.broadcast_to(slots[s : s + 1], (8, 128))
                    low = jnp.broadcast_to((chosen & 63)[0:1], (64, 128))
                    low = jnp.where(low == low_ids, 1.0, 0.0).astype(BF16)
                    high = chosen >> 6
                    for n in range(8):
                        here = jnp.where(high == n, 1.0, 0.0)
                        here = jnp.concatenate([here] * 8, axis=0).astype(BF16)
                        hot.append(low * here)
                hot = [jnp.concatenate(hot[:8], axis=0), jnp.concatenate(hot[8:], axis=0)]
                found = dot(tab[...], jnp.concatenate(hot, axis=1))
            if "h" in stages:
                if by_lanes:
                    ahead = dot(win_few[...], pair_in[...])
                else:
                    ahead = dot(win[...], masked_in[:, span]) + base
            if "s" in stages:
                last = dot(wmid[...], hid_in[:, span])
            if "h" in stages:
                hid_out[:, span] = twice_gelu(ahead)
            if "s" in stages:
                last = twice_gelu(last).astype(F32)
                for n in range(2):
                    used = valid > first + (2 * part + n)
                    total = total + jnp.where(used, last[:, n * 128 : (n + 1) * 128], 0.0)
            if "g" not in stages:
                continue
            for n in range(2):
                s = 2 * part + n
                if by_lanes:
                    chosen = jnp.broadcast_to(slots[s : s + 1], (8, 128))
                    block = jnp.broadcast_to(owners[s : s + 1], (8, 128))
                    pair = looked_up(lookup, chosen, block) + centre
                    pair_out[:, pl.ds(n * 128, 128)] = pair.astype(BF16)
                else:
                    chosen = jnp.broadcast_to(owners[s : s + 1], (ROWS, 128))
                    kept = jnp.where(rowblk[...] == chosen, found[:, n * 128 : (n + 1) * 128], 0.0)
                    masked_out[:, pl.ds(s * 128, 128)] = kept.astype(BF16)
        if "s" in stages:
            acc[slab] += total

    even = (masked_a, masked_b, pair_a, pair_b, hid_a, hid_b)
    odd = (masked_b, masked_a, pair_b, pair_a, hid_b, hid_a)

    def two_steps(tt, carry):
        step(2 * tt, *even)
        step(2 * tt + 1, *odd)
        return carry

    def finish(slabs):
        for x in slabs:
            upper, lower = split_two(0.5 * acc[x])
            values = dot(kout_ref[...], upper) + dot(kout_ref[...], lower)
            latent = (values / valid_slots[x, 0:1]).astype(BF16)
            skip_ref[x] = dot_first(wskip_ref[...], latent)
            lat_ref[x] = latent.astype(F32)
        span = pl.ds(8 * slabs[0], 8 * len(slabs))
        for q in range(NZ):
            ready = lat_ref[slabs[0] : slabs[-1] + 1, pl.ds(8 * q, 8), :]
            s1[q, span, :] = ready.reshape(8 * len(slabs), 128).astype(BF16)
        r1[gz, span, :] = s1[gz, span, :]
        return span

    step(0, *even, "g")
    step(1, *odd, "gh")
    lax.fori_loop(1, 13, two_steps, 0)
    span = finish(range(6))
    pl.semaphore_wait(heard.at[2], len(flat_steps))
    for d in far_z:
        peer = along_z(d)
        send(0, s1.at[peer[2], span], r1.at[gz, span], peer)
    lax.fori_loop(13, CHUNKS // 2, two_steps, 0)
    step(CHUNKS, *even, "hs")
    step(CHUNKS + 1, *odd, "s")
    span = finish(range(6, 8))
    for d in far_z:
        peer = along_z(d)
        send(8, s1.at[peer[2], span], r1.at[gz, span], peer)
    row, lane = iota((128, 128), 0), iota((128, 128), 1)
    row_i, lane_i = row // 8 % 8 * 2 + row // 64, lane // 8 % 8 * 2 + lane // 64
    mirror = (row % 8 == lane % 8) & (row_i != 8) & (lane_i == (16 - row_i) % 16)
    mirror = jnp.where(mirror, 1.0, 0.0).astype(BF16)
    row_j, lane_j = row // 16 * 2 + row // 4 % 2, lane // 16 * 2 + lane // 4 % 2
    flip = (row % 4 == 0) & (lane % 4 == 0) & (row // 8 % 2 == lane // 8 % 2)
    flip = flip & (lane_j != 8) & (row_j == (16 - lane_j) % 16)
    flip = jnp.where(flip, jnp.where(lane // 8 % 2 == 0, 1.0, -1.0), 0.0).astype(BF16)
    pick = jnp.where(iota((16, 128), 1) % 16 == iota((16, 128), 0), 1.0, 0.0).astype(BF16)
    own_channel = iota((64, 128), 0) % 8 == iota((64, 128), 1) // 16
    own_mode = iota((32, 1024), 1) // CH == iota((32, 1024), 0) % MODES
    for n in range(5, 10):
        fetch(n).wait()
    for n, span in ((0, pl.ds(0, 48)), (8, pl.ds(48, 16))):
        part = r1.at[pl.ds(0, NZ - 1), span]
        pltpu.make_async_copy(part, part, recv_sem.at[n]).wait()
    line = jnp.concatenate([r1[q] for q in range(NZ)], axis=1)
    deep = dot(line, fzh[...]) + dot(line, fzl[...])
    for q in range(NY):
        s2[q] = deep[:, q * 128 : (q + 1) * 128]
    for d in (2, 1, 3):
        peer = along_y(d)
        send(1, s2.at[peer[1]], r2.at[gy], peer)
    r2[gy] = s2[gy]
    arrived(1, r2, NY - 1)
    upper, lower = split_two(jnp.concatenate([r2[q] for q in range(NY)], axis=1))
    flat = dot(upper, fyh_ref[...]) + dot(upper, fyl_ref[...]) + dot(lower, fyh_ref[...])
    real = iota((64, 128), 1) // 8 % 2 == 0
    turned = jnp.where(real, pltpu.roll(flat, 120, axis=1), -pltpu.roll(flat, 8, axis=1))
    upper, lower = split_two(jnp.concatenate([flat, turned], axis=0))
    share = block_swap(dot(fxh[...], upper) + dot(fxl[...], upper) + dot(fxh[...], lower))
    for i in range(2):
        s4[:, i, :] = share[64 * i : 64 * i + 64]
    for peer in plane:
        send(2, s4.at[peer[2] * NX + peer[0]], r4.at[me], peer)
    r4[me] = s4[me]
    arrived(2, r4, 63)
    for q in range(NZ):
        pair = r4[q * NX]
        for n in range(1, NX):
            pair = pair + r4[q * NX + n]
        grid[pl.ds(2 * q, 2), :] = pair
    found = []
    for i in range(2):
        values = jnp.concatenate(
            [jnp.broadcast_to(grid[pl.ds(2 * q + i, 1), :], (8, 128)) for q in range(NZ)], axis=0
        )
        values = jnp.where(own_channel, values, 0.0).astype(BF16)
        found.append(
            lax.dot_general(
                pick,
                jnp.concatenate([values, values], axis=0),
                (((1,), (1,)), ((), ())),
                preferred_element_type=F32,
            )
        )
    rows = jnp.concatenate(
        [found[0][0:8], found[1][0:8], found[0][8:16], found[1][8:16]], axis=0
    )
    spread = jnp.where(own_mode, jnp.concatenate([rows] * 8, axis=1), 0.0).astype(BF16)
    by_real, by_imag = dot(spread, w_ref[0:1024]), dot(spread, w_ref[1024:2048])
    mixed_real = by_real[0:16] - by_imag[16:32]
    mixed_imag = by_imag[0:16] + by_real[16:32]
    for i in range(2):
        mine = jnp.concatenate(
            [mixed_real[8 * i : 8 * i + 8], mixed_imag[8 * i : 8 * i + 8]], axis=0
        ).astype(BF16)
        placed = jnp.where(own_channel, dot_first(mine, pick), 0.0).astype(BF16)
        s5[:, i, :] = dot(gather, placed)
    for peer in plane:
        send(3, s5.at[peer[2]], r5.at[me], peer)
    r5[me] = s5[gz]
    arrived(3, r5, 63)
    values = block_swap(jnp.concatenate([r5[:, i, :] for i in range(2)], axis=0))
    is_mean = (row < 8) & ((lane == 0) | (lane == 8)) & (gy == 0)
    values = jnp.where(is_mean, 0.0, values)
    exact = values.astype(BF16)
    real = lane // 8 % 2 == 0
    turned = jnp.where(real, -pltpu.roll(values, 120, axis=1), pltpu.roll(values, 8, axis=1))
    stacked = jnp.concatenate([exact, turned.astype(BF16)], axis=0)
    plain = (dot(ixh[...], stacked) + dot(ixl[...], stacked)).astype(BF16)
    flat = dot(plain, iyh_ref[...]) + dot(plain, iyl_ref[...])
    for q in range(NY):
        s7[q] = flat[:, q * 128 : (q + 1) * 128].astype(BF16)
    halves = [pl.ds(32 * h, 32) for h in range(2)]
    for h, span in enumerate(halves):
        for d in (2, 1, 3):
            peer = along_y(d)
            send((4, 9)[h], s7.at[peer[1], span], r7.at[gy, span], peer)
    r7[gy] = s7[gy]
    weight = jnp.where((lane % 4 == 0) & (gy == 0), 0.5, 2.0)
    pairs = dot(dot(mirror, exact).astype(BF16), flip)
    pairs = jnp.where(gy == 0, 0.5 * pairs, 0.0)
    power = jnp.sum(values * (weight * values + pairs), axis=1, keepdims=True)
    power = jnp.sum(power.reshape(16, 8, 1), axis=0)
    sv[...] = jnp.broadcast_to(power, (8, 128))
    for d in range(1, NY):
        send(5, sv, rv.at[gy], along_y(d))
    rv[gy] = sv[...]
    def both_waits(sems, n, buffer, count, span):
        part = buffer.at[pl.ds(0, count), span]
        pltpu.make_async_copy(part, part, sems.at[n]).wait()

    for h, span in enumerate(halves):
        both_waits(recv_sem, (4, 9)[h], r7, NY - 1, span)
        line = jnp.concatenate([r7[q, span, :] for q in range(NY)], axis=1)
        depth = dot(line, iz[...])
        if h == 0:
            arrived(5, rv, NY - 1)
            power = (rv[0] + rv[1]) + (rv[2] + rv[3])
            scale = 1.0 / jnp.sqrt(power * (1.0 / float(GRID) ** 6) + 1.0)
            scale = jnp.concatenate([scale] * 4, axis=0)
        for q in range(NZ):
            s8[q, span, :] = (depth[:, q * 128 : (q + 1) * 128] * scale).astype(BF16)
        for d in far_z:
            peer = along_z(d)
            send((6, 10)[h], s8.at[peer[2], span], r8.at[gz, span], peer)
        r8[gz, span, :] = s8[gz, span, :]

    def put(x):
        return pltpu.make_async_copy(result.at[x], out_ref.at[x], out_sem.at[x])

    for h, span in enumerate(halves):
        both_waits(recv_sem, (6, 10)[h], r8, NZ - 1, span)
        wide[:, span, :] = r8[:, span, :].astype(F32)
        for x in range(4 * h, 4 * h + 4):
            result[x] = gelu(wide[:, pl.ds(8 * x, 8), :].reshape(CH, 128) + skip_ref[x]).T
            put(x).start()
    for n, span in ((0, pl.ds(0, 48)), (8, pl.ds(48, 16))):
        part = r1.at[pl.ds(0, NZ - 1), span]
        pltpu.make_async_copy(part, part, send_sem.at[n]).wait()
    left(1, r2, NY - 1)
    left(2, r4, 63)
    left(3, r5, 63)
    for h, span in enumerate(halves):
        both_waits(send_sem, (4, 9)[h], r7, NY - 1, span)
        both_waits(send_sem, (6, 10)[h], r8, NZ - 1, span)
    for x in range(8):
        put(x).wait()
    left(5, rv, NY - 1)
    left(7, around, 26)


def whole(points, counts, kin, kmid, kout, wskip, near, weights):
    fz, fy, fx, ix, iy, iz = transform_tables()
    tables = [wide_table(fz), *two_tables(fy), wide_table(fx), wide_table(ix)]
    tables += [*two_tables(iy), wide_table(iz)]
    anywhere = pl.BlockSpec(memory_space=pl.ANY)
    v = pltpu.VMEM
    return pl.pallas_call(
        whole_kernel,
        out_shape=jax.ShapeDtypeStruct((8, 128, CH), F32),
        in_specs=[anywhere] * (8 + len(tables)),
        out_specs=anywhere,
        scratch_shapes=[
            v((24, 128), F32), v((64, 16), jnp.int32), v((6, KH), BF16), v((KH, KH), BF16),
            v((CH, KH), BF16), v((CH, CH), BF16),
            v((8, 128, NB), jnp.int32), v((2048, CH), BF16),
            v((GRID, 512), F32), v((512, 128), BF16), v((512, 128), BF16),
            v((16, 128), F32), v((8, 256), F32), v((128, 512), BF16), v((128, 512), BF16),
            v((32, 1024), F32),
            v((27, 24, 128), F32), v((ROWS, PTS), F32), v((ROWS, PTS), BF16),
            v((CHUNKS, 8, 128), jnp.int32), v((CHUNKS, 8, 128), jnp.int32), v((8, 8, 128), F32),
            v((108, 8, 128), F32), v((8, 8, 128), F32), v((KH, 8), BF16),
            v((8, 256), BF16), v((8, 256), BF16),
            v((8, KH, 128), F32), v((ROWS, 128), jnp.int32),
            v((KH, ROWS), BF16), v((KH, KH), BF16),
            v((ROWS, 1024), BF16), v((ROWS, 1024), BF16), v((KH, 1024), BF16), v((KH, 1024), BF16),
            v((8, KH, 128), F32), v((8, CH, 128), F32), v((8, CH, 128), F32),
            v((128, 128), BF16), v((128, 128), BF16), v((64, 256), BF16), v((64, 256), BF16),
            v((NZ, 64, 128), BF16), v((NZ, 64, 128), BF16),
            v((NY, 64, 128), F32), v((NY, 64, 128), F32),
            v((CH, 2, 128), F32), v((CH, 2, 128), F32),
            v((NZ, 2, 128), F32), v((CH, 2, 128), F32),
            v((NY, 64, 128), BF16), v((NY, 64, 128), BF16),
            v((8, 128), F32), v((NY, 8, 128), F32),
            v((NZ, 64, 128), BF16), v((NZ, 64, 128), BF16),
            v((1024, 512), BF16), v((1024, 512), BF16), v((512, 1024), BF16),
            v((MODES, 128), F32), v((NZ, 64, 128), F32),
            v((8, 128, CH), F32), pltpu.SemaphoreType.DMA((11,)), pltpu.SemaphoreType.DMA((11,)),
            pltpu.SemaphoreType.DMA((16,)), pltpu.SemaphoreType.REGULAR((3,)),
            pltpu.SemaphoreType.DMA((8,)),
        ],
        compiler_params=pltpu.CompilerParams(collective_id=0, has_side_effects=True),
        name="whole",
    )(points, counts, kin, kmid, kout, wskip, near, weights, *tables)


def body(point_data, neighbours, counts, kernel_in, kernel_mid, kernel_out, spectral, skip_weight):
    out = whole(
        point_data.reshape(24, 128),
        jnp.swapaxes(counts[0], 1, 2).reshape(64, 16),
        kernel_in,
        kernel_mid,
        kernel_out.T,
        skip_weight,
        neighbours.reshape(8, 128, NB),
        spectral.reshape(2048, CH),
    )
    return out.reshape(1, 8, 16, 8, CH)


def solution(mesh):
    cells = P(None, "gx", "gy", "gz", None)
    return jax.shard_map(
        body,
        mesh=mesh,
        in_specs=(
            P(None, None, ("gx", "gy", "gz")),
            cells,
            P(None, "gx", "gy", "gz"),
            P(),
            P(),
            P(),
            P(None, "gz", "gx", "gy", None, None),
            P(),
        ),
        out_specs=cells,
        check_vma=False,
    )
```
